128 devices in a mesh: dp: 1, tp: 16 (over z, y), dm: 8 (over x, core).
Axes of the slice: x: 4, y: 4, z: 4, core: 2. Of those that a mesh axis runs over, the one named last changes fastest.
Arguments:
- resid_in: bfloat16 [1536, 3072], P('dp', 'dm')
- k_cache: bfloat16 [1536, 16, 16, 256], P(('dp', 'dm'), 'tp')
- v_cache: bfloat16 [1536, 16, 16, 256], P(('dp', 'dm'), 'tp')
- cache_len: int32 [1536], P('dp')
- norm_attn: bfloat16 [3072], P('dm')
- w_q: bfloat16 [3072, 4096], P('dm', 'tp')
- w_k: bfloat16 [3072, 4096], P('dm', 'tp')
- w_v: bfloat16 [3072, 4096], P('dm', 'tp')
- w_o: bfloat16 [4096, 3072], P('tp', 'dm')
- norm_mlp: bfloat16 [3072], P('dm')
- w_gate: bfloat16 [3072, 24576], P('dm', 'tp')
- w_up: bfloat16 [3072, 24576], P('dm', 'tp')
- w_down: bfloat16 [24576, 3072], P('tp', 'dm')
Outputs:
- output 1: bfloat16 [1536, 3072], P('dp', 'dm')
- output 2: bfloat16 [1536, 16, 16, 256], P(('dp', 'dm'), 'tp')
- output 3: bfloat16 [1536, 16, 16, 256], P(('dp', 'dm'), 'tp')
All inputs are finite; a program needn't handle non-finite values.
Results may differ from the reference program's by a relative error of at most 0.010591.
Values are sent between devices in bfloat16 or wider.
A program may use at most 1 GiB of HBM per device.

```python
import jax
import jax.numpy as jnp
from jax import lax

D_MODEL = 3072
NUM_HEADS = 16
HEAD_DIM = 256
FF_DIM = 24576
BATCH_ROWS = 1536
MAX_LEN = 16
EPSILON = 1e-6
ROPE_THETA = 10000.0


def setup_inputs(seed: int = 0, part: int = 0) -> dict:
    root_key = jax.random.key(seed)
    part_key = jax.random.fold_in(root_key, part)
    weight_keys = jax.random.split(root_key, 9)
    part_keys = jax.random.split(part_key, 6)
    attn_width = NUM_HEADS * HEAD_DIM
    col_pos = jnp.arange(D_MODEL, dtype=jnp.float32) / D_MODEL - 0.5
    slope_val = jax.random.uniform(part_keys[0], (), minval=1.2, maxval=1.8)
    col_scale = jnp.exp(slope_val * col_pos)
    resid_in = (jax.random.normal(part_keys[1], (BATCH_ROWS, D_MODEL)) * col_scale).astype(jnp.bfloat16)
    cache_shape = (BATCH_ROWS, NUM_HEADS, MAX_LEN, HEAD_DIM)
    k_cache = jax.random.normal(part_keys[2], cache_shape).astype(jnp.bfloat16)
    value_mean = 0.5 * jax.random.normal(part_keys[3], (BATCH_ROWS, NUM_HEADS, 1, HEAD_DIM))
    v_cache = (value_mean + jax.random.normal(part_keys[4], cache_shape)).astype(jnp.bfloat16)
    len_keys = jax.random.split(part_keys[5], 2)
    len_draw = jax.random.randint(len_keys[0], (BATCH_ROWS,), 0, MAX_LEN, dtype=jnp.int32)
    row_order = jax.random.permutation(len_keys[1], BATCH_ROWS)
    cache_len = len_draw.at[row_order[0]].set(MAX_LEN - 1).at[row_order[1]].set(0)
    d_scale = D_MODEL ** -0.5
    return {
        'resid_in': resid_in,
        'k_cache': k_cache,
        'v_cache': v_cache,
        'cache_len': cache_len,
        'norm_attn': (0.4 * jax.random.normal(weight_keys[0], (D_MODEL,))).astype(jnp.bfloat16),
        'w_q': (jax.random.normal(weight_keys[1], (D_MODEL, attn_width)) * d_scale).astype(jnp.bfloat16),
        'w_k': (jax.random.normal(weight_keys[2], (D_MODEL, attn_width)) * d_scale).astype(jnp.bfloat16),
        'w_v': (jax.random.normal(weight_keys[3], (D_MODEL, attn_width)) * d_scale).astype(jnp.bfloat16),
        'w_o': (jax.random.normal(weight_keys[4], (attn_width, D_MODEL)) * attn_width ** -0.5).astype(jnp.bfloat16),
        'norm_mlp': (0.4 * jax.random.normal(weight_keys[5], (D_MODEL,))).astype(jnp.bfloat16),
        'w_gate': (jax.random.normal(weight_keys[6], (D_MODEL, FF_DIM)) * d_scale).astype(jnp.bfloat16),
        'w_up': (jax.random.normal(weight_keys[7], (D_MODEL, FF_DIM)) * d_scale).astype(jnp.bfloat16),
        'w_down': (jax.random.normal(weight_keys[8], (FF_DIM, D_MODEL)) * FF_DIM ** -0.5).astype(jnp.bfloat16),
    }


def rope_rotate(vectors, positions):
    half_dim = HEAD_DIM // 2
    inv_freq = ROPE_THETA ** (-2.0 * jnp.arange(half_dim, dtype=jnp.float32) / HEAD_DIM)
    angles = positions.astype(jnp.float32)[:, None] * inv_freq[None, :]
    cos_part = jnp.cos(angles)[:, None, :]
    sin_part = jnp.sin(angles)[:, None, :]
    first_half = vectors[..., :half_dim]
    second_half = vectors[..., half_dim:]
    return jnp.concatenate([first_half * cos_part - second_half * sin_part, second_half * cos_part + first_half * sin_part], axis=-1)


def rms_norm(rows_f, norm_gain):
    mean_sq = jnp.mean(rows_f * rows_f, axis=-1, keepdims=True)
    return (rows_f * lax.rsqrt(mean_sq + EPSILON) * (1.0 + norm_gain.astype(jnp.float32))).astype(jnp.bfloat16)


def reference(resid_in, k_cache, v_cache, cache_len, norm_attn, w_q, w_k, w_v, w_o, norm_mlp, w_gate, w_up, w_down):
    attn_width = NUM_HEADS * HEAD_DIM
    head_shape = (BATCH_ROWS, NUM_HEADS, HEAD_DIM)
    resid_f = resid_in.astype(jnp.float32)
    normed = rms_norm(resid_f, norm_attn)
    q_proj = jnp.dot(normed, w_q, preferred_element_type=jnp.float32).reshape(head_shape)
    k_proj = jnp.dot(normed, w_k, preferred_element_type=jnp.float32).reshape(head_shape)
    v_new = jnp.dot(normed, w_v, preferred_element_type=jnp.float32).reshape(head_shape).astype(jnp.bfloat16)
    q_rot = (rope_rotate(q_proj, cache_len) * HEAD_DIM ** -0.5).astype(jnp.bfloat16)
    k_new = rope_rotate(k_proj, cache_len).astype(jnp.bfloat16)
    slot_ids = jnp.arange(MAX_LEN)
    slot_hit = (slot_ids[None, :] == cache_len[:, None])[:, :, None]
    valid_mask = slot_ids[None, :] <= cache_len[:, None]

    def head_step(head_args):
        q_head, k_head, v_head, new_k_head, new_v_head = head_args
        k_upd = jnp.where(slot_hit, new_k_head[:, None, :], k_head)
        v_upd = jnp.where(slot_hit, new_v_head[:, None, :], v_head)
        scores = jnp.einsum('be,bte->bt', q_head.astype(jnp.float32), k_upd.astype(jnp.float32))
        scores = jnp.where(valid_mask, scores, -1e30)
        attn_probs = jax.nn.softmax(scores, axis=-1).astype(jnp.bfloat16)
        head_out = jnp.einsum('bt,bte->be', attn_probs.astype(jnp.float32), v_upd.astype(jnp.float32))
        return head_out.astype(jnp.bfloat16), k_upd, v_upd

    head_outs, k_heads, v_heads = lax.map(head_step, (jnp.moveaxis(q_rot, 1, 0), jnp.moveaxis(k_cache, 1, 0), jnp.moveaxis(v_cache, 1, 0), jnp.moveaxis(k_new, 1, 0), jnp.moveaxis(v_new, 1, 0)))
    attn_flat = jnp.moveaxis(head_outs, 0, 1).reshape(BATCH_ROWS, attn_width)
    mid_f = (resid_f + jnp.dot(attn_flat, w_o, preferred_element_type=jnp.float32)).astype(jnp.bfloat16).astype(jnp.float32)
    normed_mlp = rms_norm(mid_f, norm_mlp)
    gate_val = jnp.dot(normed_mlp, w_gate, preferred_element_type=jnp.float32)
    up_val = jnp.dot(normed_mlp, w_up, preferred_element_type=jnp.float32)
    hidden = (jax.nn.gelu(gate_val, approximate=True) * up_val).astype(jnp.bfloat16)
    resid_out = (mid_f + jnp.dot(hidden, w_down, preferred_element_type=jnp.float32)).astype(jnp.bfloat16)
    return resid_out, jnp.moveaxis(k_heads, 0, 1), jnp.moveaxis(v_heads, 0, 1)
```

```python
import functools

import jax
import jax.numpy as jnp
from jax import lax
from jax.experimental import pallas as pl
from jax.experimental.pallas import tpu as pltpu
from jax.sharding import PartitionSpec as P

EPSILON = 1e-6
ROPE_THETA = 10000.0
BF = jnp.bfloat16
F32 = jnp.float32
LOGICAL = pl.DeviceIdType.LOGICAL


class Comm:
    def __init__(self, ssem, rsem):
        self.ssem, self.rsem, self.n, self.copies = ssem, rsem, 0, []
        tp, dm = lax.axis_index('tp'), lax.axis_index('dm')
        self.tp, self.dm = tp, dm
        self.z, self.y = lax.div(tp, 4), lax.rem(tp, 4)
        self.x, self.c = lax.div(dm, 2), lax.rem(dm, 2)

    def ring(self, axis):
        i = {'x': self.x, 'y': self.y, 'z': self.z}[axis]
        idx = [lax.rem(i + k, 4) for k in range(4)]
        dev = [self.at(axis, j) for j in idx]
        return idx, dev

    def at(self, axis, j):
        if axis == 'x':
            return self.tp * 8 + j * 2 + self.c
        if axis == 'y':
            return (self.z * 4 + j) * 8 + self.dm
        return (j * 4 + self.y) * 8 + self.dm

    def other(self):
        return self.tp * 8 + self.x * 2 + 1 - self.c

    def barrier(self, peers):
        sem = pltpu.get_barrier_semaphore()
        for dev in peers:
            pl.semaphore_signal(sem, inc=1, device_id=dev, device_id_type=LOGICAL)
        pl.semaphore_wait(sem, len(peers))

    def send(self, src, dst, dev):
        k = self.n
        self.n += 1
        copy = pltpu.make_async_remote_copy(src_ref=src, dst_ref=dst, send_sem=self.ssem.at[k], recv_sem=self.rsem.at[k], device_id=dev, device_id_type=LOGICAL)
        copy.start()
        self.copies.append(copy)
        return copy

    def drain(self):
        for copy in self.copies:
            copy.wait_send()


def run(*gens):
    gens = list(gens)
    while gens:
        for g in list(gens):
            try:
                next(g)
            except StopIteration:
                gens.remove(g)


def gather4(cm, axis, blk, hf, own=None):
    (i, r, o, l), (_, dr, _, dl) = cm.ring(axis)
    own = blk(i) if own is None else own
    a = cm.send(own, blk(i), dr)
    b = cm.send(own, blk(i), dl)
    yield
    a.wait_recv()
    c = cm.send(hf(l, 0), hf(l, 0), dr)
    b.wait_recv()
    d = cm.send(hf(r, 1), hf(r, 1), dl)
    yield
    c.wait_recv()
    d.wait_recv()


def scatter4(cm, axis, blk, hf, ro0, ro1, rl, rr, hrx):
    (i, r, o, l), (_, dr, _, dl) = cm.ring(axis)
    c0 = cm.send(hf(o, 0), ro0, dr)
    c1 = cm.send(hf(o, 1), ro1, dl)
    c2 = cm.send(hf(r, 1), hrx(rl, 1), dr)
    c3 = cm.send(hf(l, 0), hrx(rr, 0), dl)
    yield
    c0.wait_recv()
    hf(r, 0)[...] += ro0[...]
    c4 = cm.send(hf(r, 0), hrx(rl, 0), dr)
    c1.wait_recv()
    hf(l, 1)[...] += ro1[...]
    c5 = cm.send(hf(l, 1), hrx(rr, 1), dl)
    yield
    for c in (c2, c3, c4, c5):
        c.wait_recv()
    blk(i)[...] += rl[...] + rr[...]


def plane_scatter(cm, p, h, rx):
    ro, rb, so, sb = rx
    ph = p.at[h]
    if h == 0:
        big = lambda j: ph.at[:, j]
        bigh = lambda j, s: ph.at[2 * s:2 * s + 2, j]
        small = lambda j: ph.at[j, cm.y]
        smallh = lambda j, s: ph.at[j, cm.y, 24 * s:24 * s + 24]
        axes = ('y', 'z')
    else:
        big = lambda j: ph.at[j]
        bigh = lambda j, s: ph.at[j, 2 * s:2 * s + 2]
        small = lambda j: ph.at[cm.z, j]
        smallh = lambda j, s: ph.at[cm.z, j, 24 * s:24 * s + 24]
        axes = ('z', 'y')
    yield from scatter4(cm, axes[0], big, bigh, ro.at[h, 0], ro.at[h, 1], rb.at[h, 0], rb.at[h, 1], lambda b, s: b.at[2 * s:2 * s + 2])
    yield from scatter4(cm, axes[1], small, smallh, so.at[h, 0], so.at[h, 1], sb.at[h, 0], sb.at[h, 1], lambda b, s: b.at[24 * s:24 * s + 24])


def plane_gather(cm, m, h, split):
    mh = m.at[h]
    cols = m.shape[-1]
    cut = lambda s: pl.ds(0, split) if s == 0 else pl.ds(split, cols - split)
    if h == 0:
        yield from gather4(cm, 'y', lambda j: mh.at[cm.z, j], lambda j, s: mh.at[cm.z, j, :, cut(s)])
        yield from gather4(cm, 'z', lambda j: mh.at[j], lambda j, s: mh.at[j, 2 * s:2 * s + 2])
    else:
        yield from gather4(cm, 'z', lambda j: mh.at[j, cm.y], lambda j, s: mh.at[j, cm.y, :, cut(s)])
        yield from gather4(cm, 'y', lambda j: mh.at[:, j], lambda j, s: mh.at[2 * s:2 * s + 2, j])


def gain_row(g_ref, d, k):
    g = g_ref[d]
    return jnp.concatenate([g[3 * k + j:3 * k + j + 1] for j in range(3)], axis=1)


def qkv_kernel(x_ref, wq_ref, wk_ref, wv_ref, gain_ref, q_ref, k_ref, v_ref, g_ref, w_buf, xg, n_buf, ssem, rsem):
    cm = Comm(ssem, rsem)
    x, c, dm = cm.x, cm.c, cm.dm
    ring_y, ring_z, ring_x = cm.ring('y'), cm.ring('z'), cm.ring('x')
    peers = [cm.tp * 8 + lax.rem(dm + k, 8) for k in range(1, 8)]
    plane = [ring_y[1][1], ring_y[1][3], ring_z[1][1], ring_z[1][3]]
    cm.barrier(peers + plane)

    sl = jnp.where(c == 0, cm.y, cm.z)
    xs = []
    for k, dev in enumerate(peers):
        start = pl.multiple_of(lax.rem(dm + k + 1, 8) * 192 + sl * 48, 16)
        xs.append(cm.send(x_ref.at[pl.ds(start, 48), :], xg.at[c, sl, x], dev))
    gs = [cm.send(gain_ref, g_ref.at[dm], dev) for dev in peers]
    (i, r, o, l), (_, dr, _, dl) = ring_x
    dev_o = cm.other()
    rows = lambda j: w_buf.at[j * 2 + c]
    ws = (wq_ref, wk_ref, wv_ref)
    a = [cm.send(w, rows(i).at[n], dr) for n, w in enumerate(ws)]
    b = [cm.send(w, rows(i).at[n], dl) for n, w in enumerate(ws)]
    e = [cm.send(w, rows(i).at[n], dev_o) for n, w in enumerate(ws)]
    for n, w in enumerate(ws):
        w_buf[dm, n] = w[...]
    g_ref[dm] = gain_ref[...]
    own = pl.multiple_of(dm * 192 + sl * 48, 16)
    xg[c, sl, x] = x_ref[pl.ds(own, 48), :]
    for cp in xs:
        cp.wait_recv()

    def w_ring():
        yield
        yield
        for cp in a:
            cp.wait_recv()
        f0 = cm.send(rows(l).at[:, 0:192], rows(l).at[:, 0:192], dr)
        e1 = cm.send(rows(l), rows(l), dev_o)
        for cp in b:
            cp.wait_recv()
        f1 = cm.send(rows(r).at[:, 192:384], rows(r).at[:, 192:384], dl)
        e2 = cm.send(rows(r), rows(r), dev_o)
        yield
        f0.wait_recv()
        f1.wait_recv()
        e3 = cm.send(rows(o), rows(o), dev_o)
        for cp in e + [e1, e2, e3]:
            cp.wait_recv()

    gy = gather4(cm, 'y', lambda j: xg.at[0, j], lambda j, s: xg.at[0, j, 2 * s:2 * s + 2])
    gz = gather4(cm, 'z', lambda j: xg.at[1, j], lambda j, s: xg.at[1, j, 2 * s:2 * s + 2])
    run(gy, gz, w_ring())
    for cp in gs:
        cp.wait_recv()

    total = jnp.zeros((192, 1), F32)
    for d in range(8):
        v = xg[d % 2, :, d // 2].reshape(192, 384).astype(F32)
        total += jnp.sum(v * v, axis=1, keepdims=True)
    inv = lax.rsqrt(total / 3072 + EPSILON)
    for d in range(8):
        v = xg[d % 2, :, d // 2].reshape(192, 384).astype(F32)
        n_buf[d] = (v * inv * (1.0 + gain_row(g_ref, d, 0))).astype(BF)
    for n, out in enumerate((q_ref, k_ref, v_ref)):
        acc = jnp.zeros((192, 256), F32)
        for d in range(8):
            acc += jnp.dot(n_buf[d], w_buf[d, n], preferred_element_type=F32)
        out[...] = acc
    cm.drain()


def proj_kernel(o_ref, x_ref, wo_ref, wg_ref, wu_ref, g_ref, m_buf, w_gu, h_ref, o_buf, wo_o, x_o, p1, ro, rb, so, sb, hs, t0, t1, ssem, rsem):
    cm = Comm(ssem, rsem)
    x, c, dm, y, z = cm.x, cm.c, cm.dm, cm.y, cm.z
    (_, r, o, l), (_, dr, _, dl) = cm.ring('x')
    ring_y, ring_z = cm.ring('y'), cm.ring('z')
    dev_o = cm.other()
    cm.barrier([dev_o, dr, dl, ring_y[1][1], ring_y[1][3], ring_z[1][1], ring_z[1][3]])

    ro_0, ro_1 = ro, so
    go = gather4(cm, 'x', lambda j: o_buf.at[j], lambda j, s: o_buf.at[j, 96 * s:96 * s + 96], own=o_ref)
    next(go)
    o_buf[x] = o_ref[...]
    row = lambda core: pl.multiple_of(192 * (2 * z + core) + 48 * y, 16)
    c_wo = cm.send(wo_ref, wo_o, dev_o)
    c_x = cm.send(x_ref.at[pl.ds(row(1 - c), 48), :], x_o, dev_o)
    for _ in go:
        pass
    kblk = lambda j, core: pl.ds(pl.multiple_of((j * 2 + core) * 384, 16), 384)
    hcol = lambda j: pl.ds(pl.multiple_of(j * 384, 128), 384)
    c_t0 = cm.send(wg_ref.at[:, hcol(o)], t0, dr)
    c_t1 = cm.send(wu_ref.at[:, hcol(o)], t1, dl)
    c_gr = cm.send(wg_ref.at[:, hcol(r)], w_gu.at[kblk(x, c), 0:384], dr)
    c_gl = cm.send(wg_ref.at[:, hcol(l)], w_gu.at[kblk(x, c), 0:384], dl)
    c_ur = cm.send(wu_ref.at[:, hcol(r)], w_gu.at[kblk(x, c), 384:768], dr)
    c_ul = cm.send(wu_ref.at[:, hcol(l)], w_gu.at[kblk(x, c), 384:768], dl)
    c_og = cm.send(wg_ref.at[:, hcol(x)], w_gu.at[kblk(x, c), 0:384], dev_o)
    c_ou = cm.send(wu_ref.at[:, hcol(x)], w_gu.at[kblk(x, c), 384:768], dev_o)
    w_gu[kblk(x, c), 0:384] = wg_ref[:, hcol(x)]
    w_gu[kblk(x, c), 384:768] = wu_ref[:, hcol(x)]

    c_wo.wait_recv()

    def o_proj(j, carry):
        v = o_buf[j]
        p1[c, j] = jnp.dot(v, wo_ref[...], preferred_element_type=F32).reshape(4, 48, 384)
        p1[1 - c, j] = jnp.dot(v, wo_o[...], preferred_element_type=F32).reshape(4, 48, 384)
        return carry

    lax.fori_loop(0, 4, o_proj, 0)

    def w_deal():
        yield
        yield
        yield
        c_t0.wait_recv()
        f0 = cm.send(t0, w_gu.at[kblk(l, c), 0:384], dr)
        c_t1.wait_recv()
        f1 = cm.send(t1, w_gu.at[kblk(r, c), 384:768], dl)
        yield
        c_gr.wait_recv()
        c_ur.wait_recv()
        e1 = cm.send(w_gu.at[kblk(l, c)], w_gu.at[kblk(l, c)], dev_o)
        c_gl.wait_recv()
        c_ul.wait_recv()
        e2 = cm.send(w_gu.at[kblk(r, c)], w_gu.at[kblk(r, c)], dev_o)
        deal.extend([f0, f1, e1, e2])

    deal = []
    run(plane_scatter(cm, p1, 0, (ro, rb, so, sb)), plane_scatter(cm, p1, 1, (ro, rb, so, sb)), w_deal())

    c_x.wait_recv()
    hs[x, c] = (x_ref[pl.ds(row(c), 48), :].astype(F32) + p1[c, z, y]).astype(BF)
    hs[x, 1 - c] = (x_o[...].astype(F32) + p1[1 - c, z, y]).astype(BF)
    run(gather4(cm, 'x', lambda j: hs.at[j], lambda j, s: hs.at[j, s]))
    total = jnp.zeros((48, 1), F32)
    for d in range(8):
        v = hs[d // 2, d % 2].astype(F32)
        total += jnp.sum(v * v, axis=1, keepdims=True)
    inv = lax.rsqrt(total / 3072 + EPSILON)
    for d in range(8):
        v = hs[d // 2, d % 2].astype(F32)
        m_buf[d // 4, z, y, :, 384 * (d % 4):384 * (d % 4) + 384] = (v * inv * (1.0 + gain_row(g_ref, d, 1))).astype(BF)

    def w_last():
        f0, f1, e1, e2 = deal
        yield
        f0.wait_recv()
        f1.wait_recv()
        e3 = cm.send(w_gu.at[kblk(o, c)], w_gu.at[kblk(o, c)], dev_o)
        yield
        for cp in (c_og, c_ou, e1, e2, e3):
            cp.wait_recv()

    run(plane_gather(cm, m_buf, 0, 768), plane_gather(cm, m_buf, 1, 768), w_last())
    h_ref[...] = hs[x]
    cm.drain()


def mlp_kernel(m_buf, w_gu, h_ref, wd_ref, out_ref, wd_o, p2, ro, rb, so, sb, a_buf, u_buf, v_buf, ssem, rsem):
    cm = Comm(ssem, rsem)
    x, c, dm, y, z = cm.x, cm.c, cm.dm, cm.y, cm.z
    (_, r, o, l), (_, dr, _, dl) = cm.ring('x')
    ring_y, ring_z = cm.ring('y'), cm.ring('z')
    dev_o = cm.other()
    cm.barrier([dev_o, dr, dl, ring_y[1][1], ring_y[1][3], ring_z[1][1], ring_z[1][3]])
    hcol = lambda j: pl.ds(pl.multiple_of(j * 384, 128), 384)
    c_wd = cm.send(wd_ref, wd_o, dev_o)

    def gate_up(j, carry):
        m0 = m_buf[0, j].reshape(192, 1536)
        m1 = m_buf[1, j].reshape(192, 1536)
        acc = jnp.dot(m0, w_gu[0:1536], preferred_element_type=F32) + jnp.dot(m1, w_gu[1536:3072], preferred_element_type=F32)
        gate, up = acc[:, 0:384], acc[:, 384:768]
        a_buf[j, :, hcol(x)] = (0.5 * gate * (1.0 + jnp.tanh(0.7978845608 * (gate + 0.044715 * (gate * gate * gate)))) * up).astype(BF)
        return carry

    lax.fori_loop(0, 4, gate_up, 0)
    run(gather4(cm, 'x', lambda j: a_buf.at[:, :, hcol(j)], lambda j, s: a_buf.at[2 * s:2 * s + 2, :, hcol(j)]))
    c_wd.wait_recv()

    def down(j, carry):
        v = a_buf[j]
        p2[c, j] = jnp.dot(v, wd_ref[...], preferred_element_type=F32).reshape(4, 48, 384)
        p2[1 - c, j] = jnp.dot(v, wd_o[...], preferred_element_type=F32).reshape(4, 48, 384)
        return carry

    lax.fori_loop(0, 4, down, 0)
    run(plane_scatter(cm, p2, 0, (ro, rb, so, sb)), plane_scatter(cm, p2, 1, (ro, rb, so, sb)))
    for h in range(2):
        u_buf[h, z, y] = (h_ref[h].astype(F32) + p2[h, z, y]).astype(BF)
    run(plane_gather(cm, u_buf, 0, 256), plane_gather(cm, u_buf, 1, 256))
    c_v = cm.send(u_buf.at[1 - c], v_buf, dev_o)
    blk = lambda j, core: pl.ds(pl.multiple_of(192 * (2 * j + core), 16), 192)
    for j in range(4):
        out_ref[blk(j, c), :] = u_buf[c, j].reshape(192, 384)
    c_v.wait_recv()
    for j in range(4):
        out_ref[blk(j, 1 - c), :] = v_buf[j].reshape(192, 384)
    cm.drain()


def rope_rotate(vectors, positions):
    half_dim = vectors.shape[-1] // 2
    inv_freq = ROPE_THETA ** (-2.0 * jnp.arange(half_dim, dtype=jnp.float32) / vectors.shape[-1])
    angles = positions.astype(jnp.float32)[:, None] * inv_freq[None, :]
    cos_part = jnp.cos(angles)[:, None, :]
    sin_part = jnp.sin(angles)[:, None, :]
    first_half = vectors[..., :half_dim]
    second_half = vectors[..., half_dim:]
    return jnp.concatenate([first_half * cos_part - second_half * sin_part, second_half * cos_part + first_half * sin_part], axis=-1)


def attend(q_rot, k_cache, v_cache, k_new, v_new, lengths):
    slot_ids = jnp.arange(k_cache.shape[2])
    slot_hit = slot_ids[None, :] == lengths[:, None]
    valid_mask = slot_ids[None, :] <= lengths[:, None]
    k_upd = jnp.where(slot_hit[:, None, :, None], k_new[:, :, None, :], k_cache)
    v_upd = jnp.where(slot_hit[:, None, :, None], v_new[:, :, None, :], v_cache)
    scores = jnp.einsum('bhe,bhte->bht', q_rot, k_upd, preferred_element_type=jnp.float32)
    scores = jnp.where(valid_mask[:, None, :], scores, -1e30)
    attn_probs = jax.nn.softmax(scores, axis=-1).astype(jnp.bfloat16)
    attn_out = jnp.einsum('bht,bhte->bhe', attn_probs, v_upd, preferred_element_type=jnp.float32)
    return attn_out.astype(jnp.bfloat16), k_upd, v_upd


VM = pl.BlockSpec(memory_space=pltpu.VMEM)
VMEM_LIMIT = 60 * 1024 * 1024


def call(body, outs, scratch, sems, cid, flops, *args):
    single = len(outs) == 1
    return pl.pallas_call(
        body,
        out_shape=outs[0] if single else outs,
        in_specs=[VM] * len(args),
        out_specs=VM if single else [VM] * len(outs),
        scratch_shapes=scratch + [pltpu.SemaphoreType.DMA((sems,)), pltpu.SemaphoreType.DMA((sems,))],
        compiler_params=pltpu.CompilerParams(collective_id=cid, has_side_effects=True, vmem_limit_bytes=VMEM_LIMIT),
        cost_estimate=pl.CostEstimate(flops=flops, bytes_accessed=8_000_000, transcendentals=0),
    )(*args)


def call2(body, outs, scratch, sems, cid, flops, *args):
    single = len(outs) == 1
    return pl.pallas_call(
        body,
        out_shape=outs[0] if single else outs,
        in_specs=[VM] * len(args),
        out_specs=VM if single else [VM] * len(outs),
        scratch_shapes=scratch + [pltpu.SemaphoreType.DMA((sems,)), pltpu.SemaphoreType.DMA((sems,))],
        compiler_params=pltpu.CompilerParams(collective_id=cid, has_side_effects=True, vmem_limit_bytes=VMEM_LIMIT),
        cost_estimate=pl.CostEstimate(flops=flops, bytes_accessed=8_000_000, transcendentals=0),
    )(*args)


def call3(body, outs, scratch, sems, cid, flops, *args):
    single = len(outs) == 1
    return pl.pallas_call(
        body,
        out_shape=outs[0] if single else outs,
        in_specs=[VM] * len(args),
        out_specs=VM if single else [VM] * len(outs),
        scratch_shapes=scratch + [pltpu.SemaphoreType.DMA((sems,)), pltpu.SemaphoreType.DMA((sems,))],
        compiler_params=pltpu.CompilerParams(collective_id=cid, has_side_effects=True, vmem_limit_bytes=VMEM_LIMIT),
        cost_estimate=pl.CostEstimate(flops=flops, bytes_accessed=8_000_000, transcendentals=0),
    )(*args)


def solution(mesh):
    cache_spec = P(('dp', 'dm'), 'tp', None, None)
    resid_spec = P('dp', 'dm')
    col_spec = P('dm', 'tp')
    row_spec = P('tp', 'dm')
    in_specs = (resid_spec, cache_spec, cache_spec, P('dp'), P('dm'), col_spec, col_spec, col_spec, row_spec, P('dm'), col_spec, col_spec, row_spec)
    out_specs = (resid_spec, cache_spec, cache_spec)
    sds = jax.ShapeDtypeStruct
    V = pltpu.VMEM

    def local_step(resid_in, k_cache, v_cache, cache_len, norm_attn, w_q, w_k, w_v, w_o, norm_mlp, w_gate, w_up, w_down):
        lengths = lax.dynamic_slice_in_dim(cache_len, lax.axis_index('dm') * 192, 192)
        gains = jnp.concatenate([norm_attn.reshape(3, 128), norm_mlp.reshape(3, 128), jnp.zeros((2, 128), BF)]).astype(F32)
        q_sum, k_sum, v_sum, gain_all = call(
            qkv_kernel,
            (sds((192, 256), F32),) * 3 + (sds((8, 8, 128), F32),),
            [V((8, 3, 384, 256), BF), V((2, 4, 4, 48, 384), BF), V((8, 192, 384), BF)],
            40, 0, 2 * 10**9,
            resid_in, w_q, w_k, w_v, gains)
        heads = lambda a: a.reshape(192, 1, 256)
        q_rot = (rope_rotate(heads(q_sum), lengths) * 256 ** -0.5).astype(BF)
        k_new = rope_rotate(heads(k_sum), lengths).astype(BF)
        v_new = heads(v_sum).astype(BF)
        attn_out, k_upd, v_upd = attend(q_rot, k_cache, v_cache, k_new, v_new, lengths)
        rx = [V((2, 2, 2, 48, 384), F32), V((2, 2, 4, 48, 384), F32), V((2, 2, 24, 384), F32), V((2, 2, 48, 384), F32)]
        m_all, w_gu, h_own = call2(
            proj_kernel,
            (sds((2, 4, 4, 48, 1536), BF), sds((3072, 768), BF), sds((2, 48, 384), BF)),
            [V((4, 192, 256), BF), V((256, 384), BF), V((48, 384), BF), V((2, 4, 4, 48, 384), F32)] + rx + [V((4, 2, 48, 384), BF), V((384, 384), BF), V((384, 384), BF)],
            80, 1, 10**9,
            attn_out.reshape(192, 256), resid_in, w_o, w_gate, w_up, gain_all)
        resid_out = call3(
            mlp_kernel,
            (sds((1536, 384), BF),),
            [V((1536, 384), BF), V((2, 4, 4, 48, 384), F32)] + rx + [V((4, 192, 1536), BF), V((2, 4, 4, 48, 384), BF), V((4, 4, 48, 384), BF)],
            80, 2, 6 * 10**9,
            m_all, w_gu, h_own, w_down)
        return resid_out, k_upd, v_upd

    return jax.shard_map(local_step, mesh=mesh, in_specs=in_specs, out_specs=out_specs, check_vma=False)
```

```python
import math

import jax
import jax.numpy as jnp
from jax import lax
from jax.experimental import pallas as pl
from jax.experimental.pallas import tpu as pltpu
from jax.sharding import PartitionSpec as P

EPSILON = 1e-6
ROPE_THETA = 10000.0
BF = jnp.bfloat16
F32 = jnp.float32
LOGICAL = pl.DeviceIdType.LOGICAL


class Comm:
    def __init__(self, wait_buf, sems):
        self.wait_buf, self.sems = wait_buf, list(sems)
        self.groups = []
        tp, dm = lax.axis_index('tp'), lax.axis_index('dm')
        self.tp, self.dm = tp, dm
        self.z, self.y = lax.div(tp, 4), lax.rem(tp, 4)
        self.x, self.c = lax.div(dm, 2), lax.rem(dm, 2)
        self.other = tp * 8 + self.x * 2 + 1 - self.c
        self.rings = {}
        for axis, me, base, step in (('x', self.x, tp * 8 + self.c, 2), ('y', self.y, self.z * 32 + dm, 8), ('z', self.z, self.y * 8 + dm, 32)):
            idx = [me] + [lax.rem(me + k, 4) for k in (1, 2, 3)]
            self.rings[axis] = idx, base + idx[1] * step, base + idx[3] * step

    def neighbours(self):
        return [self.other] + [d for r in self.rings.values() for d in r[1:]]

    def barrier(self, peers):
        sem = pltpu.get_barrier_semaphore()
        for dev in peers:
            pl.semaphore_signal(sem, inc=1, device_id=dev, device_id_type=LOGICAL)
        pl.semaphore_wait(sem, len(peers))

    def send(self, src, dst, dev):
        rows = math.prod(dst.shape) * dst.dtype.itemsize // 256
        if not self.groups or self.groups[-1][1] + rows > self.wait_buf.shape[0]:
            self.groups.append([self.sems.pop(), 0])
        self.groups[-1][1] += rows
        recv = self.sems.pop()
        pltpu.make_async_remote_copy(src_ref=src, dst_ref=dst, send_sem=self.groups[-1][0], recv_sem=recv, device_id=dev, device_id_type=LOGICAL).start()
        return recv, rows

    def wait(self, *copies):
        for sem, rows in copies:
            part = self.wait_buf.at[0:rows]
            pltpu.make_async_copy(part, part, sem).wait()

    def local(self, src, dst):
        rows = math.prod(dst.shape) * dst.dtype.itemsize // 256
        sem = self.sems.pop()
        pltpu.make_async_copy(src, dst, sem).start()
        return sem, rows

    def drain(self):
        self.wait(*self.groups)


def run(*gens):
    gens = list(gens)
    while gens:
        for g in list(gens):
            try:
                next(g)
            except StopIteration:
                gens.remove(g)


def gather4(cm, axis, blk, hf, fine=True):
    (i, r, o, l), dr, dl = cm.rings[axis]
    if fine:
        a0 = cm.send(hf(i, 0), hf(i, 0), dr)
        b1 = cm.send(hf(i, 1), hf(i, 1), dl)
        a1 = cm.send(hf(i, 1), hf(i, 1), dr)
        b0 = cm.send(hf(i, 0), hf(i, 0), dl)
        late = (a1, b0)
    else:
        a0 = cm.send(blk(i), blk(i), dr)
        b1 = cm.send(blk(i), blk(i), dl)
        late = ()
    yield
    cm.wait(a0)
    c = cm.send(hf(l, 0), hf(l, 0), dr)
    cm.wait(b1)
    d = cm.send(hf(r, 1), hf(r, 1), dl)
    yield
    cm.wait(*late)
    yield
    cm.wait(c, d)


def scatter4(cm, axis, blk, hf, rx, hrx):
    (i, r, o, l), dr, dl = cm.rings[axis]
    ro0, ro1, rl, rr = rx
    c0 = cm.send(hf(o, 0), ro0, dr)
    c1 = cm.send(hf(o, 1), ro1, dl)
    c2 = cm.send(hf(r, 1), hrx(rl, 1), dr)
    c3 = cm.send(hf(l, 0), hrx(rr, 0), dl)
    yield
    cm.wait(c0)
    hf(r, 0)[...] += ro0[...]
    c4 = cm.send(hf(r, 0), hrx(rl, 0), dr)
    cm.wait(c1)
    hf(l, 1)[...] += ro1[...]
    c5 = cm.send(hf(l, 1), hrx(rr, 1), dl)
    yield
    cm.wait(c2, c3, c4, c5)
    blk(i)[...] += rl[...] + rr[...]


def rows48(j, start=0, size=48, align=8):
    return pl.ds(pl.multiple_of(j * 48 + start, align), size)


def plane_scatter(cm, p, h, rx):
    y = (lambda j: p.at[:, rows48(j)]), (lambda j, s: p.at[2 * s:2 * s + 2, rows48(j)]), rx[:4], (lambda b, s: b.at[2 * s:2 * s + 2])
    z = (lambda j: p.at[j]), (lambda j, s: p.at[j, 96 * s:96 * s + 96]), rx[:4], (lambda b, s: b.at[96 * s:96 * s + 96])
    ys = (lambda j: p.at[cm.z, rows48(j)]), (lambda j, s: p.at[cm.z, rows48(j, 24 * s, 24)]), rx[4:], (lambda b, s: b.at[24 * s:24 * s + 24])
    zs = (lambda j: p.at[j, rows48(cm.y)]), (lambda j, s: p.at[j, rows48(cm.y, 24 * s, 24)]), rx[4:], (lambda b, s: b.at[24 * s:24 * s + 24])
    if h == 0:
        yield from scatter4(cm, 'y', *y)
        yield from scatter4(cm, 'z', *zs)
    else:
        yield from scatter4(cm, 'z', *z)
        yield from scatter4(cm, 'y', *ys)


def scatter_scratch():
    V = pltpu.VMEM
    small = [V((24, 384), F32)] * 2 + [V((48, 384), F32)] * 2
    return [V((2, 48, 384), F32)] * 2 + [V((4, 48, 384), F32)] * 2 + small + [V((96, 384), F32)] * 2 + [V((192, 384), F32)] * 2 + small


def plane_gather(cm, m, h, split, near=None, fine=(False, True)):
    cols = m.shape[-1]
    cut = lambda s: pl.ds(0, split) if s == 0 else pl.ds(split, cols - split)
    at = lambda j: rows48(j, align=16)
    if h == 0:
        first, second = 'y', 'z'
        blk, hf = (lambda j: m.at[cm.z, at(j)]), (lambda j, s: m.at[cm.z, at(j), cut(s)])
        big, bigh = (lambda j: m.at[j]), (lambda j, s: m.at[j, 96 * s:96 * s + 96])
    else:
        first, second = 'z', 'y'
        blk, hf = (lambda j: m.at[j, at(cm.y)]), (lambda j, s: m.at[j, at(cm.y), cut(s)])
        big, bigh = (lambda j: m.at[:, at(j)]), (lambda j, s: m.at[2 * s:2 * s + 2, at(j)])
    yield from gather4(cm, first, blk, hf, fine[0])
    i, r, o, l = cm.rings[second][0]
    g = gather4(cm, second, big, bigh, fine[1])
    next(g)
    yield
    next(g)
    yield
    if near:
        near(i)
    yield
    next(g)
    if near:
        near(l)
        near(r)
    yield
    for _ in g:
        pass
    if near:
        near(o)


def gain_row(g_ref, d, k):
    g = g_ref[d]
    return jnp.concatenate([g[3 * k + j:3 * k + j + 1] for j in range(3)], axis=1)


def qkv_kernel(x_ref, wq_ref, wk_ref, wv_ref, ga_ref, gm_ref, q_ref, k_ref, v_ref, g_ref, w_buf, xg, n_buf, gain_buf, wait_buf, *sems):
    cm = Comm(wait_buf, sems)
    x, c, dm = cm.x, cm.c, cm.dm
    peers = [cm.tp * 8 + lax.rem(dm + k, 8) for k in range(1, 8)]
    cm.barrier(peers + [d for a in 'yz' for d in cm.rings[a][1:]])

    sl = jnp.where(c == 0, cm.y, cm.z)
    xs = []
    for k, dev in enumerate(peers):
        start = pl.multiple_of(lax.rem(dm + k + 1, 8) * 192 + sl * 48, 16)
        xs.append(cm.send(x_ref.at[pl.ds(start, 48), :], xg.at[c, sl, x], dev))
    gain_buf[0:3] = ga_ref[...].astype(F32)
    gain_buf[3:6] = gm_ref[...].astype(F32)
    gain_buf[6:8] = jnp.zeros((2, 128), F32)
    (i, r, o, l), dr, dl = cm.rings['x']
    dev_o = cm.other
    rows = lambda j: w_buf.at[j * 2 + c]
    ws = (wq_ref, wk_ref, wv_ref)
    lo, hi, full = pl.ds(0, 192), pl.ds(192, 192), pl.ds(0, 384)
    pieces = ((0, full), (1, lo), (1, hi), (2, full))
    a = [cm.send(ws[n].at[p], rows(i).at[n, p], dr) for n, p in pieces]
    b = [cm.send(ws[n].at[p], rows(i).at[n, p], dl) for n, p in pieces[::-1]]
    e = [cm.send(w, rows(i).at[n], dev_o) for n, w in enumerate(ws)]
    gs = [cm.send(gain_buf, g_ref.at[dm], dev) for dev in peers]
    mine = [cm.local(w, w_buf.at[dm, n]) for n, w in enumerate(ws)]
    own = pl.multiple_of(dm * 192 + sl * 48, 16)
    xs.append(cm.local(x_ref.at[pl.ds(own, 48), :], xg.at[c, sl, x]))
    g_ref[dm] = gain_buf[...]
    cm.wait(*xs)

    def on(cps, src, ps, dev):
        f = []
        for cp, (n, p) in zip(cps, ps):
            cm.wait(cp)
            f.append(cm.send(rows(src).at[n, p], rows(src).at[n, p], dev))
        return f

    gy = gather4(cm, 'y', lambda j: xg.at[0, j], lambda j, s: xg.at[0, j, 2 * s:2 * s + 2])
    gz = gather4(cm, 'z', lambda j: xg.at[1, j], lambda j, s: xg.at[1, j, 2 * s:2 * s + 2])
    for g in (gy, gz, gy, gz):
        next(g)
    f0 = on(a[:2], l, pieces[:2], dr)
    f1 = on(b[:2], r, pieces[::-1][:2], dl)
    run(gy, gz)
    cm.wait(*gs)
    total = jnp.zeros((192, 1), F32)
    for d in range(8):
        v = xg[d % 2, :, d // 2].reshape(192, 384).astype(F32)
        total += jnp.sum(v * v, axis=1, keepdims=True)
    inv = lax.rsqrt(total / 3072 + EPSILON)
    for d in range(8):
        v = xg[d % 2, :, d // 2].reshape(192, 384).astype(F32)
        n_buf[d] = (v * inv * (1.0 + gain_row(g_ref, d, 0))).astype(BF)
    outs = (q_ref, k_ref, v_ref)

    def add(j, first=False):
        for n, out in enumerate(outs):
            part = jnp.dot(n_buf[j * 2], w_buf[j * 2, n], preferred_element_type=F32) + jnp.dot(n_buf[j * 2 + 1], w_buf[j * 2 + 1, n], preferred_element_type=F32)
            out[...] = part if first else out[...] + part

    cm.wait(*e, *mine)
    add(i, True)
    cm.wait(*a[2:])
    e1 = cm.send(rows(l), rows(l), dev_o)
    cm.wait(*b[2:])
    e2 = cm.send(rows(r), rows(r), dev_o)
    cm.wait(e1)
    add(l)
    cm.wait(e2)
    add(r)
    cm.wait(*f0, *f1)
    cm.wait(cm.send(rows(o), rows(o), dev_o))
    add(o)
    cm.drain()


def post_kernel(o_ref, x_ref, wo_ref, wg_ref, wu_ref, wd_ref, g_ref, u_out, v_out, o_buf, wo, x_o, wd, pa, pb, pc, pd, hs, ma, mb, acc_a, acc_b, w_gu, ta, tb, tc, td, a_buf, u_buf, wait_buf, *rest):
    rx, rx2, sems = rest[:16], rest[16:32], rest[32:]
    cm = Comm(wait_buf, sems)
    x, c, y, z = cm.x, cm.c, cm.y, cm.z
    (i, r, o, l), dr, dl = cm.rings['x']
    dev_o = cm.other
    cm.barrier(cm.neighbours())

    o_buf[x] = o_ref[...]
    go = gather4(cm, 'x', lambda j: o_buf.at[j], lambda j, s: o_buf.at[j, 96 * s:96 * s + 96])
    next(go)
    row = lambda core: pl.multiple_of(192 * (2 * z + core) + 48 * y, 16)
    c_wo = cm.send(wo_ref, wo.at[c], dev_o)
    c_x = cm.send(x_ref.at[pl.ds(row(1 - c), 48), :], x_o, dev_o)
    c_wd = cm.send(wd_ref, wd.at[c], dev_o)
    wo[c] = wo_ref[...]
    own_wd = cm.local(wd_ref, wd.at[c])
    kblk = lambda j: pl.ds(pl.multiple_of((j * 2 + c) * 384, 16), 384)
    hcol = lambda j: pl.ds(pl.multiple_of(j * 384, 128), 384)

    def deal(w_ref, col, t0, t1):
        to = pl.ds(col, 384)
        half = lambda j, s: pl.ds(pl.multiple_of((j * 2 + c) * 384 + 192 * s, 16), 192)
        c_own = cm.send(w_ref.at[:, hcol(i)], w_gu.at[kblk(i), to], dev_o)
        c0 = cm.send(w_ref.at[0:192, hcol(o)], t0, dr)
        c1 = cm.send(w_ref.at[192:384, hcol(o)], t1, dl)
        c_r = cm.send(w_ref.at[:, hcol(r)], w_gu.at[kblk(i), to], dr)
        c_l = cm.send(w_ref.at[:, hcol(l)], w_gu.at[kblk(i), to], dl)
        own = cm.local(w_ref.at[:, hcol(i)], w_gu.at[kblk(i), to])
        yield
        yield
        cm.wait(c0)
        f0 = cm.send(t0, w_gu.at[half(l, 0), to], dr)
        cm.wait(c1)
        f1 = cm.send(t1, w_gu.at[half(r, 1), to], dl)
        yield
        yield
        cm.wait(c_r)
        e1 = cm.send(w_gu.at[kblk(l), to], w_gu.at[kblk(l), to], dev_o)
        cm.wait(c_l)
        e2 = cm.send(w_gu.at[kblk(r), to], w_gu.at[kblk(r), to], dev_o)
        cm.wait(f0, f1)
        e3 = cm.send(w_gu.at[kblk(o), to], w_gu.at[kblk(o), to], dev_o)
        yield
        cm.wait(c_own, own, e1, e2, e3)

    for _ in go:
        pass
    deal_g = deal(wg_ref, 0, ta, tb)
    next(deal_g)
    cm.wait(c_wo)

    def o_proj(j, carry):
        v = o_buf[j]
        pa[j] = jnp.dot(v, wo[0], preferred_element_type=F32)
        pb[j] = jnp.dot(v, wo[1], preferred_element_type=F32)
        return carry

    lax.fori_loop(0, 4, o_proj, 0)
    run(plane_scatter(cm, pa, 0, rx[:8]), plane_scatter(cm, pb, 1, rx[8:]), deal_g)

    cm.wait(c_x)
    mine, theirs = x_ref[pl.ds(row(c), 48), :].astype(F32), x_o[...].astype(F32)
    first = c == 0
    hs[x, 0] = (jnp.where(first, mine, theirs) + pa[z, rows48(y)]).astype(BF)
    hs[x, 1] = (jnp.where(first, theirs, mine) + pb[z, rows48(y)]).astype(BF)
    run(gather4(cm, 'x', lambda j: hs.at[j], lambda j, s: hs.at[j, s]))
    deal_u = deal(wu_ref, 384, tc, td)
    next(deal_u)
    total = jnp.zeros((48, 1), F32)
    for d in range(8):
        v = hs[d // 2, d % 2].astype(F32)
        total += jnp.sum(v * v, axis=1, keepdims=True)
    inv = lax.rsqrt(total / 3072 + EPSILON)
    for d in range(8):
        v = hs[d // 2, d % 2].astype(F32)
        (ma, mb)[d // 4][z, rows48(y, align=16), 384 * (d % 4):384 * (d % 4) + 384] = (v * inv * (1.0 + gain_row(g_ref, d, 1))).astype(BF)

    def part_a(j):
        acc_a[j] = jnp.dot(ma[j], w_gu[0:1536], preferred_element_type=F32)

    def part_b(j):
        acc_b[:, rows48(j)] = jnp.dot(mb[:, rows48(j, align=16)].reshape(192, 1536), w_gu[1536:3072], preferred_element_type=F32).reshape(4, 48, 768)

    run(plane_gather(cm, ma, 0, 768, part_a), plane_gather(cm, mb, 1, 768, part_b), deal_u)

    def hidden(j):
        s = acc_a[j] + acc_b[j]
        gate, up = s[:, 0:384], s[:, 384:768]
        gelu = 0.5 * gate * (1.0 + jnp.tanh(0.7978845608 * (gate + 0.044715 * (gate * gate * gate))))
        a_buf[j, :, hcol(x)] = (gelu * up).astype(BF)

    right, left = {}, {}
    for j in (0, 2, 1, 3):
        hidden(j)
        own = a_buf.at[j, :, hcol(x)]
        right[j] = cm.send(own, own, dr)
        left[j] = cm.send(own, own, dl)
    fwd = []
    for j in (0, 1):
        cm.wait(right[j])
        src = a_buf.at[j, :, hcol(l)]
        fwd.append(cm.send(src, src, dr))
        cm.wait(left[j + 2])
        src = a_buf.at[j + 2, :, hcol(r)]
        fwd.append(cm.send(src, src, dl))
    cm.wait(right[2], right[3], left[0], left[1], c_wd, own_wd)
    for j, k in ((0, 0), (2, 1), (1, 2), (3, 3)):
        cm.wait(fwd[k])
        v = a_buf[j]
        pc[j] = jnp.dot(v, wd[0], preferred_element_type=F32)
        pd[j] = jnp.dot(v, wd[1], preferred_element_type=F32)
    run(plane_scatter(cm, pc, 0, rx2[:8]), plane_scatter(cm, pd, 1, rx2[8:]))
    u_buf[0, z, rows48(y, align=16)] = (hs[x, 0].astype(F32) + pc[z, rows48(y)]).astype(BF)
    u_buf[1, z, rows48(y, align=16)] = (hs[x, 1].astype(F32) + pd[z, rows48(y)]).astype(BF)
    run(plane_gather(cm, u_buf.at[0], 0, 256, None, (False, False)), plane_gather(cm, u_buf.at[1], 1, 256, None, (False, False)))
    c_v = cm.send(u_buf.at[1 - c], v_out, dev_o)
    u_out[...] = u_buf[c]
    cm.wait(c_v)
    cm.drain()


def rope_rotate(vectors, positions):
    half_dim = vectors.shape[-1] // 2
    inv_freq = ROPE_THETA ** (-2.0 * jnp.arange(half_dim, dtype=jnp.float32) / vectors.shape[-1])
    angles = positions.astype(jnp.float32)[:, None] * inv_freq[None, :]
    cos_part = jnp.cos(angles)[:, None, :]
    sin_part = jnp.sin(angles)[:, None, :]
    first_half = vectors[..., :half_dim]
    second_half = vectors[..., half_dim:]
    return jnp.concatenate([first_half * cos_part - second_half * sin_part, second_half * cos_part + first_half * sin_part], axis=-1)


def attend(q_rot, k_cache, v_cache, k_new, v_new, lengths):
    slot_ids = jnp.arange(k_cache.shape[2])
    slot_hit = slot_ids[None, :] == lengths[:, None]
    valid_mask = slot_ids[None, :] <= lengths[:, None]
    k_upd = jnp.where(slot_hit[:, None, :, None], k_new[:, :, None, :], k_cache)
    v_upd = jnp.where(slot_hit[:, None, :, None], v_new[:, :, None, :], v_cache)
    scores = jnp.einsum('bhe,bhte->bht', q_rot, k_upd, preferred_element_type=jnp.float32)
    scores = jnp.where(valid_mask[:, None, :], scores, -1e30)
    attn_probs = jax.nn.softmax(scores, axis=-1).astype(jnp.bfloat16)
    attn_out = jnp.einsum('bht,bhte->bhe', attn_probs, v_upd, preferred_element_type=jnp.float32)
    return attn_out.astype(jnp.bfloat16), k_upd, v_upd


VM = pl.BlockSpec(memory_space=pltpu.VMEM)
VMEM_LIMIT = 60 * 1024 * 1024


ANY = pl.BlockSpec(memory_space=pl.ANY)


def call(body, outs, scratch, sems, cid, flops, where, *args):
    single = len(outs) == 1
    return pl.pallas_call(
        body,
        out_shape=outs[0] if single else outs,
        in_specs=[ANY if w == 'h' else VM for w in where],
        out_specs=VM if single else [VM] * len(outs),
        scratch_shapes=scratch + [pltpu.SemaphoreType.DMA] * sems,
        compiler_params=pltpu.CompilerParams(collective_id=cid, has_side_effects=True, vmem_limit_bytes=VMEM_LIMIT),
        cost_estimate=pl.CostEstimate(flops=flops, bytes_accessed=8_000_000, transcendentals=0),
    )(*args)


def call2(body, outs, scratch, sems, cid, flops, where, *args):
    single = len(outs) == 1
    return pl.pallas_call(
        body,
        out_shape=outs[0] if single else outs,
        in_specs=[ANY if w == 'h' else VM for w in where],
        out_specs=VM if single else [VM] * len(outs),
        scratch_shapes=scratch + [pltpu.SemaphoreType.DMA] * sems,
        compiler_params=pltpu.CompilerParams(collective_id=cid, has_side_effects=True, vmem_limit_bytes=VMEM_LIMIT),
        cost_estimate=pl.CostEstimate(flops=flops, bytes_accessed=8_000_000, transcendentals=0),
    )(*args)


def join_kernel(u_ref, v_ref, out_ref):
    c = lax.rem(lax.axis_index('dm'), 2)
    for j in range(4):
        out_ref[pl.ds(pl.multiple_of(192 * (2 * j + c), 16), 192), :] = u_ref[j]
        out_ref[pl.ds(pl.multiple_of(192 * (2 * j + 1 - c), 16), 192), :] = v_ref[j]


def solution(mesh):
    cache_spec = P(('dp', 'dm'), 'tp', None, None)
    resid_spec = P('dp', 'dm')
    col_spec = P('dm', 'tp')
    row_spec = P('tp', 'dm')
    in_specs = (resid_spec, cache_spec, cache_spec, P('dp'), P('dm'), col_spec, col_spec, col_spec, row_spec, P('dm'), col_spec, col_spec, row_spec)
    out_specs = (resid_spec, cache_spec, cache_spec)
    sds = jax.ShapeDtypeStruct
    V = pltpu.VMEM

    def local_step(resid_in, k_cache, v_cache, cache_len, norm_attn, w_q, w_k, w_v, w_o, norm_mlp, w_gate, w_up, w_down):
        lengths = lax.dynamic_slice_in_dim(cache_len, lax.axis_index('dm') * 192, 192)
        q_sum, k_sum, v_sum, gain_all = call(
            qkv_kernel,
            (sds((192, 256), F32),) * 3 + (sds((8, 8, 128), F32),),
            [V((8, 3, 384, 256), BF), V((2, 4, 4, 48, 384), BF), V((8, 192, 384), BF), V((8, 128), F32), V((8192, 128), BF)],
            60, 0, 2 * 10**9, 'hhhhvv',
            resid_in, w_q, w_k, w_v, norm_attn.reshape(3, 128), norm_mlp.reshape(3, 128))
        heads = lambda a: a.reshape(192, 1, 256)
        q_rot = (rope_rotate(heads(q_sum), lengths) * 256 ** -0.5).astype(BF)
        k_new = rope_rotate(heads(k_sum), lengths).astype(BF)
        v_new = heads(v_sum).astype(BF)
        attn_out, k_upd, v_upd = attend(q_rot, k_cache, v_cache, k_new, v_new, lengths)
        mine, theirs = call2(
            post_kernel,
            (sds((4, 192, 384), BF), sds((4, 192, 384), BF)),
            [V((4, 192, 256), BF), V((2, 256, 384), BF), V((48, 384), BF), V((2, 1536, 384), BF)]
            + [V((4, 192, 384), F32)] * 4 + [V((4, 2, 48, 384), BF)] + [V((4, 192, 1536), BF)] * 2 + [V((4, 192, 768), F32)] * 2
            + [V((3072, 768), BF)] + [V((192, 384), BF)] * 4 + [V((4, 192, 1536), BF), V((2, 4, 192, 384), BF), V((16384, 128), BF)]
            + scatter_scratch() + scatter_scratch(),
            170, 1, 7 * 10**9, 'vvvhhhv',
            attn_out.reshape(192, 256), resid_in, w_o, w_gate, w_up, w_down, gain_all)
        resid_out = pl.pallas_call(join_kernel, out_shape=sds((1536, 384), BF), in_specs=[VM, VM], out_specs=VM)(mine, theirs)
        return resid_out, k_upd, v_upd

    return jax.shard_map(local_step, mesh=mesh, in_specs=in_specs, out_specs=out_specs, check_vma=False)
```

```python
import math

import jax
import jax.numpy as jnp
from jax import lax
from jax.experimental import pallas as pl
from jax.experimental.pallas import tpu as pltpu
from jax.sharding import PartitionSpec as P

EPSILON = 1e-6
ROPE_THETA = 10000.0
BF = jnp.bfloat16
F32 = jnp.float32
LOGICAL = pl.DeviceIdType.LOGICAL


class Comm:
    def __init__(self, wait_buf, sems):
        self.wait_buf, self.sems = wait_buf, list(sems)
        self.groups = []
        tp, dm = lax.axis_index('tp'), lax.axis_index('dm')
        self.tp, self.dm = tp, dm
        self.z, self.y = lax.div(tp, 4), lax.rem(tp, 4)
        self.x, self.c = lax.div(dm, 2), lax.rem(dm, 2)
        self.other = tp * 8 + self.x * 2 + 1 - self.c
        self.rings, self.opposite = {}, {}
        for axis, me, base, step in (('x', self.x, tp * 8 + self.c, 2), ('y', self.y, self.z * 32 + dm, 8), ('z', self.z, self.y * 8 + dm, 32)):
            idx = [me] + [lax.rem(me + k, 4) for k in (1, 2, 3)]
            self.rings[axis] = idx, base + idx[1] * step, base + idx[3] * step
            self.opposite[axis] = base + idx[2] * step

    def neighbours(self):
        return [self.other] + [d for r in self.rings.values() for d in r[1:]] + list(self.opposite.values())

    def barrier(self, peers):
        sem = pltpu.get_barrier_semaphore()
        for dev in peers:
            pl.semaphore_signal(sem, inc=1, device_id=dev, device_id_type=LOGICAL)
        pl.semaphore_wait(sem, len(peers))

    def send(self, src, dst, dev):
        rows = math.prod(dst.shape) * dst.dtype.itemsize // 256
        if not self.groups or self.groups[-1][1] + rows > self.wait_buf.shape[0]:
            self.groups.append([self.sems.pop(), 0])
        self.groups[-1][1] += rows
        recv = self.sems.pop()
        pltpu.make_async_remote_copy(src_ref=src, dst_ref=dst, send_sem=self.groups[-1][0], recv_sem=recv, device_id=dev, device_id_type=LOGICAL).start()
        return recv, rows

    def wait(self, *copies):
        for sem, rows in copies:
            part = self.wait_buf.at[0:rows]
            pltpu.make_async_copy(part, part, sem).wait()

    def local(self, src, dst):
        rows = math.prod(dst.shape) * dst.dtype.itemsize // 256
        sem = self.sems.pop()
        pltpu.make_async_copy(src, dst, sem).start()
        return sem, rows

    def drain(self):
        self.wait(*self.groups)


def run(*gens):
    gens = list(gens)
    while gens:
        for g in list(gens):
            try:
                next(g)
            except StopIteration:
                gens.remove(g)


def gather4(cm, axis, blk, hf, fine=True):
    (i, r, o, l), dr, dl = cm.rings[axis]
    if fine:
        a0 = cm.send(hf(i, 0), hf(i, 0), dr)
        b1 = cm.send(hf(i, 1), hf(i, 1), dl)
        a1 = cm.send(hf(i, 1), hf(i, 1), dr)
        b0 = cm.send(hf(i, 0), hf(i, 0), dl)
        late = (a1, b0)
    else:
        a0 = cm.send(blk(i), blk(i), dr)
        b1 = cm.send(blk(i), blk(i), dl)
        late = ()
    yield
    cm.wait(a0)
    c = cm.send(hf(l, 0), hf(l, 0), dr)
    cm.wait(b1)
    d = cm.send(hf(r, 1), hf(r, 1), dl)
    yield
    cm.wait(*late)
    yield
    cm.wait(c, d)


def direct4(cm, axis, src, dst):
    (i, r, o, l), dr, dl = cm.rings[axis]
    return [cm.send(src(o), dst(1), cm.opposite[axis]), cm.send(src(r), dst(0), dr), cm.send(src(l), dst(2), dl)]


def direct_gather(cm, axis, blk):
    own = blk(cm.rings[axis][0][0])
    cps = direct4(cm, axis, lambda j: own, lambda k: own)
    yield
    cm.wait(*cps)


def direct_scatter(cm, axis, blk, rx):
    cps = direct4(cm, axis, blk, lambda k: rx[k])
    yield
    cm.wait(*cps)
    blk(cm.rings[axis][0][0])[...] += (rx[0][...] + rx[2][...]) + rx[1][...]


def scatter4(cm, axis, blk, hf, rx, hrx):
    (i, r, o, l), dr, dl = cm.rings[axis]
    ro0, ro1, rl, rr = rx
    c0 = cm.send(hf(o, 0), ro0, dr)
    c1 = cm.send(hf(o, 1), ro1, dl)
    c2 = cm.send(hf(r, 1), hrx(rl, 1), dr)
    c3 = cm.send(hf(l, 0), hrx(rr, 0), dl)
    yield
    cm.wait(c0)
    hf(r, 0)[...] += ro0[...]
    c4 = cm.send(hf(r, 0), hrx(rl, 0), dr)
    cm.wait(c1)
    hf(l, 1)[...] += ro1[...]
    c5 = cm.send(hf(l, 1), hrx(rr, 1), dl)
    yield
    cm.wait(c2, c3, c4, c5)
    blk(i)[...] += rl[...] + rr[...]


def rows48(j, start=0, size=48, align=8):
    return pl.ds(pl.multiple_of(j * 48 + start, align), size)


def plane_scatter(cm, p, h, rx):
    y = (lambda j: p.at[:, rows48(j)]), (lambda j, s: p.at[2 * s:2 * s + 2, rows48(j)]), rx[:4], (lambda b, s: b.at[2 * s:2 * s + 2])
    z = (lambda j: p.at[j]), (lambda j, s: p.at[j, 96 * s:96 * s + 96]), rx[:4], (lambda b, s: b.at[96 * s:96 * s + 96])
    if h == 0:
        yield from scatter4(cm, 'y', *y)
        yield from direct_scatter(cm, 'z', lambda j: p.at[j, rows48(cm.y)], rx[4:])
    else:
        yield from scatter4(cm, 'z', *z)
        yield from direct_scatter(cm, 'y', lambda j: p.at[cm.z, rows48(j)], rx[4:])


def scatter_scratch():
    V = pltpu.VMEM
    small = [V((48, 384), F32)] * 3
    return [V((2, 48, 384), F32)] * 2 + [V((4, 48, 384), F32)] * 2 + small + [V((96, 384), F32)] * 2 + [V((192, 384), F32)] * 2 + small


def plane_gather(cm, m, h, near=None):
    at = lambda j: rows48(j, align=16)
    if h == 0:
        second = 'z'
        yield from direct_gather(cm, 'y', lambda j: m.at[cm.z, at(j)])
        big, bigh = (lambda j: m.at[j]), (lambda j, s: m.at[j, 96 * s:96 * s + 96])
    else:
        second = 'y'
        yield from direct_gather(cm, 'z', lambda j: m.at[j, at(cm.y)])
        big, bigh = (lambda j: m.at[:, at(j)]), (lambda j, s: m.at[2 * s:2 * s + 2, at(j)])
    if near is None:
        yield from direct_gather(cm, second, big)
        return
    i, r, o, l = cm.rings[second][0]
    g = gather4(cm, second, big, bigh)
    next(g)
    yield
    next(g)
    yield
    near(i)
    yield
    next(g)
    near(l)
    near(r)
    yield
    for _ in g:
        pass
    near(o)


def gain_row(g_ref, d, k):
    g = g_ref[d]
    return jnp.concatenate([g[3 * k + j:3 * k + j + 1] for j in range(3)], axis=1)


def qkv_kernel(x_ref, wq_ref, wk_ref, wv_ref, ga_ref, gm_ref, q_ref, k_ref, v_ref, g_ref, w_buf, xg, n_buf, gain_buf, wait_buf, *sems):
    cm = Comm(wait_buf, sems)
    x, c, dm = cm.x, cm.c, cm.dm
    peers = [cm.tp * 8 + lax.rem(dm + k, 8) for k in range(1, 8)]
    cm.barrier(peers + [d for a in 'yz' for d in cm.rings[a][1:] + (cm.opposite[a],)])

    first = jnp.where(c == 0, cm.y, cm.z)
    second = jnp.where(c == 0, cm.z, cm.y)
    start = first * 48 + jnp.minimum(second, 2) * 16
    piece = lambda d: x_ref.at[pl.ds(pl.multiple_of(d * 192 + start, 16), 16), :]
    xs = [cm.send(piece(lax.rem(dm + k + 1, 8)), xg.at[c, first, second, x], dev) for k, dev in enumerate(peers)]
    gain_buf[0:3] = ga_ref[...].astype(F32)
    gain_buf[3:6] = gm_ref[...].astype(F32)
    gain_buf[6:8] = jnp.zeros((2, 128), F32)
    (i, r, o, l), dr, dl = cm.rings['x']
    dev_o = cm.other
    rows = lambda j: w_buf.at[j * 2 + c]
    ws = (wq_ref, wk_ref, wv_ref)
    lo, hi, full = pl.ds(0, 192), pl.ds(192, 192), pl.ds(0, 384)
    pieces = ((0, full), (1, lo), (1, hi), (2, full))
    a = [cm.send(ws[n].at[p], rows(i).at[n, p], dr) for n, p in pieces]
    b = [cm.send(ws[n].at[p], rows(i).at[n, p], dl) for n, p in pieces[::-1]]
    e = [cm.send(w, rows(i).at[n], dev_o) for n, w in enumerate(ws)]
    gs = [cm.send(gain_buf, g_ref.at[dm], dev) for dev in peers]
    mine = [cm.local(w, w_buf.at[dm, n]) for n, w in enumerate(ws)]
    xs.append(cm.local(piece(dm), xg.at[c, first, second, x]))
    g_ref[dm] = gain_buf[...]
    cm.wait(*xs)

    def on(cps, src, ps, dev):
        f = []
        for cp, (n, p) in zip(cps, ps):
            cm.wait(cp)
            f.append(cm.send(rows(src).at[n, p], rows(src).at[n, p], dev))
        return f

    def rows_gather(k, small, big, where):
        yield from direct_gather(cm, small, where)
        yield from gather4(cm, big, lambda j: xg.at[k, j], lambda j, s: xg.at[k, j, :, 2 * s:2 * s + 2])

    gy = rows_gather(0, 'z', 'y', lambda j: xg.at[0, cm.y, j])
    gz = rows_gather(1, 'y', 'z', lambda j: xg.at[1, cm.z, j])
    for g in (gy, gz, gy, gz):
        next(g)
    f0 = on(a[:2], l, pieces[:2], dr)
    f1 = on(b[:2], r, pieces[::-1][:2], dl)
    run(gy, gz)
    cm.wait(*gs)
    total = jnp.zeros((192, 1), F32)
    for d in range(8):
        v = xg[d % 2, :, 0:3, d // 2].reshape(192, 384).astype(F32)
        total += jnp.sum(v * v, axis=1, keepdims=True)
    inv = lax.rsqrt(total / 3072 + EPSILON)
    for d in range(8):
        v = xg[d % 2, :, 0:3, d // 2].reshape(192, 384).astype(F32)
        n_buf[d] = (v * inv * (1.0 + gain_row(g_ref, d, 0))).astype(BF)
    outs = (q_ref, k_ref, v_ref)

    def add(j, first=False):
        for n, out in enumerate(outs):
            part = jnp.dot(n_buf[j * 2], w_buf[j * 2, n], preferred_element_type=F32) + jnp.dot(n_buf[j * 2 + 1], w_buf[j * 2 + 1, n], preferred_element_type=F32)
            out[...] = part if first else out[...] + part

    cm.wait(*e, *mine)
    add(i, True)
    cm.wait(*a[2:])
    e1 = cm.send(rows(l), rows(l), dev_o)
    cm.wait(*b[2:])
    e2 = cm.send(rows(r), rows(r), dev_o)
    cm.wait(e1)
    add(l)
    cm.wait(e2)
    add(r)
    cm.wait(*f0, *f1)
    cm.wait(cm.send(rows(o), rows(o), dev_o))
    add(o)
    cm.drain()


def post_kernel(o_ref, x_ref, wo_ref, wg_ref, wu_ref, wd_ref, g_ref, u_out, v_out, o_buf, wo, x_o, wd, pa, pb, pc, pd, hs, ma, mb, acc_a, acc_b, w_gu, a_buf, u_buf, wait_buf, *rest):
    rx, rx2, sems = rest[:14], rest[14:28], rest[28:]
    cm = Comm(wait_buf, sems)
    x, c, y, z = cm.x, cm.c, cm.y, cm.z
    (i, r, o, l), dr, dl = cm.rings['x']
    dev_o = cm.other
    cm.barrier(cm.neighbours())

    o_buf[x] = o_ref[...]
    go = direct_gather(cm, 'x', lambda j: o_buf.at[j])
    next(go)
    row = lambda core: pl.multiple_of(192 * (2 * z + core) + 48 * y, 16)
    c_wo = cm.send(wo_ref, wo.at[c], dev_o)
    c_x = cm.send(x_ref.at[pl.ds(row(1 - c), 48), :], x_o, dev_o)
    c_wd = cm.send(wd_ref, wd.at[c], dev_o)
    wo[c] = wo_ref[...]
    own_wd = cm.local(wd_ref, wd.at[c])
    kblk = lambda j: pl.ds(pl.multiple_of((j * 2 + c) * 384, 16), 384)
    hcol = lambda j: pl.ds(pl.multiple_of(j * 384, 128), 384)

    def deal(w_ref, col):
        to = pl.ds(col, 384)
        own = w_gu.at[kblk(i), to]
        cps = direct4(cm, 'x', lambda j: w_ref.at[:, hcol(j)], lambda k: own)
        here = [cm.local(w_ref.at[:, hcol(i)], own), cm.send(w_ref.at[:, hcol(i)], own, dev_o)]
        for _ in range(3):
            yield
        for cp, j in zip(cps[1:] + cps[:1], (l, r, o)):
            cm.wait(cp)
            here.append(cm.send(w_gu.at[kblk(j), to], w_gu.at[kblk(j), to], dev_o))
        yield
        cm.wait(*here)

    for _ in go:
        pass
    deal_g = deal(wg_ref, 0)
    next(deal_g)
    cm.wait(c_wo)

    def o_proj(j, carry):
        v = o_buf[j]
        pa[j] = jnp.dot(v, wo[0], preferred_element_type=F32)
        pb[j] = jnp.dot(v, wo[1], preferred_element_type=F32)
        return carry

    lax.fori_loop(0, 4, o_proj, 0)
    run(plane_scatter(cm, pa, 0, rx[:7]), plane_scatter(cm, pb, 1, rx[7:]), deal_g)

    cm.wait(c_x)
    mine, theirs = x_ref[pl.ds(row(c), 48), :].astype(F32), x_o[...].astype(F32)
    first = c == 0
    hs[x, 0] = (jnp.where(first, mine, theirs) + pa[z, rows48(y)]).astype(BF)
    hs[x, 1] = (jnp.where(first, theirs, mine) + pb[z, rows48(y)]).astype(BF)
    run(direct_gather(cm, 'x', lambda j: hs.at[j]))
    deal_u = deal(wu_ref, 384)
    next(deal_u)
    total = jnp.zeros((48, 1), F32)
    for d in range(8):
        v = hs[d // 2, d % 2].astype(F32)
        total += jnp.sum(v * v, axis=1, keepdims=True)
    inv = lax.rsqrt(total / 3072 + EPSILON)
    for d in range(8):
        v = hs[d // 2, d % 2].astype(F32)
        (ma, mb)[d // 4][z, rows48(y, align=16), 384 * (d % 4):384 * (d % 4) + 384] = (v * inv * (1.0 + gain_row(g_ref, d, 1))).astype(BF)

    def part_a(j):
        acc_a[j] = jnp.dot(ma[j], w_gu[0:1536], preferred_element_type=F32)

    def part_b(j):
        acc_b[:, rows48(j)] = jnp.dot(mb[:, rows48(j, align=16)].reshape(192, 1536), w_gu[1536:3072], preferred_element_type=F32).reshape(4, 48, 768)

    run(deal_u, plane_gather(cm, ma, 0, part_a), plane_gather(cm, mb, 1, part_b))

    def hidden(j):
        s = acc_a[j] + acc_b[j]
        gate, up = s[:, 0:384], s[:, 384:768]
        gelu = 0.5 * gate * (1.0 + jnp.tanh(0.7978845608 * (gate + 0.044715 * (gate * gate * gate))))
        a_buf[j, :, hcol(x)] = (gelu * up).astype(BF)

    right, left = {}, {}
    for j in (0, 2, 1, 3):
        hidden(j)
        own = a_buf.at[j, :, hcol(x)]
        right[j] = cm.send(own, own, dr)
        left[j] = cm.send(own, own, dl)
    fwd = []
    for j in (0, 1):
        cm.wait(right[j])
        src = a_buf.at[j, :, hcol(l)]
        fwd.append(cm.send(src, src, dr))
        cm.wait(left[j + 2])
        src = a_buf.at[j + 2, :, hcol(r)]
        fwd.append(cm.send(src, src, dl))
    cm.wait(right[2], right[3], left[0], left[1], c_wd, own_wd)
    for j, k in ((0, 0), (2, 1), (1, 2), (3, 3)):
        cm.wait(fwd[k])
        v = a_buf[j]
        pc[j] = jnp.dot(v, wd[0], preferred_element_type=F32)
        pd[j] = jnp.dot(v, wd[1], preferred_element_type=F32)
    run(plane_scatter(cm, pc, 0, rx2[:7]), plane_scatter(cm, pd, 1, rx2[7:]))
    u_buf[0, z, rows48(y, align=16)] = (hs[x, 0].astype(F32) + pc[z, rows48(y)]).astype(BF)
    u_buf[1, z, rows48(y, align=16)] = (hs[x, 1].astype(F32) + pd[z, rows48(y)]).astype(BF)
    run(plane_gather(cm, u_buf.at[0], 0), plane_gather(cm, u_buf.at[1], 1))
    c_v = cm.send(u_buf.at[1 - c], v_out, dev_o)
    u_out[...] = u_buf[c]
    cm.wait(c_v)
    cm.drain()


def rope_rotate(vectors, positions):
    half_dim = vectors.shape[-1] // 2
    inv_freq = ROPE_THETA ** (-2.0 * jnp.arange(half_dim, dtype=jnp.float32) / vectors.shape[-1])
    angles = positions.astype(jnp.float32)[:, None] * inv_freq[None, :]
    cos_part = jnp.cos(angles)[:, None, :]
    sin_part = jnp.sin(angles)[:, None, :]
    first_half = vectors[..., :half_dim]
    second_half = vectors[..., half_dim:]
    return jnp.concatenate([first_half * cos_part - second_half * sin_part, second_half * cos_part + first_half * sin_part], axis=-1)


def attend(q_rot, k_cache, v_cache, k_new, v_new, lengths):
    slot_ids = jnp.arange(k_cache.shape[2])
    slot_hit = slot_ids[None, :] == lengths[:, None]
    valid_mask = slot_ids[None, :] <= lengths[:, None]
    k_upd = jnp.where(slot_hit[:, None, :, None], k_new[:, :, None, :], k_cache)
    v_upd = jnp.where(slot_hit[:, None, :, None], v_new[:, :, None, :], v_cache)
    scores = jnp.einsum('bhe,bhte->bht', q_rot, k_upd, preferred_element_type=jnp.float32)
    scores = jnp.where(valid_mask[:, None, :], scores, -1e30)
    attn_probs = jax.nn.softmax(scores, axis=-1).astype(jnp.bfloat16)
    attn_out = jnp.einsum('bht,bhte->bhe', attn_probs, v_upd, preferred_element_type=jnp.float32)
    return attn_out.astype(jnp.bfloat16), k_upd, v_upd


VM = pl.BlockSpec(memory_space=pltpu.VMEM)
VMEM_LIMIT = 60 * 1024 * 1024


ANY = pl.BlockSpec(memory_space=pl.ANY)


def call(body, outs, scratch, sems, cid, flops, where, *args):
    single = len(outs) == 1
    return pl.pallas_call(
        body,
        out_shape=outs[0] if single else outs,
        in_specs=[ANY if w == 'h' else VM for w in where],
        out_specs=VM if single else [VM] * len(outs),
        scratch_shapes=scratch + [pltpu.SemaphoreType.DMA] * sems,
        compiler_params=pltpu.CompilerParams(collective_id=cid, has_side_effects=True, vmem_limit_bytes=VMEM_LIMIT),
        cost_estimate=pl.CostEstimate(flops=flops, bytes_accessed=8_000_000, transcendentals=0),
    )(*args)


def call2(body, outs, scratch, sems, cid, flops, where, *args):
    single = len(outs) == 1
    return pl.pallas_call(
        body,
        out_shape=outs[0] if single else outs,
        in_specs=[ANY if w == 'h' else VM for w in where],
        out_specs=VM if single else [VM] * len(outs),
        scratch_shapes=scratch + [pltpu.SemaphoreType.DMA] * sems,
        compiler_params=pltpu.CompilerParams(collective_id=cid, has_side_effects=True, vmem_limit_bytes=VMEM_LIMIT),
        cost_estimate=pl.CostEstimate(flops=flops, bytes_accessed=8_000_000, transcendentals=0),
    )(*args)


def join_kernel(u_ref, v_ref, out_ref):
    c = lax.rem(lax.axis_index('dm'), 2)
    for j in range(4):
        out_ref[pl.ds(pl.multiple_of(192 * (2 * j + c), 16), 192), :] = u_ref[j]
        out_ref[pl.ds(pl.multiple_of(192 * (2 * j + 1 - c), 16), 192), :] = v_ref[j]


def solution(mesh):
    cache_spec = P(('dp', 'dm'), 'tp', None, None)
    resid_spec = P('dp', 'dm')
    col_spec = P('dm', 'tp')
    row_spec = P('tp', 'dm')
    in_specs = (resid_spec, cache_spec, cache_spec, P('dp'), P('dm'), col_spec, col_spec, col_spec, row_spec, P('dm'), col_spec, col_spec, row_spec)
    out_specs = (resid_spec, cache_spec, cache_spec)
    sds = jax.ShapeDtypeStruct
    V = pltpu.VMEM

    def local_step(resid_in, k_cache, v_cache, cache_len, norm_attn, w_q, w_k, w_v, w_o, norm_mlp, w_gate, w_up, w_down):
        lengths = lax.dynamic_slice_in_dim(cache_len, lax.axis_index('dm') * 192, 192)
        q_sum, k_sum, v_sum, gain_all = call(
            qkv_kernel,
            (sds((192, 256), F32),) * 3 + (sds((8, 8, 128), F32),),
            [V((8, 3, 384, 256), BF), V((2, 4, 4, 4, 16, 384), BF), V((8, 192, 384), BF), V((8, 128), F32), V((8192, 128), BF)],
            60, 0, 2 * 10**9, 'hhhhvv',
            resid_in, w_q, w_k, w_v, norm_attn.reshape(3, 128), norm_mlp.reshape(3, 128))
        heads = lambda a: a.reshape(192, 1, 256)
        q_rot = (rope_rotate(heads(q_sum), lengths) * 256 ** -0.5).astype(BF)
        k_new = rope_rotate(heads(k_sum), lengths).astype(BF)
        v_new = heads(v_sum).astype(BF)
        attn_out, k_upd, v_upd = attend(q_rot, k_cache, v_cache, k_new, v_new, lengths)
        mine, theirs = call2(
            post_kernel,
            (sds((4, 192, 384), BF), sds((4, 192, 384), BF)),
            [V((4, 192, 256), BF), V((2, 256, 384), BF), V((48, 384), BF), V((2, 1536, 384), BF)]
            + [V((4, 192, 384), F32)] * 4 + [V((4, 2, 48, 384), BF)] + [V((4, 192, 1536), BF)] * 2 + [V((4, 192, 768), F32)] * 2
            + [V((3072, 768), BF), V((4, 192, 1536), BF), V((2, 4, 192, 384), BF), V((16384, 128), BF)]
            + scatter_scratch() + scatter_scratch(),
            170, 1, 7 * 10**9, 'vvvhhhv',
            attn_out.reshape(192, 256), resid_in, w_o, w_gate, w_up, w_down, gain_all)
        resid_out = pl.pallas_call(join_kernel, out_shape=sds((1536, 384), BF), in_specs=[VM, VM], out_specs=VM)(mine, theirs)
        return resid_out, k_upd, v_upd

    return jax.shard_map(local_step, mesh=mesh, in_specs=in_specs, out_specs=out_specs, check_vma=False)
```

```python
import math

import jax
import jax.numpy as jnp
import numpy as np
from jax import lax
from jax.experimental import pallas as pl
from jax.experimental.pallas import tpu as pltpu
from jax.sharding import PartitionSpec as P

EPSILON = 1e-6
ROPE_THETA = 10000.0
BF = jnp.bfloat16
F32 = jnp.float32
LOGICAL = pl.DeviceIdType.LOGICAL


class Comm:
    def __init__(self, wait_buf, sems):
        self.wait_buf, self.sems = wait_buf, list(sems)
        self.groups = []
        tp, dm = lax.axis_index('tp'), lax.axis_index('dm')
        self.tp, self.dm = tp, dm
        self.z, self.y = lax.div(tp, 4), lax.rem(tp, 4)
        self.x, self.c = lax.div(dm, 2), lax.rem(dm, 2)
        self.other = tp * 8 + self.x * 2 + 1 - self.c
        self.rings, self.opposite = {}, {}
        for axis, me, base, step in (('x', self.x, tp * 8 + self.c, 2), ('y', self.y, self.z * 32 + dm, 8), ('z', self.z, self.y * 8 + dm, 32)):
            idx = [me] + [lax.rem(me + k, 4) for k in (1, 2, 3)]
            self.rings[axis] = idx, base + idx[1] * step, base + idx[3] * step
            self.opposite[axis] = base + idx[2] * step

    def neighbours(self):
        return [self.other] + [d for r in self.rings.values() for d in r[1:]] + list(self.opposite.values())

    def barrier(self, peers):
        sem = pltpu.get_barrier_semaphore()
        for dev in peers:
            pl.semaphore_signal(sem, inc=1, device_id=dev, device_id_type=LOGICAL)
        pl.semaphore_wait(sem, len(peers))

    def send(self, src, dst, dev):
        rows = math.prod(dst.shape) * dst.dtype.itemsize // 256
        if not self.groups or self.groups[-1][1] + rows > self.wait_buf.shape[0]:
            self.groups.append([self.sems.pop(), 0])
        self.groups[-1][1] += rows
        recv = self.sems.pop()
        pltpu.make_async_remote_copy(src_ref=src, dst_ref=dst, send_sem=self.groups[-1][0], recv_sem=recv, device_id=dev, device_id_type=LOGICAL).start()
        return recv, rows

    def wait(self, *copies):
        for sem, rows in copies:
            part = self.wait_buf.at[0:rows]
            pltpu.make_async_copy(part, part, sem).wait()

    def local(self, src, dst):
        rows = math.prod(dst.shape) * dst.dtype.itemsize // 256
        sem = self.sems.pop()
        pltpu.make_async_copy(src, dst, sem).start()
        return sem, rows

    def drain(self):
        self.wait(*self.groups)


def run(*gens):
    gens = list(gens)
    while gens:
        for g in list(gens):
            try:
                next(g)
            except StopIteration:
                gens.remove(g)


def gather4(cm, axis, blk, hf, fine=True):
    (i, r, o, l), dr, dl = cm.rings[axis]
    if fine:
        a0 = cm.send(hf(i, 0), hf(i, 0), dr)
        b1 = cm.send(hf(i, 1), hf(i, 1), dl)
        a1 = cm.send(hf(i, 1), hf(i, 1), dr)
        b0 = cm.send(hf(i, 0), hf(i, 0), dl)
        late = (a1, b0)
    else:
        a0 = cm.send(blk(i), blk(i), dr)
        b1 = cm.send(blk(i), blk(i), dl)
        late = ()
    yield
    cm.wait(a0)
    c = cm.send(hf(l, 0), hf(l, 0), dr)
    cm.wait(b1)
    d = cm.send(hf(r, 1), hf(r, 1), dl)
    yield
    cm.wait(*late)
    yield
    cm.wait(c, d)


def direct4(cm, axis, src, dst):
    (i, r, o, l), dr, dl = cm.rings[axis]
    return [cm.send(src(o), dst(1), cm.opposite[axis]), cm.send(src(r), dst(0), dr), cm.send(src(l), dst(2), dl)]


def direct_gather(cm, axis, blk):
    own = blk(cm.rings[axis][0][0])
    cps = direct4(cm, axis, lambda j: own, lambda k: own)
    yield
    cm.wait(*cps)


def direct_scatter(cm, axis, blk, rx):
    cps = direct4(cm, axis, blk, lambda k: rx[k])
    yield
    cm.wait(*cps)
    blk(cm.rings[axis][0][0])[...] += (rx[0][...] + rx[2][...]) + rx[1][...]


def scatter4(cm, axis, blk, hf, rx, hrx):
    (i, r, o, l), dr, dl = cm.rings[axis]
    ro0, ro1, rl, rr = rx
    c0 = cm.send(hf(o, 0), ro0, dr)
    c1 = cm.send(hf(o, 1), ro1, dl)
    c2 = cm.send(hf(r, 1), hrx(rl, 1), dr)
    c3 = cm.send(hf(l, 0), hrx(rr, 0), dl)
    yield
    cm.wait(c0)
    hf(r, 0)[...] += ro0[...]
    c4 = cm.send(hf(r, 0), hrx(rl, 0), dr)
    cm.wait(c1)
    hf(l, 1)[...] += ro1[...]
    c5 = cm.send(hf(l, 1), hrx(rr, 1), dl)
    yield
    cm.wait(c2, c3, c4, c5)
    blk(i)[...] += rl[...] + rr[...]


def rows48(j, start=0, size=48, align=8):
    return pl.ds(pl.multiple_of(j * 48 + start, align), size)


def plane_scatter(cm, p, h, rx):
    y = (lambda j: p.at[:, rows48(j)]), (lambda j, s: p.at[2 * s:2 * s + 2, rows48(j)]), rx[:4], (lambda b, s: b.at[2 * s:2 * s + 2])
    z = (lambda j: p.at[j]), (lambda j, s: p.at[j, 96 * s:96 * s + 96]), rx[:4], (lambda b, s: b.at[96 * s:96 * s + 96])
    if h == 0:
        yield from scatter4(cm, 'y', *y)
        yield from direct_scatter(cm, 'z', lambda j: p.at[j, rows48(cm.y)], rx[4:])
    else:
        yield from scatter4(cm, 'z', *z)
        yield from direct_scatter(cm, 'y', lambda j: p.at[cm.z, rows48(j)], rx[4:])


def scatter_scratch():
    V = pltpu.VMEM
    small = [V((48, 384), F32)] * 3
    return [V((2, 48, 384), F32)] * 2 + [V((4, 48, 384), F32)] * 2 + small + [V((96, 384), F32)] * 2 + [V((192, 384), F32)] * 2 + small


def plane_gather(cm, m, h, near=None):
    at = lambda j: rows48(j, align=16)
    if h == 0:
        second = 'z'
        yield from direct_gather(cm, 'y', lambda j: m.at[cm.z, at(j)])
        big, bigh = (lambda j: m.at[j]), (lambda j, s: m.at[j, 96 * s:96 * s + 96])
    else:
        second = 'y'
        yield from direct_gather(cm, 'z', lambda j: m.at[j, at(cm.y)])
        big, bigh = (lambda j: m.at[:, at(j)]), (lambda j, s: m.at[2 * s:2 * s + 2, at(j)])
    if near is None:
        yield from direct_gather(cm, second, big)
        return
    i, r, o, l = cm.rings[second][0]
    g = gather4(cm, second, big, bigh)
    next(g)
    yield
    next(g)
    yield
    near(i)
    yield
    next(g)
    near(l)
    near(r)
    yield
    for _ in g:
        pass
    near(o)


def gain_row(g_ref, d, k):
    g = g_ref[d]
    return jnp.concatenate([g[3 * k + j:3 * k + j + 1] for j in range(3)], axis=1)


def qkv_kernel(x_ref, wq_ref, wk_ref, wv_ref, ga_ref, gm_ref, qkv_ref, g_ref, w_buf, xg, n_buf, gain_buf, wait_buf, *sems):
    cm = Comm(wait_buf, sems)
    x, c, dm = cm.x, cm.c, cm.dm
    peers = [cm.tp * 8 + lax.rem(dm + k, 8) for k in range(1, 8)]
    cm.barrier(peers + [d for a in 'yz' for d in cm.rings[a][1:] + (cm.opposite[a],)])

    first = jnp.where(c == 0, cm.y, cm.z)
    second = jnp.where(c == 0, cm.z, cm.y)
    start = first * 48 + jnp.minimum(second, 2) * 16
    piece = lambda d: x_ref.at[pl.ds(pl.multiple_of(d * 192 + start, 16), 16), :]
    xs = [cm.send(piece(lax.rem(dm + k + 1, 8)), xg.at[c, first, second, x], dev) for k, dev in enumerate(peers)]
    gain_buf[0:3] = ga_ref[...].astype(F32)
    gain_buf[3:6] = gm_ref[...].astype(F32)
    gain_buf[6:8] = jnp.zeros((2, 128), F32)
    (i, r, o, l), dr, dl = cm.rings['x']
    dev_o = cm.other
    rows = lambda j: w_buf.at[j * 2 + c]
    ws = (wq_ref, wk_ref, wv_ref)
    lo, hi, full = pl.ds(0, 192), pl.ds(192, 192), pl.ds(0, 384)
    pieces = ((0, full), (1, lo), (1, hi), (2, full))
    a = [cm.send(ws[n].at[p], rows(i).at[n, p], dr) for n, p in pieces]
    b = [cm.send(ws[n].at[p], rows(i).at[n, p], dl) for n, p in pieces[::-1]]
    e = [cm.send(w, rows(i).at[n], dev_o) for n, w in enumerate(ws)]
    gs = [cm.send(gain_buf, g_ref.at[dm], dev) for dev in peers]
    mine = [cm.local(w, w_buf.at[dm, n]) for n, w in enumerate(ws)]
    xs.append(cm.local(piece(dm), xg.at[c, first, second, x]))
    g_ref[dm] = gain_buf[...]
    cm.wait(*xs)

    def on(cps, src, ps, dev):
        f = []
        for cp, (n, p) in zip(cps, ps):
            cm.wait(cp)
            f.append(cm.send(rows(src).at[n, p], rows(src).at[n, p], dev))
        return f

    def rows_gather(k, small, big, where):
        yield from direct_gather(cm, small, where)
        yield from gather4(cm, big, lambda j: xg.at[k, j], lambda j, s: xg.at[k, j, :, 2 * s:2 * s + 2])

    gy = rows_gather(0, 'z', 'y', lambda j: xg.at[0, cm.y, j])
    gz = rows_gather(1, 'y', 'z', lambda j: xg.at[1, cm.z, j])
    for g in (gy, gz, gy, gz):
        next(g)
    f0 = on(a[:2], l, pieces[:2], dr)
    f1 = on(b[:2], r, pieces[::-1][:2], dl)
    run(gy, gz)
    cm.wait(*gs)
    total = jnp.zeros((192, 1), F32)
    for d in range(8):
        v = xg[d % 2, :, 0:3, d // 2].reshape(192, 384).astype(F32)
        total += jnp.sum(v * v, axis=1, keepdims=True)
    inv = lax.rsqrt(total / 3072 + EPSILON)
    for d in range(8):
        v = xg[d % 2, :, 0:3, d // 2].reshape(192, 384).astype(F32)
        n_buf[d] = (v * inv * (1.0 + gain_row(g_ref, d, 0))).astype(BF)
    def add(j, first=False):
        for n in range(3):
            part = jnp.dot(n_buf[j * 2], w_buf[j * 2, n], preferred_element_type=F32) + jnp.dot(n_buf[j * 2 + 1], w_buf[j * 2 + 1, n], preferred_element_type=F32)
            qkv_ref[n] = part if first else qkv_ref[n] + part

    cm.wait(*e, *mine)
    add(i, True)
    cm.wait(*a[2:])
    e1 = cm.send(rows(l), rows(l), dev_o)
    cm.wait(*b[2:])
    e2 = cm.send(rows(r), rows(r), dev_o)
    cm.wait(e1)
    add(l)
    cm.wait(e2)
    add(r)
    cm.wait(*f0, *f1)
    cm.wait(cm.send(rows(o), rows(o), dev_o))
    add(o)
    cm.drain()


def post_kernel(o_ref, x_ref, wo_ref, wg_ref, wu_ref, wd_ref, g_ref, u_out, v_out, o_buf, wo, x_o, wd, pa, pb, pc, pd, hs, ma, mb, acc_a, acc_b, w_gu, a_buf, u_buf, wait_buf, *rest):
    rx, rx2, sems = rest[:14], rest[14:28], rest[28:]
    cm = Comm(wait_buf, sems)
    x, c, y, z = cm.x, cm.c, cm.y, cm.z
    (i, r, o, l), dr, dl = cm.rings['x']
    dev_o = cm.other
    cm.barrier(cm.neighbours())

    o_buf[x] = o_ref[...]
    go = direct_gather(cm, 'x', lambda j: o_buf.at[j])
    next(go)
    row = lambda core: pl.multiple_of(192 * (2 * z + core) + 48 * y, 16)
    c_wo = cm.send(wo_ref, wo.at[c], dev_o)
    c_x = cm.send(x_ref.at[pl.ds(row(1 - c), 48), :], x_o, dev_o)
    c_wd = cm.send(wd_ref, wd.at[c], dev_o)
    wo[c] = wo_ref[...]
    own_wd = cm.local(wd_ref, wd.at[c])
    kblk = lambda j: pl.ds(pl.multiple_of((j * 2 + c) * 384, 16), 384)
    hcol = lambda j: pl.ds(pl.multiple_of(j * 384, 128), 384)

    def deal(w_ref, col):
        to = pl.ds(col, 384)
        own = w_gu.at[kblk(i), to]
        cps = direct4(cm, 'x', lambda j: w_ref.at[:, hcol(j)], lambda k: own)
        here = [cm.local(w_ref.at[:, hcol(i)], own), cm.send(w_ref.at[:, hcol(i)], own, dev_o)]
        for _ in range(3):
            yield
        for cp, j in zip(cps[1:] + cps[:1], (l, r, o)):
            cm.wait(cp)
            here.append(cm.send(w_gu.at[kblk(j), to], w_gu.at[kblk(j), to], dev_o))
        yield
        cm.wait(*here)

    for _ in go:
        pass
    deal_g = deal(wg_ref, 0)
    next(deal_g)
    cm.wait(c_wo)

    def o_proj(j, carry):
        v = o_buf[j]
        pa[j] = jnp.dot(v, wo[0], preferred_element_type=F32)
        pb[j] = jnp.dot(v, wo[1], preferred_element_type=F32)
        return carry

    lax.fori_loop(0, 4, o_proj, 0)
    run(plane_scatter(cm, pa, 0, rx[:7]), plane_scatter(cm, pb, 1, rx[7:]), deal_g)

    cm.wait(c_x)
    mine, theirs = x_ref[pl.ds(row(c), 48), :].astype(F32), x_o[...].astype(F32)
    first = c == 0
    hs[x, 0] = (jnp.where(first, mine, theirs) + pa[z, rows48(y)]).astype(BF)
    hs[x, 1] = (jnp.where(first, theirs, mine) + pb[z, rows48(y)]).astype(BF)
    run(direct_gather(cm, 'x', lambda j: hs.at[j]))
    deal_u = deal(wu_ref, 384)
    next(deal_u)
    total = jnp.zeros((48, 1), F32)
    for d in range(8):
        v = hs[d // 2, d % 2].astype(F32)
        total += jnp.sum(v * v, axis=1, keepdims=True)
    inv = lax.rsqrt(total / 3072 + EPSILON)
    for d in range(8):
        v = hs[d // 2, d % 2].astype(F32)
        (ma, mb)[d // 4][z, rows48(y, align=16), 384 * (d % 4):384 * (d % 4) + 384] = (v * inv * (1.0 + gain_row(g_ref, d, 1))).astype(BF)

    def part_a(j):
        acc_a[j] = jnp.dot(ma[j], w_gu[0:1536], preferred_element_type=F32)

    def part_b(j):
        acc_b[:, rows48(j)] = jnp.dot(mb[:, rows48(j, align=16)].reshape(192, 1536), w_gu[1536:3072], preferred_element_type=F32).reshape(4, 48, 768)

    run(deal_u, plane_gather(cm, ma, 0, part_a), plane_gather(cm, mb, 1, part_b))

    def hidden(j):
        s = acc_a[j] + acc_b[j]
        gate, up = s[:, 0:384], s[:, 384:768]
        gelu = 0.5 * gate * (1.0 + jnp.tanh(0.7978845608 * (gate + 0.044715 * (gate * gate * gate))))
        a_buf[j, :, hcol(x)] = (gelu * up).astype(BF)

    right, left = {}, {}
    for j in (0, 2, 1, 3):
        hidden(j)
        own = a_buf.at[j, :, hcol(x)]
        right[j] = cm.send(own, own, dr)
        left[j] = cm.send(own, own, dl)
    fwd = []
    for j in (0, 1):
        cm.wait(right[j])
        src = a_buf.at[j, :, hcol(l)]
        fwd.append(cm.send(src, src, dr))
        cm.wait(left[j + 2])
        src = a_buf.at[j + 2, :, hcol(r)]
        fwd.append(cm.send(src, src, dl))
    cm.wait(right[2], right[3], left[0], left[1], c_wd, own_wd)
    for j, k in ((0, 0), (2, 1), (1, 2), (3, 3)):
        cm.wait(fwd[k])
        v = a_buf[j]
        pc[j] = jnp.dot(v, wd[0], preferred_element_type=F32)
        pd[j] = jnp.dot(v, wd[1], preferred_element_type=F32)
    run(plane_scatter(cm, pc, 0, rx2[:7]), plane_scatter(cm, pd, 1, rx2[7:]))
    u_buf[0, z, rows48(y, align=16)] = (hs[x, 0].astype(F32) + pc[z, rows48(y)]).astype(BF)
    u_buf[1, z, rows48(y, align=16)] = (hs[x, 1].astype(F32) + pd[z, rows48(y)]).astype(BF)
    run(plane_gather(cm, u_buf.at[0], 0), plane_gather(cm, u_buf.at[1], 1))
    c_v = cm.send(u_buf.at[1 - c], v_out, dev_o)
    u_out[...] = u_buf[c]
    cm.wait(c_v)
    cm.drain()


def rope_table():
    inv_freq = np.float32(ROPE_THETA) ** (np.float32(-2.0) * np.arange(128, dtype=np.float32) / np.float32(256))
    angles = np.arange(16, dtype=np.float32)[:, None] * inv_freq[None, :].astype(np.float32)
    return np.stack([np.cos(angles), np.sin(angles)]).astype(np.float32)


def attend_kernel(qkv_ref, kc_ref, vc_ref, len_ref, tab_ref, o_ref, ku_ref, vu_ref):
    step = o_ref.shape[0]
    at = pl.ds(pl.multiple_of(pl.program_id(0) * step, step), step)
    pos = len_ref[at, :]
    cos = jnp.zeros((step, 128), F32)
    sin = jnp.zeros((step, 128), F32)
    for t in range(16):
        cos = jnp.where(pos == t, tab_ref[0, t:t + 1], cos)
        sin = jnp.where(pos == t, tab_ref[1, t:t + 1], sin)

    def rope(n):
        lo, hi = qkv_ref[n, at, 0:128], qkv_ref[n, at, 128:256]
        return lo * cos - hi * sin, hi * cos + lo * sin

    tall = lambda a: a.reshape(step, 1, 128)
    rounded = lambda a: a.astype(BF).astype(F32)
    q = [tall(rounded(a * 256 ** -0.5)) for a in rope(0)]
    k_new = [tall(rounded(a)) for a in rope(1)]
    v_new = [tall(rounded(qkv_ref[2, at, 128 * n:128 * n + 128])) for n in range(2)]
    slot = lax.broadcasted_iota(jnp.int32, (step, 16, 128), 1)
    pos3 = pos.reshape(step, 1, 128)
    hit = slot == pos3
    prod = None
    for n in range(2):
        lanes = slice(128 * n, 128 * n + 128)
        k = jnp.where(hit, k_new[n], kc_ref[at, :, lanes].astype(F32))
        ku_ref[:, :, lanes] = k.astype(BF)
        prod = k * q[n] if prod is None else prod + k * q[n]
    score = jnp.sum(prod, axis=2, keepdims=True)
    valid = (slot <= pos3)[:, :, 0:1]
    score = jnp.where(valid, score, -1e30)
    e = jnp.exp(score - jnp.max(score, axis=1, keepdims=True))
    p = rounded(e / jnp.sum(e, axis=1, keepdims=True))
    for n in range(2):
        lanes = slice(128 * n, 128 * n + 128)
        v = jnp.where(hit, v_new[n], vc_ref[at, :, lanes].astype(F32))
        vu_ref[:, :, lanes] = v.astype(BF)
        o_ref[:, lanes] = jnp.sum(jnp.where(slot <= pos3, p * v, 0.0), axis=1).astype(BF)


VM = pl.BlockSpec(memory_space=pltpu.VMEM)


HB = pl.BlockSpec(memory_space=pltpu.HBM)


def call(body, outs, scratch, sems, cid, limit, flops, where, *args):
    single = len(outs) == 1
    return pl.pallas_call(
        body,
        out_shape=outs[0] if single else outs,
        in_specs=[HB if w == 'h' else VM for w in where],
        out_specs=VM if single else [VM] * len(outs),
        scratch_shapes=scratch + [pltpu.SemaphoreType.DMA] * sems,
        compiler_params=pltpu.CompilerParams(collective_id=cid, has_side_effects=True, vmem_limit_bytes=limit * 2**20),
        cost_estimate=pl.CostEstimate(flops=flops, bytes_accessed=8_000_000, transcendentals=0),
    )(*args)


def call2(body, outs, scratch, sems, cid, limit, flops, where, *args):
    single = len(outs) == 1
    return pl.pallas_call(
        body,
        out_shape=outs[0] if single else outs,
        in_specs=[HB if w == 'h' else VM for w in where],
        out_specs=VM if single else [VM] * len(outs),
        scratch_shapes=scratch + [pltpu.SemaphoreType.DMA] * sems,
        compiler_params=pltpu.CompilerParams(collective_id=cid, has_side_effects=True, vmem_limit_bytes=limit * 2**20),
        cost_estimate=pl.CostEstimate(flops=flops, bytes_accessed=8_000_000, transcendentals=0),
    )(*args)


def join_kernel(u_ref, v_ref, out_ref):
    c = lax.rem(lax.axis_index('dm'), 2)
    for j in range(4):
        out_ref[pl.ds(pl.multiple_of(192 * (2 * j + c), 16), 192), :] = u_ref[j]
        out_ref[pl.ds(pl.multiple_of(192 * (2 * j + 1 - c), 16), 192), :] = v_ref[j]


def solution(mesh):
    cache_spec = P(('dp', 'dm'), 'tp', None, None)
    resid_spec = P('dp', 'dm')
    col_spec = P('dm', 'tp')
    row_spec = P('tp', 'dm')
    in_specs = (resid_spec, cache_spec, cache_spec, P('dp'), P('dm'), col_spec, col_spec, col_spec, row_spec, P('dm'), col_spec, col_spec, row_spec)
    out_specs = (resid_spec, cache_spec, cache_spec)
    sds = jax.ShapeDtypeStruct
    V = pltpu.VMEM

    def local_step(resid_in, k_cache, v_cache, cache_len, norm_attn, w_q, w_k, w_v, w_o, norm_mlp, w_gate, w_up, w_down):
        qkv, gain_all = call(
            qkv_kernel,
            (sds((3, 192, 256), F32), sds((8, 8, 128), F32)),
            [V((8, 3, 384, 256), BF), V((2, 4, 4, 4, 16, 384), BF), V((8, 192, 384), BF), V((8, 128), F32), V((8192, 128), BF)],
            60, 0, 58, 2 * 10**9, 'hhhhvv',
            resid_in, w_q, w_k, w_v, norm_attn.reshape(3, 128), norm_mlp.reshape(3, 128))
        lengths = lax.dynamic_slice_in_dim(cache_len, lax.axis_index('dm') * 192, 192)
        cache, step = sds((192, 16, 256), BF), 48
        attn_out, k_upd, v_upd = pl.pallas_call(
            attend_kernel, name='attend', out_shape=(sds((192, 256), BF), cache, cache), grid=(192 // step,), in_specs=[VM] * 5,
            out_specs=[pl.BlockSpec((step, 256), lambda b: (b, 0))] + [pl.BlockSpec((step, 16, 256), lambda b: (b, 0, 0))] * 2,
            compiler_params=pltpu.CompilerParams(vmem_limit_bytes=20 * 2**20),
        )(qkv, k_cache.reshape(192, 16, 256), v_cache.reshape(192, 16, 256), jnp.broadcast_to(lengths[:, None], (192, 128)), jnp.asarray(rope_table()))
        k_upd, v_upd = k_upd.reshape(192, 1, 16, 256), v_upd.reshape(192, 1, 16, 256)
        mine, theirs = call2(
            post_kernel,
            (sds((4, 192, 384), BF), sds((4, 192, 384), BF)),
            [V((4, 192, 256), BF), V((2, 256, 384), BF), V((48, 384), BF), V((2, 1536, 384), BF)]
            + [V((4, 192, 384), F32)] * 4 + [V((4, 2, 48, 384), BF)] + [V((4, 192, 1536), BF)] * 2 + [V((4, 192, 768), F32)] * 2
            + [V((3072, 768), BF), V((4, 192, 1536), BF), V((2, 4, 192, 384), BF), V((16384, 128), BF)]
            + scatter_scratch() + scatter_scratch(),
            170, 1, 44, 7 * 10**9, 'vvvhhhv',
            attn_out, resid_in, w_o, w_gate, w_up, w_down, gain_all)
        resid_out = pl.pallas_call(join_kernel, out_shape=sds((1536, 384), BF), in_specs=[VM, VM], out_specs=VM, compiler_params=pltpu.CompilerParams(vmem_limit_bytes=8 * 2**20))(mine, theirs)
        return resid_out, k_upd, v_upd

    return jax.shard_map(local_step, mesh=mesh, in_specs=in_specs, out_specs=out_specs, check_vma=False)
```

```python
import math

import jax
import jax.numpy as jnp
import numpy as np
from jax import lax
from jax.experimental import pallas as pl
from jax.experimental.pallas import tpu as pltpu
from jax.sharding import PartitionSpec as P

EPSILON = 1e-6
ROPE_THETA = 10000.0
BF = jnp.bfloat16
F32 = jnp.float32
LOGICAL = pl.DeviceIdType.LOGICAL


class Comm:
    def __init__(self, wait_buf, sems):
        self.wait_buf, self.sems = wait_buf, list(sems)
        self.groups = []
        tp, dm = lax.axis_index('tp'), lax.axis_index('dm')
        self.tp, self.dm = tp, dm
        self.z, self.y = lax.div(tp, 4), lax.rem(tp, 4)
        self.x, self.c = lax.div(dm, 2), lax.rem(dm, 2)
        self.other = tp * 8 + self.x * 2 + 1 - self.c
        self.rings, self.opposite = {}, {}
        for axis, me, base, step in (('x', self.x, tp * 8 + self.c, 2), ('y', self.y, self.z * 32 + dm, 8), ('z', self.z, self.y * 8 + dm, 32)):
            idx = [me] + [lax.rem(me + k, 4) for k in (1, 2, 3)]
            self.rings[axis] = idx, base + idx[1] * step, base + idx[3] * step
            self.opposite[axis] = base + idx[2] * step

    def neighbours(self):
        return [self.other] + [d for r in self.rings.values() for d in r[1:]] + list(self.opposite.values())

    def barrier(self, peers):
        sem = pltpu.get_barrier_semaphore()
        for dev in peers:
            pl.semaphore_signal(sem, inc=1, device_id=dev, device_id_type=LOGICAL)
        pl.semaphore_wait(sem, len(peers))

    def send(self, src, dst, dev, recv=None):
        rows = math.prod(dst.shape) * dst.dtype.itemsize // 256
        if not self.groups or self.groups[-1][1] + rows > self.wait_buf.shape[0]:
            self.groups.append([self.sems.pop(), 0])
        self.groups[-1][1] += rows
        recv = self.sems.pop() if recv is None else recv
        pltpu.make_async_remote_copy(src_ref=src, dst_ref=dst, send_sem=self.groups[-1][0], recv_sem=recv, device_id=dev, device_id_type=LOGICAL).start()
        return recv, rows

    def wait(self, *copies):
        total = {}
        for sem, rows in copies:
            total[id(sem)] = sem, total.get(id(sem), (sem, 0))[1] + rows
        for sem, rows in total.values():
            part = self.wait_buf.at[0:rows]
            pltpu.make_async_copy(part, part, sem).wait()

    def local(self, src, dst):
        rows = math.prod(dst.shape) * dst.dtype.itemsize // 256
        sem = self.sems.pop()
        pltpu.make_async_copy(src, dst, sem).start()
        return sem, rows

    def drain(self):
        assert not self.sems, len(self.sems)
        self.wait(*self.groups)


def run(*gens):
    gens = list(gens)
    while gens:
        for g in list(gens):
            try:
                next(g)
            except StopIteration:
                gens.remove(g)


def gather4(cm, axis, blk, hf, fine=True):
    (i, r, o, l), dr, dl = cm.rings[axis]
    if fine:
        a0 = cm.send(hf(i, 0), hf(i, 0), dr)
        b1 = cm.send(hf(i, 1), hf(i, 1), dl)
        a1 = cm.send(hf(i, 1), hf(i, 1), dr)
        b0 = cm.send(hf(i, 0), hf(i, 0), dl, a1[0])
        late = (a1, b0)
    else:
        a0 = cm.send(blk(i), blk(i), dr)
        b1 = cm.send(blk(i), blk(i), dl)
        late = ()
    yield
    cm.wait(a0)
    c = cm.send(hf(l, 0), hf(l, 0), dr)
    cm.wait(b1)
    d = cm.send(hf(r, 1), hf(r, 1), dl, c[0])
    yield
    cm.wait(*late)
    yield
    cm.wait(c, d)


def direct4(cm, axis, src, dst, recv=None):
    (i, r, o, l), dr, dl = cm.rings[axis]
    return [cm.send(src(o), dst(1), cm.opposite[axis], recv), cm.send(src(r), dst(0), dr, recv), cm.send(src(l), dst(2), dl, recv)]


def direct_gather(cm, axis, blk):
    own = blk(cm.rings[axis][0][0])
    cps = direct4(cm, axis, lambda j: own, lambda k: own, cm.sems.pop())
    yield
    cm.wait(*cps)


def direct_scatter(cm, axis, blk, rx):
    cps = direct4(cm, axis, blk, lambda k: rx[k], cm.sems.pop())
    yield
    cm.wait(*cps)
    blk(cm.rings[axis][0][0])[...] += (rx[0][...] + rx[2][...]) + rx[1][...]


def scatter4(cm, axis, blk, hf, rx, hrx):
    (i, r, o, l), dr, dl = cm.rings[axis]
    ro0, ro1, rl, rr = rx
    c0 = cm.send(hf(o, 0), ro0, dr)
    c1 = cm.send(hf(o, 1), ro1, dl)
    c2 = cm.send(hf(r, 1), hrx(rl, 1), dr)
    c3 = cm.send(hf(l, 0), hrx(rr, 0), dl, c2[0])
    yield
    cm.wait(c0)
    hf(r, 0)[...] += ro0[...]
    c4 = cm.send(hf(r, 0), hrx(rl, 0), dr, c2[0])
    cm.wait(c1)
    hf(l, 1)[...] += ro1[...]
    c5 = cm.send(hf(l, 1), hrx(rr, 1), dl, c2[0])
    yield
    cm.wait(c2, c3, c4, c5)
    blk(i)[...] += rl[...] + rr[...]


def rows48(j, start=0, size=48, align=8):
    return pl.ds(pl.multiple_of(j * 48 + start, align), size)


def plane_scatter(cm, p, h, rx):
    y = (lambda j: p.at[:, rows48(j)]), (lambda j, s: p.at[2 * s:2 * s + 2, rows48(j)]), rx[:4], (lambda b, s: b.at[2 * s:2 * s + 2])
    z = (lambda j: p.at[j]), (lambda j, s: p.at[j, 96 * s:96 * s + 96]), rx[:4], (lambda b, s: b.at[96 * s:96 * s + 96])
    if h == 0:
        yield from scatter4(cm, 'y', *y)
        yield from direct_scatter(cm, 'z', lambda j: p.at[j, rows48(cm.y)], rx[4:])
    else:
        yield from scatter4(cm, 'z', *z)
        yield from direct_scatter(cm, 'y', lambda j: p.at[cm.z, rows48(j)], rx[4:])


def scatter_scratch():
    V = pltpu.VMEM
    small = [V((48, 384), F32)] * 3
    return [V((2, 48, 384), F32)] * 2 + [V((4, 48, 384), F32)] * 2 + small + [V((96, 384), F32)] * 2 + [V((192, 384), F32)] * 2 + small


def plane_gather(cm, m, h):
    at = lambda j: rows48(j, align=16)
    if h == 0:
        yield from direct_gather(cm, 'y', lambda j: m.at[cm.z, at(j)])
        yield from direct_gather(cm, 'z', lambda j: m.at[j])
    else:
        yield from direct_gather(cm, 'z', lambda j: m.at[j, at(cm.y)])
        yield from direct_gather(cm, 'y', lambda j: m.at[:, at(j)])


def plane_stream(cm, m, h, near):
    at = lambda j: rows48(j, align=16)
    first, second = ('y', 'z') if h == 0 else ('z', 'y')
    piece = (lambda b, k: m.at[b, at(k)]) if h == 0 else (lambda b, k: m.at[k, at(b)])
    ki, kr, ko, kl = cm.rings[first][0]
    (i, r, o, l), dr, dl = cm.rings[second]
    right, left = {}, {}

    def out(name, k):
        right[name] = cm.send(piece(i, k), piece(i, k), dr)
        left[name] = cm.send(piece(i, k), piece(i, k), dl)

    small = direct4(cm, first, lambda j: piece(i, ki), lambda k: piece(i, ki))
    yield
    out('i', ki)
    yield
    cm.wait(small[1])
    out('l', kl)
    cm.wait(small[2])
    out('r', kr)
    yield
    cm.wait(small[0])
    out('o', ko)
    yield
    cm.wait(right['i'])
    fr = [cm.send(piece(l, ki), piece(l, ki), dr)]
    cm.wait(left['i'])
    yield
    near(i)
    yield
    cm.wait(right['l'])
    fr.append(cm.send(piece(l, kl), piece(l, kl), dr, fr[0][0]))
    cm.wait(left['l'], left['r'])
    fl = [cm.send(piece(r, kr), piece(r, kr), dl)]
    yield
    cm.wait(left['o'])
    fl.append(cm.send(piece(r, ko), piece(r, ko), dl, fl[0][0]))
    cm.wait(right['r'], right['o'])
    yield
    near(l)
    near(r)
    yield
    cm.wait(*fr, *fl)
    near(o)


def gain_row(g_ref, d, k):
    g = g_ref[d]
    return jnp.concatenate([g[3 * k + j:3 * k + j + 1] for j in range(3)], axis=1)


def qkv_kernel(x_ref, wq_ref, wk_ref, wv_ref, ga_ref, gm_ref, qkv_ref, g_ref, w_buf, xg, n_buf, gain_buf, wait_buf, *sems):
    cm = Comm(wait_buf, sems)
    x, c, dm = cm.x, cm.c, cm.dm
    peers = [cm.tp * 8 + lax.rem(dm + k, 8) for k in range(1, 8)]
    cm.barrier(peers + [d for a in 'yz' for d in cm.rings[a][1:] + (cm.opposite[a],)])

    first = jnp.where(c == 0, cm.y, cm.z)
    second = jnp.where(c == 0, cm.z, cm.y)
    start = first * 48 + jnp.minimum(second, 2) * 16
    piece = lambda d: x_ref.at[pl.ds(pl.multiple_of(d * 192 + start, 16), 16), :]
    together = cm.sems.pop()
    xs = [cm.send(piece(lax.rem(dm + k + 1, 8)), xg.at[c, first, second, x], dev, together) for k, dev in enumerate(peers)]
    gain_buf[0:3] = ga_ref[...].astype(F32)
    gain_buf[3:6] = gm_ref[...].astype(F32)
    gain_buf[6:8] = jnp.zeros((2, 128), F32)
    (i, r, o, l), dr, dl = cm.rings['x']
    dev_o = cm.other
    rows = lambda j: w_buf.at[j * 2 + c]
    ws = (wq_ref, wk_ref, wv_ref)
    lo, hi, full = pl.ds(0, 192), pl.ds(192, 192), pl.ds(0, 384)
    pieces = ((0, full), (1, lo), (1, hi), (2, full))
    a = [cm.send(ws[n].at[p], rows(i).at[n, p], dr) for n, p in pieces]
    b = [cm.send(ws[n].at[p], rows(i).at[n, p], dl) for n, p in pieces[::-1]]
    e = [cm.send(w, rows(i).at[n], dev_o) for n, w in enumerate(ws)]
    together = cm.sems.pop()
    gs = [cm.send(gain_buf, g_ref.at[dm], dev, together) for dev in peers]
    mine = [cm.local(w, w_buf.at[dm, n]) for n, w in enumerate(ws)]
    xs.append(cm.local(piece(dm), xg.at[c, first, second, x]))
    g_ref[dm] = gain_buf[...]
    cm.wait(*xs)

    def on(cps, src, ps, dev):
        f = []
        for cp, (n, p) in zip(cps, ps):
            cm.wait(cp)
            f.append(cm.send(rows(src).at[n, p], rows(src).at[n, p], dev))
        return f

    def rows_gather(k, small, big, where):
        yield from direct_gather(cm, small, where)
        yield from gather4(cm, big, lambda j: xg.at[k, j], lambda j, s: xg.at[k, j, :, 2 * s:2 * s + 2])

    gy = rows_gather(0, 'z', 'y', lambda j: xg.at[0, cm.y, j])
    gz = rows_gather(1, 'y', 'z', lambda j: xg.at[1, cm.z, j])
    for g in (gy, gz, gy, gz):
        next(g)
    f0 = on(a[:2], l, pieces[:2], dr)
    f1 = on(b[:2], r, pieces[::-1][:2], dl)
    run(gy, gz)
    cm.wait(*gs)
    total = jnp.zeros((192, 1), F32)
    for d in range(8):
        v = xg[d % 2, :, 0:3, d // 2].reshape(192, 384).astype(F32)
        total += jnp.sum(v * v, axis=1, keepdims=True)
    inv = lax.rsqrt(total / 3072 + EPSILON)
    for d in range(8):
        v = xg[d % 2, :, 0:3, d // 2].reshape(192, 384).astype(F32)
        n_buf[d] = (v * inv * (1.0 + gain_row(g_ref, d, 0))).astype(BF)
    def add(j, first=False):
        for n in range(3):
            part = jnp.dot(n_buf[j * 2], w_buf[j * 2, n], preferred_element_type=F32) + jnp.dot(n_buf[j * 2 + 1], w_buf[j * 2 + 1, n], preferred_element_type=F32)
            qkv_ref[n] = part if first else qkv_ref[n] + part

    cm.wait(*e, *mine)
    add(i, True)
    cm.wait(*a[2:])
    e1 = cm.send(rows(l), rows(l), dev_o)
    cm.wait(*b[2:])
    e2 = cm.send(rows(r), rows(r), dev_o)
    cm.wait(e1)
    add(l)
    cm.wait(e2)
    add(r)
    cm.wait(*f0, *f1)
    cm.wait(cm.send(rows(o), rows(o), dev_o))
    add(o)
    cm.drain()


def post_kernel(o_ref, x_ref, wo_ref, wg_ref, wu_ref, wd_ref, g_ref, u_out, v_out, o_buf, wo, x_o, wd, pa, pb, pc, pd, hs, ma, mb, acc_a, acc_b, w_gu, a_buf, u_buf, wait_buf, *rest):
    rx, rx2, sems = rest[:14], rest[14:28], rest[28:]
    cm = Comm(wait_buf, sems)
    x, c, y, z = cm.x, cm.c, cm.y, cm.z
    (i, r, o, l), dr, dl = cm.rings['x']
    dev_o = cm.other
    cm.barrier(cm.neighbours())

    o_buf[x] = o_ref[...]
    go = direct_gather(cm, 'x', lambda j: o_buf.at[j])
    next(go)
    row = lambda core: pl.multiple_of(192 * (2 * z + core) + 48 * y, 16)
    c_wo = cm.send(wo_ref, wo.at[c], dev_o)
    c_x = cm.send(x_ref.at[pl.ds(row(1 - c), 48), :], x_o, dev_o)
    c_wd = cm.send(wd_ref, wd.at[c], dev_o)
    wo[c] = wo_ref[...]
    own_wd = cm.local(wd_ref, wd.at[c])
    kblk = lambda j: pl.ds(pl.multiple_of((j * 2 + c) * 384, 16), 384)
    hcol = lambda j: pl.ds(pl.multiple_of(j * 384, 128), 384)

    def deal(w_ref, col, pause):
        to = pl.ds(col, 384)
        own = w_gu.at[kblk(i), to]
        cps = direct4(cm, 'x', lambda j: w_ref.at[:, hcol(j)], lambda k: own)
        here = [cm.local(w_ref.at[:, hcol(i)], own), cm.send(w_ref.at[:, hcol(i)], own, dev_o)]
        for _ in range(pause):
            yield
        for cp, j in zip(cps[1:] + cps[:1], (l, r, o)):
            cm.wait(cp)
            here.append(cm.send(w_gu.at[kblk(j), to], w_gu.at[kblk(j), to], dev_o))
        yield
        cm.wait(*here)

    for _ in go:
        pass
    deal_g = deal(wg_ref, 0, 3)
    next(deal_g)
    cm.wait(c_wo)

    def o_proj(j, carry):
        v = o_buf[j]
        pa[j] = jnp.dot(v, wo[0], preferred_element_type=F32)
        pb[j] = jnp.dot(v, wo[1], preferred_element_type=F32)
        return carry

    lax.fori_loop(0, 4, o_proj, 0)
    run(plane_scatter(cm, pa, 0, rx[:7]), plane_scatter(cm, pb, 1, rx[7:]), deal_g)

    cm.wait(c_x)
    mine, theirs = x_ref[pl.ds(row(c), 48), :].astype(F32), x_o[...].astype(F32)
    first = c == 0
    hs[x, 0] = (jnp.where(first, mine, theirs) + pa[z, rows48(y)]).astype(BF)
    hs[x, 1] = (jnp.where(first, theirs, mine) + pb[z, rows48(y)]).astype(BF)
    run(direct_gather(cm, 'x', lambda j: hs.at[j]))
    deal_u = deal(wu_ref, 384, 5)
    next(deal_u)
    total = jnp.zeros((48, 1), F32)
    for d in range(8):
        v = hs[d // 2, d % 2].astype(F32)
        total += jnp.sum(v * v, axis=1, keepdims=True)
    inv = lax.rsqrt(total / 3072 + EPSILON)
    for d in range(8):
        v = hs[d // 2, d % 2].astype(F32)
        (ma, mb)[d // 4][z, rows48(y, align=16), 384 * (d % 4):384 * (d % 4) + 384] = (v * inv * (1.0 + gain_row(g_ref, d, 1))).astype(BF)

    def part_a(j):
        acc_a[j] = jnp.dot(ma[j], w_gu[0:1536], preferred_element_type=F32)

    def part_b(j):
        acc_b[:, rows48(j)] = jnp.dot(mb[:, rows48(j, align=16)].reshape(192, 1536), w_gu[1536:3072], preferred_element_type=F32).reshape(4, 48, 768)

    run(deal_u, plane_stream(cm, ma, 0, part_a), plane_stream(cm, mb, 1, part_b))

    def hidden(j):
        s = acc_a[j] + acc_b[j]
        gate, up = s[:, 0:384], s[:, 384:768]
        gelu = 0.5 * gate * (1.0 + jnp.tanh(0.7978845608 * (gate + 0.044715 * (gate * gate * gate))))
        a_buf[j, :, hcol(x)] = (gelu * up).astype(BF)

    right, left = {}, {}
    for j in (0, 2, 1, 3):
        hidden(j)
        own = a_buf.at[j, :, hcol(x)]
        right[j] = cm.send(own, own, dr)
        left[j] = cm.send(own, own, dl)
    fwd = []
    for j in (0, 1):
        cm.wait(right[j])
        src = a_buf.at[j, :, hcol(l)]
        fwd.append(cm.send(src, src, dr))
        cm.wait(left[j + 2])
        src = a_buf.at[j + 2, :, hcol(r)]
        fwd.append(cm.send(src, src, dl))
    cm.wait(right[2], right[3], left[0], left[1], c_wd, own_wd)
    for j, k in ((0, 0), (2, 1), (1, 2), (3, 3)):
        cm.wait(fwd[k])
        v = a_buf[j]
        pc[j] = jnp.dot(v, wd[0], preferred_element_type=F32)
        pd[j] = jnp.dot(v, wd[1], preferred_element_type=F32)
    run(plane_scatter(cm, pc, 0, rx2[:7]), plane_scatter(cm, pd, 1, rx2[7:]))
    u_buf[0, z, rows48(y, align=16)] = (hs[x, 0].astype(F32) + pc[z, rows48(y)]).astype(BF)
    u_buf[1, z, rows48(y, align=16)] = (hs[x, 1].astype(F32) + pd[z, rows48(y)]).astype(BF)
    run(plane_gather(cm, u_buf.at[0], 0), plane_gather(cm, u_buf.at[1], 1))
    c_v = cm.send(u_buf.at[1 - c], v_out, dev_o)
    u_out[...] = u_buf[c]
    cm.wait(c_v)
    cm.drain()


def rope_table():
    inv_freq = np.float32(ROPE_THETA) ** (np.float32(-2.0) * np.arange(128, dtype=np.float32) / np.float32(256))
    angles = np.arange(16, dtype=np.float32)[:, None] * inv_freq[None, :].astype(np.float32)
    return np.stack([np.cos(angles), np.sin(angles)]).astype(np.float32)


def attend_kernel(qkv_ref, kc_ref, vc_ref, len_ref, tab_ref, o_ref, ku_ref, vu_ref):
    step = o_ref.shape[0]
    at = pl.ds(pl.multiple_of(pl.program_id(0) * step, step), step)
    pos = len_ref[at, :]
    cos = jnp.zeros((step, 128), F32)
    sin = jnp.zeros((step, 128), F32)
    for t in range(16):
        cos = jnp.where(pos == t, tab_ref[0, t:t + 1], cos)
        sin = jnp.where(pos == t, tab_ref[1, t:t + 1], sin)

    def rope(n):
        lo, hi = qkv_ref[n, at, 0:128], qkv_ref[n, at, 128:256]
        return lo * cos - hi * sin, hi * cos + lo * sin

    tall = lambda a: a.reshape(step, 1, 128)
    rounded = lambda a: a.astype(BF).astype(F32)
    q = [tall(rounded(a * 256 ** -0.5)) for a in rope(0)]
    k_new = [tall(rounded(a)) for a in rope(1)]
    v_new = [tall(rounded(qkv_ref[2, at, 128 * n:128 * n + 128])) for n in range(2)]
    slot = lax.broadcasted_iota(jnp.int32, (step, 16, 128), 1)
    pos3 = pos.reshape(step, 1, 128)
    hit = slot == pos3
    prod = None
    for n in range(2):
        lanes = slice(128 * n, 128 * n + 128)
        k = jnp.where(hit, k_new[n], kc_ref[at, :, lanes].astype(F32))
        ku_ref[:, :, lanes] = k.astype(BF)
        prod = k * q[n] if prod is None else prod + k * q[n]
    score = jnp.sum(prod, axis=2, keepdims=True)
    valid = (slot <= pos3)[:, :, 0:1]
    score = jnp.where(valid, score, -1e30)
    e = jnp.exp(score - jnp.max(score, axis=1, keepdims=True))
    p = rounded(e / jnp.sum(e, axis=1, keepdims=True))
    for n in range(2):
        lanes = slice(128 * n, 128 * n + 128)
        v = jnp.where(hit, v_new[n], vc_ref[at, :, lanes].astype(F32))
        vu_ref[:, :, lanes] = v.astype(BF)
        o_ref[:, lanes] = jnp.sum(jnp.where(slot <= pos3, p * v, 0.0), axis=1).astype(BF)


VM = pl.BlockSpec(memory_space=pltpu.VMEM)


HB = pl.BlockSpec(memory_space=pltpu.HBM)


def call(body, outs, scratch, sems, cid, limit, flops, where, *args):
    single = len(outs) == 1
    return pl.pallas_call(
        body,
        out_shape=outs[0] if single else outs,
        in_specs=[HB if w == 'h' else VM for w in where],
        out_specs=VM if single else [VM] * len(outs),
        scratch_shapes=scratch + [pltpu.SemaphoreType.DMA] * sems,
        compiler_params=pltpu.CompilerParams(collective_id=cid, has_side_effects=True, vmem_limit_bytes=limit * 2**20),
        cost_estimate=pl.CostEstimate(flops=flops, bytes_accessed=8_000_000, transcendentals=0),
    )(*args)


def call2(body, outs, scratch, sems, cid, limit, flops, where, *args):
    single = len(outs) == 1
    return pl.pallas_call(
        body,
        out_shape=outs[0] if single else outs,
        in_specs=[HB if w == 'h' else VM for w in where],
        out_specs=VM if single else [VM] * len(outs),
        scratch_shapes=scratch + [pltpu.SemaphoreType.DMA] * sems,
        compiler_params=pltpu.CompilerParams(collective_id=cid, has_side_effects=True, vmem_limit_bytes=limit * 2**20),
        cost_estimate=pl.CostEstimate(flops=flops, bytes_accessed=8_000_000, transcendentals=0),
    )(*args)


def join_kernel(u_ref, v_ref, out_ref):
    c = lax.rem(lax.axis_index('dm'), 2)
    for j in range(4):
        out_ref[pl.ds(pl.multiple_of(192 * (2 * j + c), 16), 192), :] = u_ref[j]
        out_ref[pl.ds(pl.multiple_of(192 * (2 * j + 1 - c), 16), 192), :] = v_ref[j]


def solution(mesh):
    cache_spec = P(('dp', 'dm'), 'tp', None, None)
    resid_spec = P('dp', 'dm')
    col_spec = P('dm', 'tp')
    row_spec = P('tp', 'dm')
    in_specs = (resid_spec, cache_spec, cache_spec, P('dp'), P('dm'), col_spec, col_spec, col_spec, row_spec, P('dm'), col_spec, col_spec, row_spec)
    out_specs = (resid_spec, cache_spec, cache_spec)
    sds = jax.ShapeDtypeStruct
    V = pltpu.VMEM

    def local_step(resid_in, k_cache, v_cache, cache_len, norm_attn, w_q, w_k, w_v, w_o, norm_mlp, w_gate, w_up, w_down):
        qkv, gain_all = call(
            qkv_kernel,
            (sds((3, 192, 256), F32), sds((8, 8, 128), F32)),
            [V((8, 3, 384, 256), BF), V((2, 4, 4, 4, 16, 384), BF), V((8, 192, 384), BF), V((8, 128), F32), V((8192, 128), BF)],
            37, 0, 58, 2 * 10**9, 'hhhhvv',
            resid_in, w_q, w_k, w_v, norm_attn.reshape(3, 128), norm_mlp.reshape(3, 128))
        lengths = lax.dynamic_slice_in_dim(cache_len, lax.axis_index('dm') * 192, 192)
        cache, step = sds((192, 16, 256), BF), 48
        attn_out, k_upd, v_upd = pl.pallas_call(
            attend_kernel, name='attend', out_shape=(sds((192, 256), BF), cache, cache), grid=(192 // step,), in_specs=[VM] * 5,
            out_specs=[pl.BlockSpec((step, 256), lambda b: (b, 0))] + [pl.BlockSpec((step, 16, 256), lambda b: (b, 0, 0))] * 2,
            compiler_params=pltpu.CompilerParams(vmem_limit_bytes=20 * 2**20),
        )(qkv, k_cache.reshape(192, 16, 256), v_cache.reshape(192, 16, 256), jnp.broadcast_to(lengths[:, None], (192, 128)), jnp.asarray(rope_table()))
        k_upd, v_upd = k_upd.reshape(192, 1, 16, 256), v_upd.reshape(192, 1, 16, 256)
        mine, theirs = call2(
            post_kernel,
            (sds((4, 192, 384), BF), sds((4, 192, 384), BF)),
            [V((4, 192, 256), BF), V((2, 256, 384), BF), V((48, 384), BF), V((2, 1536, 384), BF)]
            + [V((4, 192, 384), F32)] * 4 + [V((4, 2, 48, 384), BF)] + [V((4, 192, 1536), BF)] * 2 + [V((4, 192, 768), F32)] * 2
            + [V((3072, 768), BF), V((4, 192, 1536), BF), V((2, 4, 192, 384), BF), V((16384, 128), BF)]
            + scatter_scratch() + scatter_scratch(),
            86, 1, 44, 7 * 10**9, 'vvvhhhv',
            attn_out, resid_in, w_o, w_gate, w_up, w_down, gain_all)
        resid_out = pl.pallas_call(join_kernel, out_shape=sds((1536, 384), BF), in_specs=[VM, VM], out_specs=VM, compiler_params=pltpu.CompilerParams(vmem_limit_bytes=8 * 2**20))(mine, theirs)
        return resid_out, k_upd, v_upd

    return jax.shard_map(local_step, mesh=mesh, in_specs=in_specs, out_specs=out_specs, check_vma=False)
```

```python
import math

import jax
import jax.numpy as jnp
import numpy as np
from jax import lax
from jax.experimental import pallas as pl
from jax.experimental.pallas import tpu as pltpu
from jax.sharding import PartitionSpec as P

EPSILON = 1e-6
ROPE_THETA = 10000.0
BF = jnp.bfloat16
F32 = jnp.float32
LOGICAL = pl.DeviceIdType.LOGICAL


class Comm:
    def __init__(self, wait_buf, sems):
        self.wait_buf, self.sems = wait_buf, list(sems)
        self.groups = []
        tp, dm = lax.axis_index('tp'), lax.axis_index('dm')
        self.tp, self.dm = tp, dm
        self.z, self.y = lax.div(tp, 4), lax.rem(tp, 4)
        self.x, self.c = lax.div(dm, 2), lax.rem(dm, 2)
        self.other = tp * 8 + self.x * 2 + 1 - self.c
        self.rings, self.opposite = {}, {}
        for axis, me, base, step in (('x', self.x, tp * 8 + self.c, 2), ('y', self.y, self.z * 32 + dm, 8), ('z', self.z, self.y * 8 + dm, 32)):
            idx = [me] + [lax.rem(me + k, 4) for k in (1, 2, 3)]
            self.rings[axis] = idx, base + idx[1] * step, base + idx[3] * step
            self.opposite[axis] = base + idx[2] * step

    def neighbours(self):
        return [self.other] + [d for r in self.rings.values() for d in r[1:]] + list(self.opposite.values())

    def barrier(self, peers):
        sem = pltpu.get_barrier_semaphore()
        for dev in peers:
            pl.semaphore_signal(sem, inc=1, device_id=dev, device_id_type=LOGICAL)
        pl.semaphore_wait(sem, len(peers))

    def send(self, src, dst, dev, recv=None):
        rows = math.prod(dst.shape) * dst.dtype.itemsize // 256
        if not self.groups or self.groups[-1][1] + rows > self.wait_buf.shape[0]:
            self.groups.append([self.sems.pop(), 0])
        self.groups[-1][1] += rows
        recv = self.sems.pop() if recv is None else recv
        pltpu.make_async_remote_copy(src_ref=src, dst_ref=dst, send_sem=self.groups[-1][0], recv_sem=recv, device_id=dev, device_id_type=LOGICAL).start()
        return recv, rows

    def wait(self, *copies):
        total = {}
        for sem, rows in copies:
            total[id(sem)] = sem, total.get(id(sem), (sem, 0))[1] + rows
        for sem, rows in total.values():
            part = self.wait_buf.at[0:rows]
            pltpu.make_async_copy(part, part, sem).wait()

    def local(self, src, dst):
        rows = math.prod(dst.shape) * dst.dtype.itemsize // 256
        sem = self.sems.pop()
        pltpu.make_async_copy(src, dst, sem).start()
        return sem, rows

    def drain(self):
        assert not self.sems, len(self.sems)
        self.wait(*self.groups)


def run(*gens):
    gens = list(gens)
    while gens:
        for g in list(gens):
            try:
                next(g)
            except StopIteration:
                gens.remove(g)


def gather4(cm, axis, blk, hf, fine=True):
    (i, r, o, l), dr, dl = cm.rings[axis]
    if fine:
        a0 = cm.send(hf(i, 0), hf(i, 0), dr)
        b1 = cm.send(hf(i, 1), hf(i, 1), dl)
        a1 = cm.send(hf(i, 1), hf(i, 1), dr)
        b0 = cm.send(hf(i, 0), hf(i, 0), dl, a1[0])
        late = (a1, b0)
    else:
        a0 = cm.send(blk(i), blk(i), dr)
        b1 = cm.send(blk(i), blk(i), dl)
        late = ()
    yield
    cm.wait(a0)
    c = cm.send(hf(l, 0), hf(l, 0), dr)
    cm.wait(b1)
    d = cm.send(hf(r, 1), hf(r, 1), dl, c[0])
    yield
    cm.wait(*late)
    yield
    cm.wait(c, d)


def direct4(cm, axis, src, dst, recv=None):
    (i, r, o, l), dr, dl = cm.rings[axis]
    return [cm.send(src(o), dst(1), cm.opposite[axis], recv), cm.send(src(r), dst(0), dr, recv), cm.send(src(l), dst(2), dl, recv)]


def direct_gather(cm, axis, blk):
    own = blk(cm.rings[axis][0][0])
    cps = direct4(cm, axis, lambda j: own, lambda k: own, cm.sems.pop())
    yield
    cm.wait(*cps)


def direct_scatter(cm, axis, blk, rx):
    cps = direct4(cm, axis, blk, lambda k: rx[k], cm.sems.pop())
    yield
    cm.wait(*cps)
    blk(cm.rings[axis][0][0])[...] += (rx[0][...] + rx[2][...]) + rx[1][...]


def scatter4(cm, axis, blk, hf, rx, hrx):
    (i, r, o, l), dr, dl = cm.rings[axis]
    ro0, ro1, rl, rr = rx
    c0 = cm.send(hf(o, 0), ro0, dr)
    c1 = cm.send(hf(o, 1), ro1, dl)
    c2 = cm.send(hf(r, 1), hrx(rl, 1), dr)
    c3 = cm.send(hf(l, 0), hrx(rr, 0), dl, c2[0])
    yield
    cm.wait(c0)
    hf(r, 0)[...] += ro0[...]
    c4 = cm.send(hf(r, 0), hrx(rl, 0), dr, c2[0])
    cm.wait(c1)
    hf(l, 1)[...] += ro1[...]
    c5 = cm.send(hf(l, 1), hrx(rr, 1), dl, c2[0])
    yield
    cm.wait(c2, c3, c4, c5)
    blk(i)[...] += rl[...] + rr[...]


def rows48(j, start=0, size=48, align=8):
    return pl.ds(pl.multiple_of(j * 48 + start, align), size)


def plane_scatter(cm, p, h, rx):
    y = (lambda j: p.at[:, rows48(j)]), (lambda j, s: p.at[2 * s:2 * s + 2, rows48(j)]), rx[:4], (lambda b, s: b.at[2 * s:2 * s + 2])
    z = (lambda j: p.at[j]), (lambda j, s: p.at[j, 96 * s:96 * s + 96]), rx[:4], (lambda b, s: b.at[96 * s:96 * s + 96])
    if h == 0:
        yield from scatter4(cm, 'y', *y)
        yield from direct_scatter(cm, 'z', lambda j: p.at[j, rows48(cm.y)], rx[4:])
    else:
        yield from scatter4(cm, 'z', *z)
        yield from direct_scatter(cm, 'y', lambda j: p.at[cm.z, rows48(j)], rx[4:])


def scatter_scratch():
    V = pltpu.VMEM
    small = [V((48, 384), F32)] * 3
    return [V((2, 48, 384), F32)] * 2 + [V((4, 48, 384), F32)] * 2 + small + [V((96, 384), F32)] * 2 + [V((192, 384), F32)] * 2 + small


def plane_gather(cm, m, h):
    at = lambda j: rows48(j, align=16)
    if h == 0:
        yield from direct_gather(cm, 'y', lambda j: m.at[cm.z, at(j)])
        yield from direct_gather(cm, 'z', lambda j: m.at[j])
    else:
        yield from direct_gather(cm, 'z', lambda j: m.at[j, at(cm.y)])
        yield from direct_gather(cm, 'y', lambda j: m.at[:, at(j)])


def plane_stream(cm, m, h, near):
    at = lambda j: rows48(j, align=16)
    first, second = ('y', 'z') if h == 0 else ('z', 'y')
    piece = (lambda b, k: m.at[b, at(k)]) if h == 0 else (lambda b, k: m.at[k, at(b)])
    ki, kr, ko, kl = cm.rings[first][0]
    (i, r, o, l), dr, dl = cm.rings[second]
    right, left = {}, {}

    def out(name, k):
        right[name] = cm.send(piece(i, k), piece(i, k), dr)
        left[name] = cm.send(piece(i, k), piece(i, k), dl)

    small = direct4(cm, first, lambda j: piece(i, ki), lambda k: piece(i, ki))
    yield
    out('i', ki)
    yield
    cm.wait(small[1])
    out('l', kl)
    cm.wait(small[2])
    out('r', kr)
    yield
    cm.wait(small[0])
    out('o', ko)
    yield
    cm.wait(right['i'])
    fr = [cm.send(piece(l, ki), piece(l, ki), dr)]
    cm.wait(left['i'])
    yield
    near(i)
    yield
    cm.wait(right['l'])
    fr.append(cm.send(piece(l, kl), piece(l, kl), dr, fr[0][0]))
    cm.wait(left['l'], left['r'])
    fl = [cm.send(piece(r, kr), piece(r, kr), dl)]
    yield
    cm.wait(left['o'])
    fl.append(cm.send(piece(r, ko), piece(r, ko), dl, fl[0][0]))
    cm.wait(right['r'], right['o'])
    yield
    near(l)
    near(r)
    yield
    cm.wait(*fr, *fl)
    near(o)


def gain_row(g_ref, d, k):
    g = g_ref[d]
    return jnp.concatenate([g[3 * k + j:3 * k + j + 1] for j in range(3)], axis=1)


def qkv_kernel(x_ref, wq_ref, wk_ref, wv_ref, ga_ref, gm_ref, qkv_ref, g_ref, w_buf, xg, n_buf, gain_buf, wait_buf, *sems):
    cm = Comm(wait_buf, sems)
    x, c, dm = cm.x, cm.c, cm.dm
    peers = [cm.tp * 8 + lax.rem(dm + k, 8) for k in range(1, 8)]
    cm.barrier(peers + [d for a in 'yz' for d in cm.rings[a][1:] + (cm.opposite[a],)])

    first = jnp.where(c == 0, cm.y, cm.z)
    second = jnp.where(c == 0, cm.z, cm.y)
    start = first * 48 + jnp.minimum(second, 2) * 16
    piece = lambda d: x_ref.at[pl.ds(pl.multiple_of(d * 192 + start, 16), 16), :]
    together = cm.sems.pop()
    xs = [cm.send(piece(lax.rem(dm + k + 1, 8)), xg.at[c, first, second, x], dev, together) for k, dev in enumerate(peers)]
    gain_buf[0:3] = ga_ref[...].astype(F32)
    gain_buf[3:6] = gm_ref[...].astype(F32)
    gain_buf[6:8] = jnp.zeros((2, 128), F32)
    (i, r, o, l), dr, dl = cm.rings['x']
    dev_o = cm.other
    rows = lambda j: w_buf.at[j * 2 + c]
    ws = (wq_ref, wk_ref, wv_ref)
    lo, hi, full = pl.ds(0, 192), pl.ds(192, 192), pl.ds(0, 384)
    pieces = ((0, full), (1, lo), (1, hi), (2, full))
    a = [cm.send(ws[n].at[p], rows(i).at[n, p], dr) for n, p in pieces]
    b = [cm.send(ws[n].at[p], rows(i).at[n, p], dl) for n, p in pieces[::-1]]
    e = [cm.send(w, rows(i).at[n], dev_o) for n, w in enumerate(ws)]
    together = cm.sems.pop()
    gs = [cm.send(gain_buf, g_ref.at[dm], dev, together) for dev in peers]
    mine = [cm.local(w, w_buf.at[dm, n]) for n, w in enumerate(ws)]
    xs.append(cm.local(piece(dm), xg.at[c, first, second, x]))
    g_ref[dm] = gain_buf[...]
    cm.wait(*xs)

    def on(cps, src, ps, dev):
        f = []
        for cp, (n, p) in zip(cps, ps):
            cm.wait(cp)
            f.append(cm.send(rows(src).at[n, p], rows(src).at[n, p], dev))
        return f

    def rows_gather(k, small, big, where):
        yield from direct_gather(cm, small, where)
        yield from gather4(cm, big, lambda j: xg.at[k, j], lambda j, s: xg.at[k, j, :, 2 * s:2 * s + 2])

    gy = rows_gather(0, 'z', 'y', lambda j: xg.at[0, cm.y, j])
    gz = rows_gather(1, 'y', 'z', lambda j: xg.at[1, cm.z, j])
    for g in (gy, gz, gy, gz):
        next(g)
    f0 = on(a[:2], l, pieces[:2], dr)
    f1 = on(b[:2], r, pieces[::-1][:2], dl)
    run(gy, gz)
    cm.wait(*gs)
    total = jnp.zeros((192, 1), F32)
    for d in range(8):
        v = xg[d % 2, :, 0:3, d // 2].reshape(192, 384).astype(F32)
        total += jnp.sum(v * v, axis=1, keepdims=True)
    inv = lax.rsqrt(total / 3072 + EPSILON)
    for d in range(8):
        v = xg[d % 2, :, 0:3, d // 2].reshape(192, 384).astype(F32)
        n_buf[d] = (v * inv * (1.0 + gain_row(g_ref, d, 0))).astype(BF)
    def add(j, first=False):
        for n in range(3):
            part = jnp.dot(n_buf[j * 2], w_buf[j * 2, n], preferred_element_type=F32) + jnp.dot(n_buf[j * 2 + 1], w_buf[j * 2 + 1, n], preferred_element_type=F32)
            qkv_ref[n] = part if first else qkv_ref[n] + part

    cm.wait(*e, *mine)
    add(i, True)
    cm.wait(*a[2:])
    e1 = cm.send(rows(l), rows(l), dev_o)
    cm.wait(*b[2:])
    e2 = cm.send(rows(r), rows(r), dev_o)
    cm.wait(e1)
    add(l)
    cm.wait(e2)
    add(r)
    cm.wait(*f0, *f1)
    cm.wait(cm.send(rows(o), rows(o), dev_o))
    add(o)
    cm.drain()


def post_kernel(o_ref, x_ref, wo_ref, wg_ref, wu_ref, wd_ref, g_ref, u_out, v_out, o_buf, wo, x_o, wd, pa, pb, pc, pd, hs, ma, mb, acc_a, acc_b, w_gu, a_buf, u_buf, wait_buf, *rest):
    rx, rx2, sems = rest[:14], rest[14:35], rest[35:]
    cm = Comm(wait_buf, sems)
    x, c, y, z = cm.x, cm.c, cm.y, cm.z
    (i, r, o, l), dr, dl = cm.rings['x']
    dev_o = cm.other
    cm.barrier(cm.neighbours())

    o_buf[x] = o_ref[...]
    go = direct_gather(cm, 'x', lambda j: o_buf.at[j])
    next(go)
    row = lambda core: pl.multiple_of(192 * (2 * z + core) + 48 * y, 16)
    c_wo = cm.send(wo_ref, wo.at[c], dev_o)
    c_x = cm.send(x_ref.at[pl.ds(row(1 - c), 48), :], x_o, dev_o)
    c_wd = cm.send(wd_ref, wd.at[c], dev_o)
    wo[c] = wo_ref[...]
    own_wd = cm.local(wd_ref, wd.at[c])
    kblk = lambda j: pl.ds(pl.multiple_of((j * 2 + c) * 384, 16), 384)
    hcol = lambda j: pl.ds(pl.multiple_of(j * 384, 128), 384)

    def deal(w_ref, col, pause):
        to = pl.ds(col, 384)
        own = w_gu.at[kblk(i), to]
        cps = direct4(cm, 'x', lambda j: w_ref.at[:, hcol(j)], lambda k: own)
        here = [cm.local(w_ref.at[:, hcol(i)], own), cm.send(w_ref.at[:, hcol(i)], own, dev_o)]
        for _ in range(pause):
            yield
        for cp, j in zip(cps[1:] + cps[:1], (l, r, o)):
            cm.wait(cp)
            here.append(cm.send(w_gu.at[kblk(j), to], w_gu.at[kblk(j), to], dev_o))
        yield
        cm.wait(*here)

    for _ in go:
        pass
    deal_g = deal(wg_ref, 0, 3)
    next(deal_g)
    cm.wait(c_wo)

    def o_proj(j, carry):
        v = o_buf[j]
        pa[j] = jnp.dot(v, wo[0], preferred_element_type=F32)
        pb[j] = jnp.dot(v, wo[1], preferred_element_type=F32)
        return carry

    lax.fori_loop(0, 4, o_proj, 0)
    run(plane_scatter(cm, pa, 0, rx[:7]), plane_scatter(cm, pb, 1, rx[7:]), deal_g)

    cm.wait(c_x)
    mine, theirs = x_ref[pl.ds(row(c), 48), :].astype(F32), x_o[...].astype(F32)
    first = c == 0
    hs[x, 0] = (jnp.where(first, mine, theirs) + pa[z, rows48(y)]).astype(BF)
    hs[x, 1] = (jnp.where(first, theirs, mine) + pb[z, rows48(y)]).astype(BF)
    run(direct_gather(cm, 'x', lambda j: hs.at[j]))
    deal_u = deal(wu_ref, 384, 5)
    next(deal_u)
    total = jnp.zeros((48, 1), F32)
    for d in range(8):
        v = hs[d // 2, d % 2].astype(F32)
        total += jnp.sum(v * v, axis=1, keepdims=True)
    inv = lax.rsqrt(total / 3072 + EPSILON)
    for d in range(8):
        v = hs[d // 2, d % 2].astype(F32)
        (ma, mb)[d // 4][z, rows48(y, align=16), 384 * (d % 4):384 * (d % 4) + 384] = (v * inv * (1.0 + gain_row(g_ref, d, 1))).astype(BF)

    def part_a(j):
        acc_a[j] = jnp.dot(ma[j], w_gu[0:1536], preferred_element_type=F32)

    def part_b(j):
        acc_b[:, rows48(j)] = jnp.dot(mb[:, rows48(j, align=16)].reshape(192, 1536), w_gu[1536:3072], preferred_element_type=F32).reshape(4, 48, 768)

    run(deal_u, plane_stream(cm, ma, 0, part_a), plane_stream(cm, mb, 1, part_b))

    def hidden(j):
        s = acc_a[j] + acc_b[j]
        gate, up = s[:, 0:384], s[:, 384:768]
        gelu = 0.5 * gate * (1.0 + jnp.tanh(0.7978845608 * (gate + 0.044715 * (gate * gate * gate))))
        a_buf[j, :, hcol(x)] = (gelu * up).astype(BF)

    block = dict(zip('irol', cm.rings['z'][0]))
    y_ring = cm.rings['y'][0]
    ra, ra2, rb, rb2 = rx2[:12], rx2[12:15], rx2[15:18], rx2[18:21]
    right, left, fwd, first, second = {}, {}, {}, {}, {}

    def ship(name, via, dev):
        own = a_buf.at[block[name], :, hcol(x)]
        via[name] = cm.send(own, own, dev)

    def pass_on(name, via, frm, dev):
        cm.wait(via[name])
        src = a_buf.at[block[name], :, hcol(frm)]
        fwd[name] = cm.send(src, src, dev)

    def down(name):
        j = block[name]
        v = a_buf[j]
        pc[j] = jnp.dot(v, wd[0], preferred_element_type=F32)
        pd[j] = jnp.dot(v, wd[1], preferred_element_type=F32)
        k = 3 * 'orli'.index(name)
        first[name] = direct4(cm, 'y', lambda q: pc.at[j, rows48(q)], lambda q: ra[k + q], cm.sems.pop())

    def finish(name):
        cm.wait(*first[name])
        q = 3 * 'orli'.index(name)
        pc[block[name], rows48(y)] += (ra[q][...] + ra[q + 2][...]) + ra[q + 1][...]

    z_dev = {'o': cm.opposite['z'], 'r': cm.rings['z'][1], 'l': cm.rings['z'][2]}
    slot = {'o': 1, 'r': 0, 'l': 2}

    def send_z(name):
        j = block[name]
        second[name] = cm.send(pd.at[j], rb[slot[name]], z_dev[name])

    def send_z2(name):
        finish(name)
        second[name + '2'] = cm.send(pc.at[block[name], rows48(y)], ra2[slot[name]], z_dev[name])

    hidden(block['o'])
    ship('o', right, dr)
    hidden(block['r'])
    ship('r', left, dl)
    ship('o', left, dl)
    hidden(block['l'])
    ship('l', right, dr)
    hidden(block['i'])
    pass_on('o', right, l, dr)
    ship('r', right, dr)
    pass_on('r', left, r, dl)
    ship('i', left, dl)
    ship('l', left, dl)
    pass_on('l', right, l, dr)
    ship('i', right, dr)
    cm.wait(c_wd, own_wd, left['o'], fwd['o'])
    down('o')
    send_z('o')
    cm.wait(right['r'], fwd['r'])
    pass_on('i', left, r, dl)
    down('r')
    send_z('r')
    cm.wait(left['l'], fwd['l'])
    down('l')
    send_z('l')
    send_z2('o')
    send_z2('r')
    cm.wait(right['i'], fwd['i'])
    down('i')
    cm.wait(second['o'], second['r'], second['l'])
    pd[z] += (rb[0][...] + rb[2][...]) + rb[1][...]
    last = direct_scatter(cm, 'y', lambda q: pd.at[z, rows48(q)], rb2)
    next(last)
    send_z2('l')
    finish('i')
    cm.wait(second['o2'], second['r2'], second['l2'])
    pc[z, rows48(y)] += (ra2[0][...] + ra2[2][...]) + ra2[1][...]
    run(last)
    u_buf[0, z, rows48(y, align=16)] = (hs[x, 0].astype(F32) + pc[z, rows48(y)]).astype(BF)
    u_buf[1, z, rows48(y, align=16)] = (hs[x, 1].astype(F32) + pd[z, rows48(y)]).astype(BF)
    run(plane_gather(cm, u_buf.at[0], 0), plane_gather(cm, u_buf.at[1], 1))
    c_v = cm.send(u_buf.at[1 - c], v_out, dev_o)
    u_out[...] = u_buf[c]
    cm.wait(c_v)
    cm.drain()


def rope_table():
    inv_freq = np.float32(ROPE_THETA) ** (np.float32(-2.0) * np.arange(128, dtype=np.float32) / np.float32(256))
    angles = np.arange(16, dtype=np.float32)[:, None] * inv_freq[None, :].astype(np.float32)
    return np.stack([np.cos(angles), np.sin(angles)]).astype(np.float32)


def attend_kernel(qkv_ref, kc_ref, vc_ref, len_ref, tab_ref, o_ref, ku_ref, vu_ref):
    step = o_ref.shape[0]
    at = pl.ds(pl.multiple_of(pl.program_id(0) * step, step), step)
    pos = len_ref[at, :]
    cos = jnp.zeros((step, 128), F32)
    sin = jnp.zeros((step, 128), F32)
    for t in range(16):
        cos = jnp.where(pos == t, tab_ref[0, t:t + 1], cos)
        sin = jnp.where(pos == t, tab_ref[1, t:t + 1], sin)

    def rope(n):
        lo, hi = qkv_ref[n, at, 0:128], qkv_ref[n, at, 128:256]
        return lo * cos - hi * sin, hi * cos + lo * sin

    tall = lambda a: a.reshape(step, 1, 128)
    rounded = lambda a: a.astype(BF).astype(F32)
    q = [tall(rounded(a * 256 ** -0.5)) for a in rope(0)]
    k_new = [tall(rounded(a)) for a in rope(1)]
    v_new = [tall(rounded(qkv_ref[2, at, 128 * n:128 * n + 128])) for n in range(2)]
    slot = lax.broadcasted_iota(jnp.int32, (step, 16, 128), 1)
    pos3 = pos.reshape(step, 1, 128)
    hit = slot == pos3
    prod = None
    for n in range(2):
        lanes = slice(128 * n, 128 * n + 128)
        k = jnp.where(hit, k_new[n], kc_ref[at, :, lanes].astype(F32))
        ku_ref[:, :, lanes] = k.astype(BF)
        prod = k * q[n] if prod is None else prod + k * q[n]
    score = jnp.sum(prod, axis=2, keepdims=True)
    valid = (slot <= pos3)[:, :, 0:1]
    score = jnp.where(valid, score, -1e30)
    e = jnp.exp(score - jnp.max(score, axis=1, keepdims=True))
    p = rounded(e / jnp.sum(e, axis=1, keepdims=True))
    for n in range(2):
        lanes = slice(128 * n, 128 * n + 128)
        v = jnp.where(hit, v_new[n], vc_ref[at, :, lanes].astype(F32))
        vu_ref[:, :, lanes] = v.astype(BF)
        o_ref[:, lanes] = jnp.sum(jnp.where(slot <= pos3, p * v, 0.0), axis=1).astype(BF)


VM = pl.BlockSpec(memory_space=pltpu.VMEM)


HB = pl.BlockSpec(memory_space=pltpu.HBM)


def call(body, outs, scratch, sems, cid, limit, flops, where, *args):
    single = len(outs) == 1
    return pl.pallas_call(
        body,
        out_shape=outs[0] if single else outs,
        in_specs=[HB if w == 'h' else VM for w in where],
        out_specs=VM if single else [VM] * len(outs),
        scratch_shapes=scratch + [pltpu.SemaphoreType.DMA] * sems,
        compiler_params=pltpu.CompilerParams(collective_id=cid, has_side_effects=True, vmem_limit_bytes=limit * 2**20),
        cost_estimate=pl.CostEstimate(flops=flops, bytes_accessed=8_000_000, transcendentals=0),
    )(*args)


def call2(body, outs, scratch, sems, cid, limit, flops, where, *args):
    single = len(outs) == 1
    return pl.pallas_call(
        body,
        out_shape=outs[0] if single else outs,
        in_specs=[HB if w == 'h' else VM for w in where],
        out_specs=VM if single else [VM] * len(outs),
        scratch_shapes=scratch + [pltpu.SemaphoreType.DMA] * sems,
        compiler_params=pltpu.CompilerParams(collective_id=cid, has_side_effects=True, vmem_limit_bytes=limit * 2**20),
        cost_estimate=pl.CostEstimate(flops=flops, bytes_accessed=8_000_000, transcendentals=0),
    )(*args)


def join_kernel(u_ref, v_ref, out_ref):
    c = lax.rem(lax.axis_index('dm'), 2)
    for j in range(4):
        out_ref[pl.ds(pl.multiple_of(192 * (2 * j + c), 16), 192), :] = u_ref[j]
        out_ref[pl.ds(pl.multiple_of(192 * (2 * j + 1 - c), 16), 192), :] = v_ref[j]


def solution(mesh):
    cache_spec = P(('dp', 'dm'), 'tp', None, None)
    resid_spec = P('dp', 'dm')
    col_spec = P('dm', 'tp')
    row_spec = P('tp', 'dm')
    in_specs = (resid_spec, cache_spec, cache_spec, P('dp'), P('dm'), col_spec, col_spec, col_spec, row_spec, P('dm'), col_spec, col_spec, row_spec)
    out_specs = (resid_spec, cache_spec, cache_spec)
    sds = jax.ShapeDtypeStruct
    V = pltpu.VMEM

    def local_step(resid_in, k_cache, v_cache, cache_len, norm_attn, w_q, w_k, w_v, w_o, norm_mlp, w_gate, w_up, w_down):
        qkv, gain_all = call(
            qkv_kernel,
            (sds((3, 192, 256), F32), sds((8, 8, 128), F32)),
            [V((8, 3, 384, 256), BF), V((2, 4, 4, 4, 16, 384), BF), V((8, 192, 384), BF), V((8, 128), F32), V((8192, 128), BF)],
            37, 0, 58, 2 * 10**9, 'hhhhvv',
            resid_in, w_q, w_k, w_v, norm_attn.reshape(3, 128), norm_mlp.reshape(3, 128))
        lengths = lax.dynamic_slice_in_dim(cache_len, lax.axis_index('dm') * 192, 192)
        cache, step = sds((192, 16, 256), BF), 48
        attn_out, k_upd, v_upd = pl.pallas_call(
            attend_kernel, name='attend', out_shape=(sds((192, 256), BF), cache, cache), grid=(192 // step,), in_specs=[VM] * 5,
            out_specs=[pl.BlockSpec((step, 256), lambda b: (b, 0))] + [pl.BlockSpec((step, 16, 256), lambda b: (b, 0, 0))] * 2,
            compiler_params=pltpu.CompilerParams(vmem_limit_bytes=20 * 2**20),
        )(qkv, k_cache.reshape(192, 16, 256), v_cache.reshape(192, 16, 256), jnp.broadcast_to(lengths[:, None], (192, 128)), jnp.asarray(rope_table()))
        k_upd, v_upd = k_upd.reshape(192, 1, 16, 256), v_upd.reshape(192, 1, 16, 256)
        mine, theirs = call2(
            post_kernel,
            (sds((4, 192, 384), BF), sds((4, 192, 384), BF)),
            [V((4, 192, 256), BF), V((2, 256, 384), BF), V((48, 384), BF), V((2, 1536, 384), BF)]
            + [V((4, 192, 384), F32)] * 4 + [V((4, 2, 48, 384), BF)] + [V((4, 192, 1536), BF)] * 2 + [V((4, 192, 768), F32)] * 2
            + [V((3072, 768), BF), V((4, 192, 1536), BF), V((2, 4, 192, 384), BF), V((16384, 128), BF)]
            + scatter_scratch() + [V((48, 384), F32)] * 15 + [V((192, 384), F32)] * 3 + [V((48, 384), F32)] * 3,
            89, 1, 44, 7 * 10**9, 'vvvhhhv',
            attn_out, resid_in, w_o, w_gate, w_up, w_down, gain_all)
        resid_out = pl.pallas_call(join_kernel, out_shape=sds((1536, 384), BF), in_specs=[VM, VM], out_specs=VM, compiler_params=pltpu.CompilerParams(vmem_limit_bytes=8 * 2**20))(mine, theirs)
        return resid_out, k_upd, v_upd

    return jax.shard_map(local_step, mesh=mesh, in_specs=in_specs, out_specs=out_specs, check_vma=False)
```

```python
import math

import jax
import jax.numpy as jnp
import numpy as np
from jax import lax
from jax.experimental import pallas as pl
from jax.experimental.pallas import tpu as pltpu
from jax.sharding import PartitionSpec as P

EPSILON = 1e-6
ROPE_THETA = 10000.0
BF = jnp.bfloat16
F32 = jnp.float32
LOGICAL = pl.DeviceIdType.LOGICAL


class Comm:
    def __init__(self, wait_buf, sems):
        self.wait_buf, self.sems = wait_buf, list(sems)
        self.groups = []
        tp, dm = lax.axis_index('tp'), lax.axis_index('dm')
        self.tp, self.dm = tp, dm
        self.z, self.y = lax.div(tp, 4), lax.rem(tp, 4)
        self.x, self.c = lax.div(dm, 2), lax.rem(dm, 2)
        self.other = tp * 8 + self.x * 2 + 1 - self.c
        self.rings, self.opposite = {}, {}
        for axis, me, base, step in (('x', self.x, tp * 8 + self.c, 2), ('y', self.y, self.z * 32 + dm, 8), ('z', self.z, self.y * 8 + dm, 32)):
            idx = [me] + [lax.rem(me + k, 4) for k in (1, 2, 3)]
            self.rings[axis] = idx, base + idx[1] * step, base + idx[3] * step
            self.opposite[axis] = base + idx[2] * step

    def neighbours(self):
        return [self.other] + [d for r in self.rings.values() for d in r[1:]] + list(self.opposite.values())

    def barrier(self, peers):
        sem = pltpu.get_barrier_semaphore()
        for dev in peers:
            pl.semaphore_signal(sem, inc=1, device_id=dev, device_id_type=LOGICAL)
        pl.semaphore_wait(sem, len(peers))

    def send(self, src, dst, dev, recv=None):
        rows = math.prod(dst.shape) * dst.dtype.itemsize // 256
        if not self.groups or self.groups[-1][1] + rows > self.wait_buf.shape[0]:
            self.groups.append([self.sems.pop(), 0])
        self.groups[-1][1] += rows
        recv = self.sems.pop() if recv is None else recv
        pltpu.make_async_remote_copy(src_ref=src, dst_ref=dst, send_sem=self.groups[-1][0], recv_sem=recv, device_id=dev, device_id_type=LOGICAL).start()
        return recv, rows

    def wait(self, *copies):
        total = {}
        for sem, rows in copies:
            total[id(sem)] = sem, total.get(id(sem), (sem, 0))[1] + rows
        for sem, rows in total.values():
            part = self.wait_buf.at[0:rows]
            pltpu.make_async_copy(part, part, sem).wait()

    def local(self, src, dst):
        rows = math.prod(dst.shape) * dst.dtype.itemsize // 256
        sem = self.sems.pop()
        pltpu.make_async_copy(src, dst, sem).start()
        return sem, rows

    def drain(self):
        assert not self.sems, len(self.sems)
        self.wait(*self.groups)


def run(*gens):
    gens = list(gens)
    while gens:
        for g in list(gens):
            try:
                next(g)
            except StopIteration:
                gens.remove(g)


def gather4(cm, axis, blk, hf, fine=True):
    (i, r, o, l), dr, dl = cm.rings[axis]
    if fine:
        a0 = cm.send(hf(i, 0), hf(i, 0), dr)
        b1 = cm.send(hf(i, 1), hf(i, 1), dl)
        a1 = cm.send(hf(i, 1), hf(i, 1), dr)
        b0 = cm.send(hf(i, 0), hf(i, 0), dl, a1[0])
        late = (a1, b0)
    else:
        a0 = cm.send(blk(i), blk(i), dr)
        b1 = cm.send(blk(i), blk(i), dl)
        late = ()
    yield
    cm.wait(a0)
    c = cm.send(hf(l, 0), hf(l, 0), dr)
    cm.wait(b1)
    d = cm.send(hf(r, 1), hf(r, 1), dl, c[0])
    yield
    cm.wait(*late)
    yield
    cm.wait(c, d)


def direct4(cm, axis, src, dst, recv=None):
    (i, r, o, l), dr, dl = cm.rings[axis]
    return [cm.send(src(o), dst(1), cm.opposite[axis], recv), cm.send(src(r), dst(0), dr, recv), cm.send(src(l), dst(2), dl, recv)]


def direct_gather(cm, axis, blk):
    own = blk(cm.rings[axis][0][0])
    cps = direct4(cm, axis, lambda j: own, lambda k: own, cm.sems.pop())
    yield
    cm.wait(*cps)


def direct_scatter(cm, axis, blk, rx):
    cps = direct4(cm, axis, blk, lambda k: rx[k], cm.sems.pop())
    yield
    cm.wait(*cps)
    blk(cm.rings[axis][0][0])[...] += (rx[0][...] + rx[2][...]) + rx[1][...]


def scatter4(cm, axis, blk, hf, rx, hrx):
    (i, r, o, l), dr, dl = cm.rings[axis]
    ro0, ro1, rl, rr = rx
    c0 = cm.send(hf(o, 0), ro0, dr)
    c1 = cm.send(hf(o, 1), ro1, dl)
    c2 = cm.send(hf(r, 1), hrx(rl, 1), dr)
    c3 = cm.send(hf(l, 0), hrx(rr, 0), dl, c2[0])
    yield
    cm.wait(c0)
    hf(r, 0)[...] += ro0[...]
    c4 = cm.send(hf(r, 0), hrx(rl, 0), dr, c2[0])
    cm.wait(c1)
    hf(l, 1)[...] += ro1[...]
    c5 = cm.send(hf(l, 1), hrx(rr, 1), dl, c2[0])
    yield
    cm.wait(c2, c3, c4, c5)
    blk(i)[...] += rl[...] + rr[...]


def rows48(j, start=0, size=48, align=8):
    return pl.ds(pl.multiple_of(j * 48 + start, align), size)


def plane_scatter(cm, p, h, rx):
    y = (lambda j: p.at[:, rows48(j)]), (lambda j, s: p.at[2 * s:2 * s + 2, rows48(j)]), rx[:4], (lambda b, s: b.at[2 * s:2 * s + 2])
    z = (lambda j: p.at[j]), (lambda j, s: p.at[j, 96 * s:96 * s + 96]), rx[:4], (lambda b, s: b.at[96 * s:96 * s + 96])
    if h == 0:
        yield from scatter4(cm, 'y', *y)
        yield from direct_scatter(cm, 'z', lambda j: p.at[j, rows48(cm.y)], rx[4:])
    else:
        yield from scatter4(cm, 'z', *z)
        yield from direct_scatter(cm, 'y', lambda j: p.at[cm.z, rows48(j)], rx[4:])


def scatter_scratch():
    V = pltpu.VMEM
    small = [V((48, 384), F32)] * 3
    return [V((2, 48, 384), F32)] * 2 + [V((4, 48, 384), F32)] * 2 + small + [V((96, 384), F32)] * 2 + [V((192, 384), F32)] * 2 + small


def plane_burst(cm, m, h):
    at = lambda j: rows48(j, align=16)
    first, second = ('y', 'z') if h == 0 else ('z', 'y')
    piece = (lambda k: m.at[cm.z, at(k)]) if h == 0 else (lambda k: m.at[k, at(cm.y)])
    ki, kr, ko, kl = cm.rings[first][0]
    recv = cm.sems.pop()
    outs = []

    def out(k):
        outs.extend(direct4(cm, second, lambda j: piece(k), lambda q: piece(k), recv))

    small = direct4(cm, first, lambda j: piece(ki), lambda k: piece(ki))
    out(ki)
    yield
    cm.wait(small[1])
    out(kl)
    cm.wait(small[2])
    out(kr)
    yield
    cm.wait(small[0])
    out(ko)
    yield
    cm.wait(*outs)


def plane_stream(cm, m, h, near):
    at = lambda j: rows48(j, align=16)
    first, second = ('y', 'z') if h == 0 else ('z', 'y')
    piece = (lambda b, k: m.at[b, at(k)]) if h == 0 else (lambda b, k: m.at[k, at(b)])
    ki, kr, ko, kl = cm.rings[first][0]
    (i, r, o, l), dr, dl = cm.rings[second]
    right, left = {}, {}

    def out(name, k):
        right[name] = cm.send(piece(i, k), piece(i, k), dr)
        left[name] = cm.send(piece(i, k), piece(i, k), dl)

    small = direct4(cm, first, lambda j: piece(i, ki), lambda k: piece(i, ki))
    yield
    out('i', ki)
    yield
    cm.wait(small[1])
    out('l', kl)
    cm.wait(small[2])
    out('r', kr)
    yield
    cm.wait(small[0])
    out('o', ko)
    yield
    cm.wait(right['i'])
    fr = [cm.send(piece(l, ki), piece(l, ki), dr)]
    cm.wait(left['i'])
    yield
    near(i)
    yield
    cm.wait(right['l'])
    fr.append(cm.send(piece(l, kl), piece(l, kl), dr, fr[0][0]))
    cm.wait(left['l'], left['r'])
    fl = [cm.send(piece(r, kr), piece(r, kr), dl)]
    yield
    cm.wait(left['o'])
    fl.append(cm.send(piece(r, ko), piece(r, ko), dl, fl[0][0]))
    cm.wait(right['r'], right['o'])
    yield
    near(l)
    near(r)
    yield
    cm.wait(*fr, *fl)
    near(o)


def gain_row(g_ref, d, k):
    g = g_ref[d]
    return jnp.concatenate([g[3 * k + j:3 * k + j + 1] for j in range(3)], axis=1)


def qkv_kernel(x_ref, wq_ref, wk_ref, wv_ref, ga_ref, gm_ref, qkv_ref, g_ref, w_buf, xg, n_buf, gain_buf, wait_buf, *sems):
    cm = Comm(wait_buf, sems)
    x, c, dm = cm.x, cm.c, cm.dm
    peers = [cm.tp * 8 + lax.rem(dm + k, 8) for k in range(1, 8)]
    cm.barrier(peers + [d for a in 'yz' for d in cm.rings[a][1:] + (cm.opposite[a],)])

    first = jnp.where(c == 0, cm.y, cm.z)
    second = jnp.where(c == 0, cm.z, cm.y)
    start = first * 48 + jnp.minimum(second, 2) * 16
    piece = lambda d: x_ref.at[pl.ds(pl.multiple_of(d * 192 + start, 16), 16), :]
    together = cm.sems.pop()
    xs = [cm.send(piece(lax.rem(dm + k + 1, 8)), xg.at[c, first, second, x], dev, together) for k, dev in enumerate(peers)]
    gain_buf[0:3] = ga_ref[...].astype(F32)
    gain_buf[3:6] = gm_ref[...].astype(F32)
    gain_buf[6:8] = jnp.zeros((2, 128), F32)
    (i, r, o, l), dr, dl = cm.rings['x']
    dev_o = cm.other
    rows = lambda j: w_buf.at[j * 2 + c]
    ws = (wq_ref, wk_ref, wv_ref)
    lo, hi, full = pl.ds(0, 192), pl.ds(192, 192), pl.ds(0, 384)
    pieces = ((0, full), (1, lo), (1, hi), (2, full))
    a = [cm.send(ws[n].at[p], rows(i).at[n, p], dr) for n, p in pieces]
    b = [cm.send(ws[n].at[p], rows(i).at[n, p], dl) for n, p in pieces[::-1]]
    e = [cm.send(w, rows(i).at[n], dev_o) for n, w in enumerate(ws)]
    together = cm.sems.pop()
    gs = [cm.send(gain_buf, g_ref.at[dm], dev, together) for dev in peers]
    mine = [cm.local(w, w_buf.at[dm, n]) for n, w in enumerate(ws)]
    xs.append(cm.local(piece(dm), xg.at[c, first, second, x]))
    g_ref[dm] = gain_buf[...]
    cm.wait(*xs)

    def on(cps, src, ps, dev):
        f = []
        for cp, (n, p) in zip(cps, ps):
            cm.wait(cp)
            f.append(cm.send(rows(src).at[n, p], rows(src).at[n, p], dev))
        return f

    def rows_gather(k, small, big, where):
        yield from direct_gather(cm, small, where)
        yield from gather4(cm, big, lambda j: xg.at[k, j], lambda j, s: xg.at[k, j, :, 2 * s:2 * s + 2])

    gy = rows_gather(0, 'z', 'y', lambda j: xg.at[0, cm.y, j])
    gz = rows_gather(1, 'y', 'z', lambda j: xg.at[1, cm.z, j])
    for g in (gy, gz, gy, gz):
        next(g)
    f0 = on(a[:2], l, pieces[:2], dr)
    f1 = on(b[:2], r, pieces[::-1][:2], dl)
    run(gy, gz)
    cm.wait(*gs)
    total = jnp.zeros((192, 1), F32)
    for d in range(8):
        v = xg[d % 2, :, 0:3, d // 2].reshape(192, 384).astype(F32)
        total += jnp.sum(v * v, axis=1, keepdims=True)
    inv = lax.rsqrt(total / 3072 + EPSILON)
    for d in range(8):
        v = xg[d % 2, :, 0:3, d // 2].reshape(192, 384).astype(F32)
        n_buf[d] = (v * inv * (1.0 + gain_row(g_ref, d, 0))).astype(BF)
    def add(j, first=False):
        for n in range(3):
            part = jnp.dot(n_buf[j * 2], w_buf[j * 2, n], preferred_element_type=F32) + jnp.dot(n_buf[j * 2 + 1], w_buf[j * 2 + 1, n], preferred_element_type=F32)
            qkv_ref[n] = part if first else qkv_ref[n] + part

    cm.wait(*e, *mine)
    add(i, True)
    cm.wait(*a[2:])
    e1 = cm.send(rows(l), rows(l), dev_o)
    cm.wait(*b[2:])
    e2 = cm.send(rows(r), rows(r), dev_o)
    cm.wait(e1)
    add(l)
    cm.wait(e2)
    add(r)
    late = []
    for cp, (n, p) in zip(f0 + f1, pieces[:2] + pieces[:1:-1]):
        cm.wait(cp)
        late.append(cm.send(rows(o).at[n, p], rows(o).at[n, p], dev_o))
    cm.wait(*late)
    add(o)
    cm.drain()


def post_kernel(o_ref, x_ref, wo_ref, wg_ref, wu_ref, wd_ref, g_ref, u_out, v_out, o_buf, wo, x_o, wd, pa, pb, pc, pd, hs, ma, mb, acc_a, acc_b, w_gu, a_buf, u_buf, wait_buf, *rest):
    rx, rx2, sems = rest[:14], rest[14:35], rest[35:]
    cm = Comm(wait_buf, sems)
    x, c, y, z = cm.x, cm.c, cm.y, cm.z
    (i, r, o, l), dr, dl = cm.rings['x']
    dev_o = cm.other
    cm.barrier(cm.neighbours())

    o_buf[x] = o_ref[...]
    go = direct_gather(cm, 'x', lambda j: o_buf.at[j])
    next(go)
    row = lambda core: pl.multiple_of(192 * (2 * z + core) + 48 * y, 16)
    c_wo = cm.send(wo_ref, wo.at[c], dev_o)
    c_x = cm.send(x_ref.at[pl.ds(row(1 - c), 48), :], x_o, dev_o)
    c_wd = cm.send(wd_ref, wd.at[c], dev_o)
    wo[c] = wo_ref[...]
    own_wd = cm.local(wd_ref, wd.at[c])
    kblk = lambda j: pl.ds(pl.multiple_of((j * 2 + c) * 384, 16), 384)
    hcol = lambda j: pl.ds(pl.multiple_of(j * 384, 128), 384)

    def deal(w_ref, col, pause):
        to = pl.ds(col, 384)
        own = w_gu.at[kblk(i), to]
        cps = direct4(cm, 'x', lambda j: w_ref.at[:, hcol(j)], lambda k: own)
        here = [cm.local(w_ref.at[:, hcol(i)], own), cm.send(w_ref.at[:, hcol(i)], own, dev_o)]
        for _ in range(pause):
            yield
        for cp, j in zip(cps[1:] + cps[:1], (l, r, o)):
            cm.wait(cp)
            here.append(cm.send(w_gu.at[kblk(j), to], w_gu.at[kblk(j), to], dev_o))
        yield
        cm.wait(*here)

    def o_proj(j):
        v = o_buf[j]
        pa[j] = jnp.dot(v, wo[0], preferred_element_type=F32)
        pb[j] = jnp.dot(v, wo[1], preferred_element_type=F32)

    cm.wait(c_wo)
    o_proj(i)
    for _ in go:
        pass
    deal_g = deal(wg_ref, 0, 3)
    next(deal_g)
    for j in (r, o, l):
        o_proj(j)
    run(plane_scatter(cm, pa, 0, rx[:7]), plane_scatter(cm, pb, 1, rx[7:]), deal_g)

    cm.wait(c_x)
    mine, theirs = x_ref[pl.ds(row(c), 48), :].astype(F32), x_o[...].astype(F32)
    first = c == 0
    hs[x, 0] = (jnp.where(first, mine, theirs) + pa[z, rows48(y)]).astype(BF)
    hs[x, 1] = (jnp.where(first, theirs, mine) + pb[z, rows48(y)]).astype(BF)
    run(direct_gather(cm, 'x', lambda j: hs.at[j]))
    deal_u = deal(wu_ref, 384, 5)
    next(deal_u)
    total = jnp.zeros((48, 1), F32)
    for d in range(8):
        v = hs[d // 2, d % 2].astype(F32)
        total += jnp.sum(v * v, axis=1, keepdims=True)
    inv = lax.rsqrt(total / 3072 + EPSILON)
    for d in range(8):
        v = hs[d // 2, d % 2].astype(F32)
        (ma, mb)[d // 4][z, rows48(y, align=16), 384 * (d % 4):384 * (d % 4) + 384] = (v * inv * (1.0 + gain_row(g_ref, d, 1))).astype(BF)

    def part_a(j):
        acc_a[j] = jnp.dot(ma[j], w_gu[0:1536], preferred_element_type=F32)

    def part_b(j):
        acc_b[:, rows48(j)] = jnp.dot(mb[:, rows48(j, align=16)].reshape(192, 1536), w_gu[1536:3072], preferred_element_type=F32).reshape(4, 48, 768)

    run(deal_u, plane_stream(cm, ma, 0, part_a), plane_stream(cm, mb, 1, part_b))

    def hidden(j):
        s = acc_a[j] + acc_b[j]
        gate, up = s[:, 0:384], s[:, 384:768]
        gelu = 0.5 * gate * (1.0 + jnp.tanh(0.7978845608 * (gate + 0.044715 * (gate * gate * gate))))
        a_buf[j, :, hcol(x)] = (gelu * up).astype(BF)

    block = dict(zip('irol', cm.rings['z'][0]))
    y_ring = cm.rings['y'][0]
    ra, ra2, rb, rb2 = rx2[:12], rx2[12:15], rx2[15:18], rx2[18:21]
    right, left, fwd, first, second = {}, {}, {}, {}, {}

    def ship(name, via, dev):
        own = a_buf.at[block[name], :, hcol(x)]
        via[name] = cm.send(own, own, dev)

    def pass_on(name, via, frm, dev):
        cm.wait(via[name])
        src = a_buf.at[block[name], :, hcol(frm)]
        fwd[name] = cm.send(src, src, dev)

    def down(name):
        j = block[name]
        v = a_buf[j]
        pc[j] = jnp.dot(v, wd[0], preferred_element_type=F32)
        pd[j] = jnp.dot(v, wd[1], preferred_element_type=F32)
        k = 3 * 'orli'.index(name)
        first[name] = direct4(cm, 'y', lambda q: pc.at[j, rows48(q)], lambda q: ra[k + q], cm.sems.pop())

    def finish(name):
        cm.wait(*first[name])
        q = 3 * 'orli'.index(name)
        pc[block[name], rows48(y)] += (ra[q][...] + ra[q + 2][...]) + ra[q + 1][...]

    z_dev = {'o': cm.opposite['z'], 'r': cm.rings['z'][1], 'l': cm.rings['z'][2]}
    slot = {'o': 1, 'r': 0, 'l': 2}

    def send_z(name):
        j = block[name]
        second[name] = cm.send(pd.at[j], rb[slot[name]], z_dev[name])

    def send_z2(name):
        finish(name)
        second[name + '2'] = cm.send(pc.at[block[name], rows48(y)], ra2[slot[name]], z_dev[name])

    hidden(block['o'])
    ship('o', right, dr)
    hidden(block['r'])
    ship('r', left, dl)
    ship('o', left, dl)
    hidden(block['l'])
    ship('l', right, dr)
    hidden(block['i'])
    pass_on('o', right, l, dr)
    ship('r', right, dr)
    pass_on('r', left, r, dl)
    ship('i', left, dl)
    ship('l', left, dl)
    pass_on('l', right, l, dr)
    ship('i', right, dr)
    cm.wait(c_wd, own_wd, left['o'], fwd['o'])
    down('o')
    send_z('o')
    cm.wait(right['r'], fwd['r'])
    pass_on('i', left, r, dl)
    down('r')
    send_z('r')
    cm.wait(left['l'], fwd['l'])
    down('l')
    send_z('l')
    send_z2('o')
    send_z2('r')
    cm.wait(right['i'], fwd['i'])
    down('i')
    cm.wait(second['o'], second['r'], second['l'])
    pd[z] += (rb[0][...] + rb[2][...]) + rb[1][...]
    last = direct_scatter(cm, 'y', lambda q: pd.at[z, rows48(q)], rb2)
    next(last)
    send_z2('l')
    finish('i')
    cm.wait(second['o2'], second['r2'], second['l2'])
    pc[z, rows48(y)] += (ra2[0][...] + ra2[2][...]) + ra2[1][...]
    at = rows48(y, align=16)
    u_buf[0, z, at] = (hs[x, 0].astype(F32) + pc[z, rows48(y)]).astype(BF)
    half0 = plane_burst(cm, u_buf.at[0], 0)
    next(half0)
    run(last)
    u_buf[1, z, at] = (hs[x, 1].astype(F32) + pd[z, rows48(y)]).astype(BF)
    half1 = plane_burst(cm, u_buf.at[1], 1)
    next(half1)
    run(half0, half1)
    c_v = cm.send(u_buf.at[1 - c], v_out, dev_o)
    u_out[...] = u_buf[c]
    cm.wait(c_v)
    cm.drain()


def rope_table():
    inv_freq = np.float32(ROPE_THETA) ** (np.float32(-2.0) * np.arange(128, dtype=np.float32) / np.float32(256))
    angles = np.arange(16, dtype=np.float32)[:, None] * inv_freq[None, :].astype(np.float32)
    return np.stack([np.cos(angles), np.sin(angles)]).astype(np.float32)


def attend_kernel(qkv_ref, kc_ref, vc_ref, len_ref, tab_ref, o_ref, ku_ref, vu_ref):
    step = o_ref.shape[0]
    at = pl.ds(pl.multiple_of(pl.program_id(0) * step, step), step)
    pos = len_ref[at, :]
    cos = jnp.zeros((step, 128), F32)
    sin = jnp.zeros((step, 128), F32)
    for t in range(16):
        cos = jnp.where(pos == t, tab_ref[0, t:t + 1], cos)
        sin = jnp.where(pos == t, tab_ref[1, t:t + 1], sin)

    def rope(n):
        lo, hi = qkv_ref[n, at, 0:128], qkv_ref[n, at, 128:256]
        return lo * cos - hi * sin, hi * cos + lo * sin

    tall = lambda a: a.reshape(step, 1, 128)
    rounded = lambda a: a.astype(BF).astype(F32)
    q = [tall(rounded(a * 256 ** -0.5)) for a in rope(0)]
    k_new = [tall(rounded(a)) for a in rope(1)]
    v_new = [tall(rounded(qkv_ref[2, at, 128 * n:128 * n + 128])) for n in range(2)]
    slot = lax.broadcasted_iota(jnp.int32, (step, 16, 128), 1)
    pos3 = pos.reshape(step, 1, 128)
    hit = slot == pos3
    prod = None
    for n in range(2):
        lanes = slice(128 * n, 128 * n + 128)
        k = jnp.where(hit, k_new[n], kc_ref[at, :, lanes].astype(F32))
        ku_ref[:, :, lanes] = k.astype(BF)
        prod = k * q[n] if prod is None else prod + k * q[n]
    score = jnp.sum(prod, axis=2, keepdims=True)
    valid = (slot <= pos3)[:, :, 0:1]
    score = jnp.where(valid, score, -1e30)
    e = jnp.exp(score - jnp.max(score, axis=1, keepdims=True))
    p = rounded(e / jnp.sum(e, axis=1, keepdims=True))
    for n in range(2):
        lanes = slice(128 * n, 128 * n + 128)
        v = jnp.where(hit, v_new[n], vc_ref[at, :, lanes].astype(F32))
        vu_ref[:, :, lanes] = v.astype(BF)
        o_ref[:, lanes] = jnp.sum(p * v, axis=1).astype(BF)


VM = pl.BlockSpec(memory_space=pltpu.VMEM)


HB = pl.BlockSpec(memory_space=pltpu.HBM)


def call(body, outs, scratch, sems, cid, limit, flops, where, *args):
    single = len(outs) == 1
    return pl.pallas_call(
        body,
        out_shape=outs[0] if single else outs,
        in_specs=[HB if w == 'h' else VM for w in where],
        out_specs=VM if single else [VM] * len(outs),
        scratch_shapes=scratch + [pltpu.SemaphoreType.DMA] * sems,
        compiler_params=pltpu.CompilerParams(collective_id=cid, has_side_effects=True, vmem_limit_bytes=limit * 2**20),
        cost_estimate=pl.CostEstimate(flops=flops, bytes_accessed=8_000_000, transcendentals=0),
    )(*args)


def call2(body, outs, scratch, sems, cid, limit, flops, where, *args):
    single = len(outs) == 1
    return pl.pallas_call(
        body,
        out_shape=outs[0] if single else outs,
        in_specs=[HB if w == 'h' else VM for w in where],
        out_specs=VM if single else [VM] * len(outs),
        scratch_shapes=scratch + [pltpu.SemaphoreType.DMA] * sems,
        compiler_params=pltpu.CompilerParams(collective_id=cid, has_side_effects=True, vmem_limit_bytes=limit * 2**20),
        cost_estimate=pl.CostEstimate(flops=flops, bytes_accessed=8_000_000, transcendentals=0),
    )(*args)


def join_kernel(u_ref, v_ref, out_ref):
    c = lax.rem(lax.axis_index('dm'), 2)
    for j in range(4):
        out_ref[pl.ds(pl.multiple_of(192 * (2 * j + c), 16), 192), :] = u_ref[j]
        out_ref[pl.ds(pl.multiple_of(192 * (2 * j + 1 - c), 16), 192), :] = v_ref[j]


def solution(mesh):
    cache_spec = P(('dp', 'dm'), 'tp', None, None)
    resid_spec = P('dp', 'dm')
    col_spec = P('dm', 'tp')
    row_spec = P('tp', 'dm')
    in_specs = (resid_spec, cache_spec, cache_spec, P('dp'), P('dm'), col_spec, col_spec, col_spec, row_spec, P('dm'), col_spec, col_spec, row_spec)
    out_specs = (resid_spec, cache_spec, cache_spec)
    sds = jax.ShapeDtypeStruct
    V = pltpu.VMEM

    def local_step(resid_in, k_cache, v_cache, cache_len, norm_attn, w_q, w_k, w_v, w_o, norm_mlp, w_gate, w_up, w_down):
        qkv, gain_all = call(
            qkv_kernel,
            (sds((3, 192, 256), F32), sds((8, 8, 128), F32)),
            [V((8, 3, 384, 256), BF), V((2, 4, 4, 4, 16, 384), BF), V((8, 192, 384), BF), V((8, 128), F32), V((8192, 128), BF)],
            40, 0, 58, 2 * 10**9, 'hhhhvv',
            resid_in, w_q, w_k, w_v, norm_attn.reshape(3, 128), norm_mlp.reshape(3, 128))
        lengths = lax.dynamic_slice_in_dim(cache_len, lax.axis_index('dm') * 192, 192)
        cache, step = sds((192, 16, 256), BF), 48
        attn_out, k_upd, v_upd = pl.pallas_call(
            attend_kernel, name='attend', out_shape=(sds((192, 256), BF), cache, cache), grid=(192 // step,), in_specs=[VM] * 5,
            out_specs=[pl.BlockSpec((step, 256), lambda b: (b, 0))] + [pl.BlockSpec((step, 16, 256), lambda b: (b, 0, 0))] * 2,
            compiler_params=pltpu.CompilerParams(vmem_limit_bytes=20 * 2**20),
        )(qkv, k_cache.reshape(192, 16, 256), v_cache.reshape(192, 16, 256), jnp.broadcast_to(lengths[:, None], (192, 128)), jnp.asarray(rope_table()))
        k_upd, v_upd = k_upd.reshape(192, 1, 16, 256), v_upd.reshape(192, 1, 16, 256)
        mine, theirs = call2(
            post_kernel,
            (sds((4, 192, 384), BF), sds((4, 192, 384), BF)),
            [V((4, 192, 256), BF), V((2, 256, 384), BF), V((48, 384), BF), V((2, 1536, 384), BF)]
            + [V((4, 192, 384), F32)] * 4 + [V((4, 2, 48, 384), BF)] + [V((4, 192, 1536), BF)] * 2 + [V((4, 192, 768), F32)] * 2
            + [V((3072, 768), BF), V((4, 192, 1536), BF), V((2, 4, 192, 384), BF), V((16384, 128), BF)]
            + scatter_scratch() + [V((48, 384), F32)] * 15 + [V((192, 384), F32)] * 3 + [V((48, 384), F32)] * 3,
            93, 1, 44, 7 * 10**9, 'vvvhhhv',
            attn_out, resid_in, w_o, w_gate, w_up, w_down, gain_all)
        resid_out = pl.pallas_call(join_kernel, out_shape=sds((1536, 384), BF), in_specs=[VM, VM], out_specs=VM, compiler_params=pltpu.CompilerParams(vmem_limit_bytes=8 * 2**20))(mine, theirs)
        return resid_out, k_upd, v_upd

    return jax.shard_map(local_step, mesh=mesh, in_specs=in_specs, out_specs=out_specs, check_vma=False)
```

```python
import math

import jax
import jax.numpy as jnp
import numpy as np
from jax import lax
from jax.experimental import pallas as pl
from jax.experimental.pallas import tpu as pltpu
from jax.sharding import PartitionSpec as P

EPSILON = 1e-6
ROPE_THETA = 10000.0
BF = jnp.bfloat16
F32 = jnp.float32
LOGICAL = pl.DeviceIdType.LOGICAL


class Comm:
    def __init__(self, wait_buf, sems):
        self.wait_buf, self.sems = wait_buf, list(sems)
        self.groups = []
        tp, dm = lax.axis_index('tp'), lax.axis_index('dm')
        self.tp, self.dm = tp, dm
        self.z, self.y = lax.div(tp, 4), lax.rem(tp, 4)
        self.x, self.c = lax.div(dm, 2), lax.rem(dm, 2)
        self.other = tp * 8 + self.x * 2 + 1 - self.c
        self.rings, self.opposite = {}, {}
        for axis, me, base, step in (('x', self.x, tp * 8 + self.c, 2), ('y', self.y, self.z * 32 + dm, 8), ('z', self.z, self.y * 8 + dm, 32)):
            idx = [me] + [lax.rem(me + k, 4) for k in (1, 2, 3)]
            self.rings[axis] = idx, base + idx[1] * step, base + idx[3] * step
            self.opposite[axis] = base + idx[2] * step

    def neighbours(self):
        return [self.other] + [d for r in self.rings.values() for d in r[1:]] + list(self.opposite.values())

    def barrier(self, peers):
        sem = pltpu.get_barrier_semaphore()
        for dev in peers:
            pl.semaphore_signal(sem, inc=1, device_id=dev, device_id_type=LOGICAL)
        pl.semaphore_wait(sem, len(peers))

    def send(self, src, dst, dev, recv=None):
        rows = math.prod(dst.shape) * dst.dtype.itemsize // 256
        if not self.groups or self.groups[-1][1] + rows > self.wait_buf.shape[0]:
            self.groups.append([self.sems.pop(), 0])
        self.groups[-1][1] += rows
        recv = self.sems.pop() if recv is None else recv
        pltpu.make_async_remote_copy(src_ref=src, dst_ref=dst, send_sem=self.groups[-1][0], recv_sem=recv, device_id=dev, device_id_type=LOGICAL).start()
        return recv, rows

    def wait(self, *copies):
        total = {}
        for sem, rows in copies:
            total[id(sem)] = sem, total.get(id(sem), (sem, 0))[1] + rows
        for sem, rows in total.values():
            part = self.wait_buf.at[0:rows]
            pltpu.make_async_copy(part, part, sem).wait()

    def local(self, src, dst):
        rows = math.prod(dst.shape) * dst.dtype.itemsize // 256
        sem = self.sems.pop()
        pltpu.make_async_copy(src, dst, sem).start()
        return sem, rows

    def drain(self):
        assert not self.sems, len(self.sems)
        self.wait(*self.groups)


def run(*gens):
    gens = list(gens)
    while gens:
        for g in list(gens):
            try:
                next(g)
            except StopIteration:
                gens.remove(g)


def gather4(cm, axis, blk, hf, fine=True):
    (i, r, o, l), dr, dl = cm.rings[axis]
    if fine:
        a0 = cm.send(hf(i, 0), hf(i, 0), dr)
        b1 = cm.send(hf(i, 1), hf(i, 1), dl)
        a1 = cm.send(hf(i, 1), hf(i, 1), dr)
        b0 = cm.send(hf(i, 0), hf(i, 0), dl, a1[0])
        late = (a1, b0)
    else:
        a0 = cm.send(blk(i), blk(i), dr)
        b1 = cm.send(blk(i), blk(i), dl)
        late = ()
    yield
    cm.wait(a0)
    c = cm.send(hf(l, 0), hf(l, 0), dr)
    cm.wait(b1)
    d = cm.send(hf(r, 1), hf(r, 1), dl, c[0])
    yield
    cm.wait(*late)
    yield
    cm.wait(c, d)


def direct4(cm, axis, src, dst, recv=None):
    (i, r, o, l), dr, dl = cm.rings[axis]
    return [cm.send(src(o), dst(1), cm.opposite[axis], recv), cm.send(src(r), dst(0), dr, recv), cm.send(src(l), dst(2), dl, recv)]


def direct_gather(cm, axis, blk):
    own = blk(cm.rings[axis][0][0])
    cps = direct4(cm, axis, lambda j: own, lambda k: own, cm.sems.pop())
    yield
    cm.wait(*cps)


def direct_scatter(cm, axis, blk, rx):
    cps = direct4(cm, axis, blk, lambda k: rx[k], cm.sems.pop())
    yield
    cm.wait(*cps)
    blk(cm.rings[axis][0][0])[...] += (rx[0][...] + rx[2][...]) + rx[1][...]


def scatter4(cm, axis, blk, hf, rx, hrx):
    (i, r, o, l), dr, dl = cm.rings[axis]
    ro0, ro1, rl, rr = rx
    c0 = cm.send(hf(o, 0), ro0, dr)
    c1 = cm.send(hf(o, 1), ro1, dl)
    c2 = cm.send(hf(r, 1), hrx(rl, 1), dr)
    c3 = cm.send(hf(l, 0), hrx(rr, 0), dl, c2[0])
    yield
    cm.wait(c0)
    hf(r, 0)[...] += ro0[...]
    c4 = cm.send(hf(r, 0), hrx(rl, 0), dr, c2[0])
    cm.wait(c1)
    hf(l, 1)[...] += ro1[...]
    c5 = cm.send(hf(l, 1), hrx(rr, 1), dl, c2[0])
    yield
    cm.wait(c2, c3, c4, c5)
    blk(i)[...] += rl[...] + rr[...]


def rows48(j, start=0, size=48, align=8):
    return pl.ds(pl.multiple_of(j * 48 + start, align), size)


def plane_scatter(cm, p, h, rx):
    y = (lambda j: p.at[:, rows48(j)]), (lambda j, s: p.at[2 * s:2 * s + 2, rows48(j)]), rx[:4], (lambda b, s: b.at[2 * s:2 * s + 2])
    z = (lambda j: p.at[j]), (lambda j, s: p.at[j, 96 * s:96 * s + 96]), rx[:4], (lambda b, s: b.at[96 * s:96 * s + 96])
    if h == 0:
        yield from scatter4(cm, 'y', *y)
        yield from direct_scatter(cm, 'z', lambda j: p.at[j, rows48(cm.y)], rx[4:])
    else:
        yield from scatter4(cm, 'z', *z)
        yield from direct_scatter(cm, 'y', lambda j: p.at[cm.z, rows48(j)], rx[4:])


def scatter_scratch():
    V = pltpu.VMEM
    small = [V((48, 384), F32)] * 3
    return [V((2, 48, 384), F32)] * 2 + [V((4, 48, 384), F32)] * 2 + small + [V((96, 384), F32)] * 2 + [V((192, 384), F32)] * 2 + small


def plane_burst(cm, m, h):
    at = lambda j: rows48(j, align=16)
    first, second = ('y', 'z') if h == 0 else ('z', 'y')
    piece = (lambda k: m.at[cm.z, at(k)]) if h == 0 else (lambda k: m.at[k, at(cm.y)])
    ki, kr, ko, kl = cm.rings[first][0]
    recv = cm.sems.pop()
    outs = []

    def out(k):
        outs.extend(direct4(cm, second, lambda j: piece(k), lambda q: piece(k), recv))

    small = direct4(cm, first, lambda j: piece(ki), lambda k: piece(ki))
    out(ki)
    yield
    cm.wait(small[1])
    out(kl)
    cm.wait(small[2])
    out(kr)
    yield
    cm.wait(small[0])
    out(ko)
    yield
    cm.wait(*outs)


def plane_stream(cm, m, h, near):
    at = lambda j: rows48(j, align=16)
    first, second = ('y', 'z') if h == 0 else ('z', 'y')
    piece = (lambda b, k: m.at[b, at(k)]) if h == 0 else (lambda b, k: m.at[k, at(b)])
    ki, kr, ko, kl = cm.rings[first][0]
    (i, r, o, l), dr, dl = cm.rings[second]
    right, left = {}, {}

    def out(name, k):
        right[name] = cm.send(piece(i, k), piece(i, k), dr)
        left[name] = cm.send(piece(i, k), piece(i, k), dl)

    small = direct4(cm, first, lambda j: piece(i, ki), lambda k: piece(i, ki))
    yield
    out('i', ki)
    yield
    cm.wait(small[1])
    out('l', kl)
    cm.wait(small[2])
    out('r', kr)
    yield
    cm.wait(small[0])
    out('o', ko)
    yield
    cm.wait(right['i'])
    fr = [cm.send(piece(l, ki), piece(l, ki), dr)]
    cm.wait(left['i'])
    yield
    near(i)
    yield
    cm.wait(right['l'])
    fr.append(cm.send(piece(l, kl), piece(l, kl), dr, fr[0][0]))
    cm.wait(left['l'], left['r'])
    fl = [cm.send(piece(r, kr), piece(r, kr), dl)]
    yield
    cm.wait(left['o'])
    fl.append(cm.send(piece(r, ko), piece(r, ko), dl, fl[0][0]))
    cm.wait(right['r'], right['o'])
    yield
    near(l)
    near(r)
    yield
    cm.wait(*fr, *fl)
    near(o)


def gain_row(g_ref, d, k):
    g = g_ref[d]
    return jnp.concatenate([g[3 * k + j:3 * k + j + 1] for j in range(3)], axis=1)


def qkv_kernel(x_ref, wq_ref, wk_ref, wv_ref, ga_ref, gm_ref, qkv_ref, g_ref, w_buf, xg, n_buf, gain_buf, wait_buf, *sems):
    cm = Comm(wait_buf, sems)
    x, c, dm = cm.x, cm.c, cm.dm
    peers = [cm.tp * 8 + lax.rem(dm + k, 8) for k in range(1, 8)]
    cm.barrier(peers + [d for a in 'yz' for d in cm.rings[a][1:] + (cm.opposite[a],)])

    first = jnp.where(c == 0, cm.y, cm.z)
    second = jnp.where(c == 0, cm.z, cm.y)
    start = first * 48 + jnp.minimum(second, 2) * 16
    piece = lambda d: x_ref.at[pl.ds(pl.multiple_of(d * 192 + start, 16), 16), :]
    together = cm.sems.pop()
    xs = [cm.send(piece(lax.rem(dm + k + 1, 8)), xg.at[c, first, second, x], dev, together) for k, dev in enumerate(peers)]
    gain_buf[0:3] = ga_ref[...].astype(F32)
    gain_buf[3:6] = gm_ref[...].astype(F32)
    gain_buf[6:8] = jnp.zeros((2, 128), F32)
    (i, r, o, l), dr, dl = cm.rings['x']
    dev_o = cm.other
    rows = lambda j: w_buf.at[j * 2 + c]
    ws = (wq_ref, wk_ref, wv_ref)
    lo, hi, full = pl.ds(0, 192), pl.ds(192, 192), pl.ds(0, 384)
    pieces = ((0, full), (1, lo), (1, hi), (2, full))
    a = [cm.send(ws[n].at[p], rows(i).at[n, p], dr) for n, p in pieces]
    b = [cm.send(ws[n].at[p], rows(i).at[n, p], dl) for n, p in pieces[::-1]]
    e = [cm.send(w, rows(i).at[n], dev_o) for n, w in enumerate(ws)]
    together = cm.sems.pop()
    gs = [cm.send(gain_buf, g_ref.at[dm], dev, together) for dev in peers]
    mine = [cm.local(w, w_buf.at[dm, n]) for n, w in enumerate(ws)]
    xs.append(cm.local(piece(dm), xg.at[c, first, second, x]))
    g_ref[dm] = gain_buf[...]
    cm.wait(*xs)

    def on(cps, src, ps, dev):
        f = []
        for cp, (n, p) in zip(cps, ps):
            cm.wait(cp)
            f.append(cm.send(rows(src).at[n, p], rows(src).at[n, p], dev))
        return f

    def rows_gather(k, small, big, where):
        yield from direct_gather(cm, small, where)
        yield from gather4(cm, big, lambda j: xg.at[k, j], lambda j, s: xg.at[k, j, :, 2 * s:2 * s + 2])

    gy = rows_gather(0, 'z', 'y', lambda j: xg.at[0, cm.y, j])
    gz = rows_gather(1, 'y', 'z', lambda j: xg.at[1, cm.z, j])
    for g in (gy, gz, gy, gz):
        next(g)
    f0 = on(a[:2], l, pieces[:2], dr)
    f1 = on(b[:2], r, pieces[::-1][:2], dl)
    run(gy, gz)
    cm.wait(*gs)
    total = jnp.zeros((192, 1), F32)
    for d in range(8):
        v = xg[d % 2, :, 0:3, d // 2].reshape(192, 384).astype(F32)
        total += jnp.sum(v * v, axis=1, keepdims=True)
    inv = lax.rsqrt(total / 3072 + EPSILON)
    for d in range(8):
        v = xg[d % 2, :, 0:3, d // 2].reshape(192, 384).astype(F32)
        n_buf[d] = (v * inv * (1.0 + gain_row(g_ref, d, 0))).astype(BF)
    def add(j, first=False):
        for n in range(3):
            part = jnp.dot(n_buf[j * 2], w_buf[j * 2, n], preferred_element_type=F32) + jnp.dot(n_buf[j * 2 + 1], w_buf[j * 2 + 1, n], preferred_element_type=F32)
            qkv_ref[n] = part if first else qkv_ref[n] + part

    cm.wait(*e, *mine)
    add(i, True)
    cm.wait(*a[2:])
    e1 = cm.send(rows(l), rows(l), dev_o)
    cm.wait(*b[2:])
    e2 = cm.send(rows(r), rows(r), dev_o)
    cm.wait(e1)
    add(l)
    cm.wait(e2)
    add(r)
    late = []
    for cp, (n, p) in zip(f0 + f1, pieces[:2] + pieces[:1:-1]):
        cm.wait(cp)
        late.append(cm.send(rows(o).at[n, p], rows(o).at[n, p], dev_o))
    cm.wait(*late)
    add(o)
    cm.drain()


def post_kernel(o_ref, x_ref, wo_ref, wg_ref, wu_ref, wd_ref, g_ref, u_out, v_out, o_buf, wo, x_o, wd, pa, pb, pc, pd, hs, ma, mb, acc_a, acc_b, w_gu, a_buf, u_buf, wait_buf, *rest):
    rx, rx2, sems = rest[:14], rest[14:35], rest[35:]
    cm = Comm(wait_buf, sems)
    x, c, y, z = cm.x, cm.c, cm.y, cm.z
    (i, r, o, l), dr, dl = cm.rings['x']
    dev_o = cm.other
    cm.barrier(cm.neighbours())

    o_buf[x] = o_ref[...]
    go = direct_gather(cm, 'x', lambda j: o_buf.at[j])
    next(go)
    row = lambda core: pl.multiple_of(192 * (2 * z + core) + 48 * y, 16)
    c_wo = cm.send(wo_ref, wo.at[c], dev_o)
    c_x = cm.send(x_ref.at[pl.ds(row(1 - c), 48), :], x_o, dev_o)
    c_wd = cm.send(wd_ref, wd.at[c], dev_o)
    wo[c] = wo_ref[...]
    own_wd = cm.local(wd_ref, wd.at[c])
    kblk = lambda j: pl.ds(pl.multiple_of((j * 2 + c) * 384, 16), 384)
    hcol = lambda j: pl.ds(pl.multiple_of(j * 384, 128), 384)

    def deal(w_ref, col, pause):
        to = pl.ds(col, 384)
        own = w_gu.at[kblk(i), to]
        cps = direct4(cm, 'x', lambda j: w_ref.at[:, hcol(j)], lambda k: own)
        here = [cm.local(w_ref.at[:, hcol(i)], own), cm.send(w_ref.at[:, hcol(i)], own, dev_o)]
        for _ in range(pause):
            yield
        for cp, j in zip(cps[1:] + cps[:1], (l, r, o)):
            cm.wait(cp)
            here.append(cm.send(w_gu.at[kblk(j), to], w_gu.at[kblk(j), to], dev_o))
        yield
        cm.wait(*here)

    def o_proj(j):
        v = o_buf[j]
        pa[j] = jnp.dot(v, wo[0], preferred_element_type=F32)
        pb[j] = jnp.dot(v, wo[1], preferred_element_type=F32)

    cm.wait(c_wo)
    o_proj(i)
    for _ in go:
        pass
    deal_g = deal(wg_ref, 0, 3)
    next(deal_g)
    for j in (r, o, l):
        o_proj(j)
    run(plane_scatter(cm, pa, 0, rx[:7]), plane_scatter(cm, pb, 1, rx[7:]), deal_g)

    cm.wait(c_x)
    mine, theirs = x_ref[pl.ds(row(c), 48), :].astype(F32), x_o[...].astype(F32)
    first = c == 0
    hs[x, 0] = (jnp.where(first, mine, theirs) + pa[z, rows48(y)]).astype(BF)
    hs[x, 1] = (jnp.where(first, theirs, mine) + pb[z, rows48(y)]).astype(BF)
    run(direct_gather(cm, 'x', lambda j: hs.at[j]))
    deal_u = deal(wu_ref, 384, 5)
    next(deal_u)
    total = jnp.zeros((48, 1), F32)
    for d in range(8):
        v = hs[d // 2, d % 2].astype(F32)
        total += jnp.sum(v * v, axis=1, keepdims=True)
    inv = lax.rsqrt(total / 3072 + EPSILON)
    for d in range(8):
        v = hs[d // 2, d % 2].astype(F32)
        (ma, mb)[d // 4][z, rows48(y, align=16), 384 * (d % 4):384 * (d % 4) + 384] = (v * inv * (1.0 + gain_row(g_ref, d, 1))).astype(BF)

    def part_a(j):
        acc_a[j] = jnp.dot(ma[j], w_gu[0:1536], preferred_element_type=F32)

    def part_b(j):
        acc_b[:, rows48(j)] = jnp.dot(mb[:, rows48(j, align=16)].reshape(192, 1536), w_gu[1536:3072], preferred_element_type=F32).reshape(4, 48, 768)

    run(deal_u, plane_stream(cm, ma, 0, part_a), plane_stream(cm, mb, 1, part_b))

    def hidden(j):
        s = acc_a[j] + acc_b[j]
        gate, up = s[:, 0:384], s[:, 384:768]
        gelu = 0.5 * gate * (1.0 + jnp.tanh(0.7978845608 * (gate + 0.044715 * (gate * gate * gate))))
        a_buf[j, :, hcol(x)] = (gelu * up).astype(BF)

    block = dict(zip('irol', cm.rings['z'][0]))
    y_ring = cm.rings['y'][0]
    ra, ra2, rb, rb2 = rx2[:12], rx2[12:15], rx2[15:18], rx2[18:21]
    right, left, fwd, first, second = {}, {}, {}, {}, {}

    def ship(name, via, dev):
        own = a_buf.at[block[name], :, hcol(x)]
        via[name] = cm.send(own, own, dev)

    def pass_on(name, via, frm, dev):
        cm.wait(via[name])
        src = a_buf.at[block[name], :, hcol(frm)]
        fwd[name] = cm.send(src, src, dev)

    def down(name):
        j = block[name]
        v = a_buf[j]
        pc[j] = jnp.dot(v, wd[0], preferred_element_type=F32)
        pd[j] = jnp.dot(v, wd[1], preferred_element_type=F32)
        k = 3 * 'orli'.index(name)
        first[name] = direct4(cm, 'y', lambda q: pc.at[j, rows48(q)], lambda q: ra[k + q], cm.sems.pop())

    def finish(name):
        cm.wait(*first[name])
        q = 3 * 'orli'.index(name)
        pc[block[name], rows48(y)] += (ra[q][...] + ra[q + 2][...]) + ra[q + 1][...]

    z_dev = {'o': cm.opposite['z'], 'r': cm.rings['z'][1], 'l': cm.rings['z'][2]}
    slot = {'o': 1, 'r': 0, 'l': 2}

    def send_z(name):
        j = block[name]
        second[name] = cm.send(pd.at[j], rb[slot[name]], z_dev[name])

    def send_z2(name):
        finish(name)
        second[name + '2'] = cm.send(pc.at[block[name], rows48(y)], ra2[slot[name]], z_dev[name])

    hidden(block['o'])
    ship('o', right, dr)
    hidden(block['r'])
    ship('r', left, dl)
    ship('o', left, dl)
    hidden(block['l'])
    ship('l', right, dr)
    hidden(block['i'])
    pass_on('o', right, l, dr)
    ship('r', right, dr)
    pass_on('r', left, r, dl)
    ship('i', left, dl)
    ship('l', left, dl)
    pass_on('l', right, l, dr)
    ship('i', right, dr)
    cm.wait(c_wd, own_wd, left['o'], fwd['o'])
    down('o')
    send_z('o')
    cm.wait(right['r'], fwd['r'])
    pass_on('i', left, r, dl)
    down('r')
    send_z('r')
    cm.wait(left['l'], fwd['l'])
    down('l')
    y_row = dict(zip('irol', y_ring))
    third = {q: cm.send(pd.at[block['l'], rows48(y_row[q])], rb[2].at[rows48(y_row[q])], z_dev['l']) for q in 'orli'}
    send_z2('o')
    send_z2('r')
    cm.wait(right['i'], fwd['i'])
    down('i')
    cm.wait(second['o'], second['r'])
    pd[z] += rb[0][...] + rb[1][...]
    y_dev = {'o': cm.opposite['y'], 'r': cm.rings['y'][1], 'l': cm.rings['y'][2]}
    recv = cm.sems.pop()
    last = []

    def third_piece(q):
        cm.wait(third[q])
        pd[z, rows48(y_row[q])] += rb[2][rows48(y_row[q]), :]
        if q != 'i':
            last.append(cm.send(pd.at[z, rows48(y_row[q])], rb2[slot[q]], y_dev[q], recv))

    third_piece('o')
    third_piece('r')
    send_z2('l')
    third_piece('l')
    third_piece('i')
    finish('i')
    cm.wait(second['o2'], second['r2'], second['l2'])
    pc[z, rows48(y)] += (ra2[0][...] + ra2[2][...]) + ra2[1][...]
    at = rows48(y, align=16)
    u_buf[0, z, at] = (hs[x, 0].astype(F32) + pc[z, rows48(y)]).astype(BF)
    half0 = plane_burst(cm, u_buf.at[0], 0)
    next(half0)
    cm.wait(*last)
    pd[z, rows48(y)] += (rb2[0][...] + rb2[2][...]) + rb2[1][...]
    u_buf[1, z, at] = (hs[x, 1].astype(F32) + pd[z, rows48(y)]).astype(BF)
    half1 = plane_burst(cm, u_buf.at[1], 1)
    next(half1)
    run(half0, half1)
    c_v = cm.send(u_buf.at[1 - c], v_out, dev_o)
    u_out[...] = u_buf[c]
    cm.wait(c_v)
    cm.drain()


def rope_table():
    inv_freq = np.float32(ROPE_THETA) ** (np.float32(-2.0) * np.arange(128, dtype=np.float32) / np.float32(256))
    angles = np.arange(16, dtype=np.float32)[:, None] * inv_freq[None, :].astype(np.float32)
    return np.stack([np.cos(angles), np.sin(angles)]).astype(np.float32)


def attend_kernel(qkv_ref, kc_ref, vc_ref, len_ref, tab_ref, o_ref, ku_ref, vu_ref):
    step = o_ref.shape[0]
    at = pl.ds(pl.multiple_of(pl.program_id(0) * step, step), step)
    pos = len_ref[at, :]
    cos = jnp.zeros((step, 128), F32)
    sin = jnp.zeros((step, 128), F32)
    for t in range(16):
        cos = jnp.where(pos == t, tab_ref[0, t:t + 1], cos)
        sin = jnp.where(pos == t, tab_ref[1, t:t + 1], sin)

    def rope(n):
        lo, hi = qkv_ref[n, at, 0:128], qkv_ref[n, at, 128:256]
        return lo * cos - hi * sin, hi * cos + lo * sin

    tall = lambda a: a.reshape(step, 1, 128)
    rounded = lambda a: a.astype(BF).astype(F32)
    q = [tall(rounded(a * 256 ** -0.5)) for a in rope(0)]
    k_new = [tall(rounded(a)) for a in rope(1)]
    v_new = [tall(rounded(qkv_ref[2, at, 128 * n:128 * n + 128])) for n in range(2)]
    slot = lax.broadcasted_iota(jnp.int32, (step, 16, 128), 1)
    pos3 = pos.reshape(step, 1, 128)
    hit = slot == pos3
    prod = None
    for n in range(2):
        lanes = slice(128 * n, 128 * n + 128)
        k = jnp.where(hit, k_new[n], kc_ref[at, :, lanes].astype(F32))
        ku_ref[:, :, lanes] = k.astype(BF)
        prod = k * q[n] if prod is None else prod + k * q[n]
    score = jnp.sum(prod, axis=2, keepdims=True)
    valid = (slot <= pos3)[:, :, 0:1]
    score = jnp.where(valid, score, -1e30)
    e = jnp.exp(score - jnp.max(score, axis=1, keepdims=True))
    p = rounded(e / jnp.sum(e, axis=1, keepdims=True))
    for n in range(2):
        lanes = slice(128 * n, 128 * n + 128)
        v = jnp.where(hit, v_new[n], vc_ref[at, :, lanes].astype(F32))
        vu_ref[:, :, lanes] = v.astype(BF)
        o_ref[:, lanes] = jnp.sum(p * v, axis=1).astype(BF)


VM = pl.BlockSpec(memory_space=pltpu.VMEM)


HB = pl.BlockSpec(memory_space=pltpu.HBM)


def call(body, outs, scratch, sems, cid, limit, flops, where, *args):
    single = len(outs) == 1
    return pl.pallas_call(
        body,
        out_shape=outs[0] if single else outs,
        in_specs=[HB if w == 'h' else VM for w in where],
        out_specs=VM if single else [VM] * len(outs),
        scratch_shapes=scratch + [pltpu.SemaphoreType.DMA] * sems,
        compiler_params=pltpu.CompilerParams(collective_id=cid, has_side_effects=True, vmem_limit_bytes=limit * 2**20),
        cost_estimate=pl.CostEstimate(flops=flops, bytes_accessed=8_000_000, transcendentals=0),
    )(*args)


def call2(body, outs, scratch, sems, cid, limit, flops, where, *args):
    single = len(outs) == 1
    return pl.pallas_call(
        body,
        out_shape=outs[0] if single else outs,
        in_specs=[HB if w == 'h' else VM for w in where],
        out_specs=VM if single else [VM] * len(outs),
        scratch_shapes=scratch + [pltpu.SemaphoreType.DMA] * sems,
        compiler_params=pltpu.CompilerParams(collective_id=cid, has_side_effects=True, vmem_limit_bytes=limit * 2**20),
        cost_estimate=pl.CostEstimate(flops=flops, bytes_accessed=8_000_000, transcendentals=0),
    )(*args)


def join_kernel(u_ref, v_ref, out_ref):
    c = lax.rem(lax.axis_index('dm'), 2)
    for j in range(4):
        out_ref[pl.ds(pl.multiple_of(192 * (2 * j + c), 16), 192), :] = u_ref[j]
        out_ref[pl.ds(pl.multiple_of(192 * (2 * j + 1 - c), 16), 192), :] = v_ref[j]


def solution(mesh):
    cache_spec = P(('dp', 'dm'), 'tp', None, None)
    resid_spec = P('dp', 'dm')
    col_spec = P('dm', 'tp')
    row_spec = P('tp', 'dm')
    in_specs = (resid_spec, cache_spec, cache_spec, P('dp'), P('dm'), col_spec, col_spec, col_spec, row_spec, P('dm'), col_spec, col_spec, row_spec)
    out_specs = (resid_spec, cache_spec, cache_spec)
    sds = jax.ShapeDtypeStruct
    V = pltpu.VMEM

    def local_step(resid_in, k_cache, v_cache, cache_len, norm_attn, w_q, w_k, w_v, w_o, norm_mlp, w_gate, w_up, w_down):
        qkv, gain_all = call(
            qkv_kernel,
            (sds((3, 192, 256), F32), sds((8, 8, 128), F32)),
            [V((8, 3, 384, 256), BF), V((2, 4, 4, 4, 16, 384), BF), V((8, 192, 384), BF), V((8, 128), F32), V((8192, 128), BF)],
            40, 0, 58, 2 * 10**9, 'hhhhvv',
            resid_in, w_q, w_k, w_v, norm_attn.reshape(3, 128), norm_mlp.reshape(3, 128))
        lengths = lax.dynamic_slice_in_dim(cache_len, lax.axis_index('dm') * 192, 192)
        cache, step = sds((192, 16, 256), BF), 48
        attn_out, k_upd, v_upd = pl.pallas_call(
            attend_kernel, name='attend', out_shape=(sds((192, 256), BF), cache, cache), grid=(192 // step,), in_specs=[VM] * 5,
            out_specs=[pl.BlockSpec((step, 256), lambda b: (b, 0))] + [pl.BlockSpec((step, 16, 256), lambda b: (b, 0, 0))] * 2,
            compiler_params=pltpu.CompilerParams(vmem_limit_bytes=20 * 2**20),
        )(qkv, k_cache.reshape(192, 16, 256), v_cache.reshape(192, 16, 256), jnp.broadcast_to(lengths[:, None], (192, 128)), jnp.asarray(rope_table()))
        k_upd, v_upd = k_upd.reshape(192, 1, 16, 256), v_upd.reshape(192, 1, 16, 256)
        mine, theirs = call2(
            post_kernel,
            (sds((4, 192, 384), BF), sds((4, 192, 384), BF)),
            [V((4, 192, 256), BF), V((2, 256, 384), BF), V((48, 384), BF), V((2, 1536, 384), BF)]
            + [V((4, 192, 384), F32)] * 4 + [V((4, 2, 48, 384), BF)] + [V((4, 192, 1536), BF)] * 2 + [V((4, 192, 768), F32)] * 2
            + [V((3072, 768), BF), V((4, 192, 1536), BF), V((2, 4, 192, 384), BF), V((16384, 128), BF)]
            + scatter_scratch() + [V((48, 384), F32)] * 15 + [V((192, 384), F32)] * 3 + [V((48, 384), F32)] * 3,
            96, 1, 44, 7 * 10**9, 'vvvhhhv',
            attn_out, resid_in, w_o, w_gate, w_up, w_down, gain_all)
        resid_out = pl.pallas_call(join_kernel, out_shape=sds((1536, 384), BF), in_specs=[VM, VM], out_specs=VM, compiler_params=pltpu.CompilerParams(vmem_limit_bytes=8 * 2**20))(mine, theirs)
        return resid_out, k_upd, v_upd

    return jax.shard_map(local_step, mesh=mesh, in_specs=in_specs, out_specs=out_specs, check_vma=False)
```
